32 devices in a mesh: dp: 4 (over z), head: 2 (over y), mp: 4 (over x, core).
Axes of the slice: x: 2, y: 2, z: 4, core: 2. Of those that a mesh axis runs over, the one named last changes fastest.
Arguments:
- hidden: bfloat16 [16384, 1536], P(('dp', 'head'), 'mp'), may hold values from -6 to 6
- in_gain: float32 [1536], replicated, may hold values from 0.5 to 1.5
- proj_gate: bfloat16 [1536, 3072], P('mp', 'head'), may hold values from -0.15625 to 0.15625
- proj_input: bfloat16 [1536, 3072], P('mp', 'head'), may hold values from -0.15625 to 0.15625
- proj_state: bfloat16 [1536, 256], P('mp'), may hold values from -0.15625 to 0.15625
- proj_step: bfloat16 [1536, 48], P('mp', 'head'), may hold values from -0.15625 to 0.15625
- conv_input: float32 [4, 3072], replicated, may hold values from -3 to 3
- bias_input: float32 [3072], replicated, may hold values from -3 to 3
- conv_state: float32 [4, 256], replicated, may hold values from -3 to 3
- bias_state: float32 [256], replicated, may hold values from -3 to 3
- step_bias: float32 [48], replicated, may hold values from -6 to -2
- decay_log: float32 [48], replicated, may hold values from -1 to 2.5
- skip_gain: float32 [48], replicated, may hold values from 0.5 to 1.5
- gate_gain: float32 [3072], replicated, may hold values from 0.5 to 1.5
- proj_out: bfloat16 [3072, 1536], P('head', 'mp'), may hold values from -0.109375 to 0.109375
- segment_ids: int32 [16, 1024], P(('dp', 'mp')), may hold values from 0 to 3, never falling along the last dimension, each value on 1 to 512 neighbouring positions
- cotangent: bfloat16 [16384, 1536], P(('dp', 'head'), 'mp'), may hold values from -6 to 6
Outputs:
- block_out: bfloat16 [16384, 1536], P(('dp', 'head'), 'mp')
- hidden_grad: float32 [16384, 1536], P(('dp', 'head'), 'mp')
- in_gain_grad: float32 [1536], replicated
- proj_gate_grad: float32 [1536, 3072], P('mp', 'head')
- proj_input_grad: float32 [1536, 3072], P('mp', 'head')
- proj_state_grad: float32 [1536, 256], P('mp', 'head')
- proj_step_grad: float32 [1536, 48], P('mp', 'head')
- conv_input_grad: float32 [4, 3072], replicated
- bias_input_grad: float32 [3072], replicated
- conv_state_grad: float32 [4, 256], replicated
- bias_state_grad: float32 [256], replicated
- step_bias_grad: float32 [48], replicated
- decay_log_grad: float32 [48], replicated
- skip_gain_grad: float32 [48], replicated
- gate_gain_grad: float32 [3072], replicated
- proj_out_grad: float32 [3072, 1536], P('head', 'mp')
The draws below stay inside these ranges and needn't reach their ends.
Inputs may be any that keep to these rules, and one draw needn't show every extreme that they name: `segment_ids`: along each row of 1024 tokens the ids never fall; every row holds all four segments, each 1 to 512 tokens long, one of exactly 512 tokens.
All inputs are finite; a program needn't handle non-finite values.
Results may differ from the reference program's by a relative error of at most 0.008.
Values may be sent and summed in bfloat16 or wider, within the bound.
A program may use at most 256 MiB of HBM per device.

```python
import math
import jax
import jax.numpy as jnp
import numpy as np
from jax import lax

D = 1536
H = 48
P_SIZE = 64
NS = 128
KW = 4
SPAN = 256
LEN = 1024
SEQ_DEV = 1
HP = 3072
SEQS = 16
TOKENS = 16384


def levels(own_key, dims, cuts, low, high):
    level, own = 1.0, jax.random.fold_in(own_key, 6)
    for position, shards_of in cuts:
        draws = jnp.exp(jax.random.uniform(jax.random.fold_in(own, position), (shards_of,), jnp.float32, low / len(cuts), high / len(cuts)))
        level = level * jnp.repeat(draws, dims[position] // shards_of).reshape([-1 if axis == position else 1 for axis in range(len(dims))])
    return level


def split_up(amount, total, limit, slope):
    weights = [(1 << 20) // math.isqrt(standing ** slope) + 1 for standing in range(2, amount + 1)]
    surplus, given = total - limit - (amount - 1), [1] * (amount - 1)
    while surplus > 0:
        free = [i for i in range(amount - 1) if given[i] < limit]
        pool, budget = sum([weights[i] for i in free]), surplus
        for i in free:
            extra = min(limit - given[i], max(1, budget * weights[i] // pool), surplus)
            given[i] = given[i] + extra
            surplus = surplus - extra
    return np.array([limit] + given)


def ragged_sizes(stream_key, amount, total, most, lean):
    if amount == 2:
        one = jax.random.randint(stream_key, (), max(1, total - most), min(most, total - 1) + 1)
        return jnp.stack([one, total - one])
    tallies = jnp.asarray(split_up(amount, total, most, lean), jnp.int32)
    couples = (amount - 1) // 2
    donor, sink = tallies[1:1 + 2 * couples:2], tallies[2:2 + 2 * couples:2]
    margin = jnp.minimum(donor - 1, most - sink)
    passed = jax.random.randint(jax.random.fold_in(stream_key, 1), (couples,), 0, 1 << 20) % (margin + 1)
    tallies = tallies.at[1:1 + 2 * couples:2].set(donor - passed).at[2:2 + 2 * couples:2].set(sink + passed)
    return tallies[jax.random.permutation(jax.random.fold_in(stream_key, 2), amount)]


def bell_draw(own_key, extent, scale, most, split=(), dtype=jnp.bfloat16):
    values = scale * jax.random.normal(own_key, extent, jnp.float32)
    if split:
        values = values * levels(own_key, extent, split, -0.22, 0.18)
    return jnp.clip(values, -most, most).astype(dtype)


def setup_inputs(seed: int = 0) -> dict:
    seeds = jax.random.split(jax.random.key(seed), 18)
    hidden = bell_draw(seeds[0], (TOKENS, D), 1.0, 6.0, ((0, 8), (1, 4)))
    in_gain = jnp.clip(1.0 + 0.1 * jax.random.normal(seeds[1], (D,), jnp.float32), 0.5, 1.5)
    proj_gate = bell_draw(seeds[2], (D, HP), D ** -0.5, 0.15625, ((0, 4), (1, 2)))
    proj_input = bell_draw(seeds[3], (D, HP), D ** -0.5, 0.15625, ((0, 4), (1, 2)))
    proj_state = bell_draw(seeds[4], (D, 2 * NS), D ** -0.5, 0.15625, ((0, 4),))
    proj_step = bell_draw(seeds[5], (D, H), D ** -0.5, 0.15625, ((0, 4), (1, 2)))
    conv_input = bell_draw(seeds[6], (KW, HP), KW ** -0.5, 3.0, (), jnp.float32)
    bias_input = bell_draw(seeds[7], (HP,), 0.5, 3.0, (), jnp.float32)
    conv_state = bell_draw(seeds[8], (KW, 2 * NS), KW ** -0.5, 3.0, (), jnp.float32)
    bias_state = bell_draw(seeds[9], (2 * NS,), 0.5, 3.0, (), jnp.float32)
    step_bias = jnp.clip(jax.random.uniform(seeds[10], (H,), jnp.float32, -6.0, -2.0), -6.0, -2.0)
    decay_log = jnp.clip(jax.random.uniform(seeds[11], (H,), jnp.float32, -1.0, 2.5), -1.0, 2.5)
    skip_gain = jnp.clip(jax.random.uniform(seeds[12], (H,), jnp.float32, 0.5, 1.5), 0.5, 1.5)
    gate_gain = jnp.clip(1.0 + 0.1 * jax.random.normal(seeds[13], (HP,), jnp.float32), 0.5, 1.5)
    proj_out = bell_draw(seeds[14], (HP, D), HP ** -0.5, 0.109375, ((0, 2), (1, 4)))
    segment_ids = jax.vmap(lambda own: jnp.searchsorted(jnp.cumsum(ragged_sizes(own, 4, LEN, LEN // 2, 0)), jnp.arange(LEN), side="right"))(jax.random.split(seeds[15], SEQS)).reshape((SEQS, LEN)).astype(jnp.int32)
    cotangent = bell_draw(seeds[16], (TOKENS, D), 1.0, 6.0, ((0, 8), (1, 4)))
    return {"hidden": hidden, "in_gain": in_gain, "proj_gate": proj_gate, "proj_input": proj_input, "proj_state": proj_state, "proj_step": proj_step, "conv_input": conv_input, "bias_input": bias_input, "conv_state": conv_state, "bias_state": bias_state, "step_bias": step_bias, "decay_log": decay_log, "skip_gain": skip_gain, "gate_gain": gate_gain, "proj_out": proj_out, "segment_ids": segment_ids, "cotangent": cotangent}


EPS = 1e-05
HIGH = lax.Precision.HIGHEST

@jax.custom_vjp
def low(v):
    return lax.optimization_barrier(v.astype(jnp.bfloat16)).astype(jnp.float32)

@jax.custom_vjp
def low_back(v):
    return v

def low_keep(v):
    return (low(v), None)

def low_pass(kept, grad):
    return (grad,)

def back_keep(v):
    return (v, None)

def back_low(kept, grad):
    return (low(grad),)
low.defvjp(low_keep, low_pass)
low_back.defvjp(back_keep, back_low)

def causal_conv(values, taps_weight, bias_row, seg_rows):
    num_seqs, length = seg_rows.shape
    channels = values.shape[1]
    field_grid = values.reshape(num_seqs, length, channels)
    tap_count = taps_weight.shape[0]
    summed = field_grid * taps_weight[tap_count - 1] + bias_row
    for offset in range(1, tap_count):
        shifted = jnp.pad(field_grid, ((0, 0), (offset, 0), (0, 0)))[:, :length]
        labels = jnp.pad(seg_rows, ((0, 0), (offset, 0)), constant_values=-1)[:, :length]
        matching = (labels == seg_rows)[:, :, None]
        summed = summed + jnp.where(matching, shifted, 0.0) * taps_weight[tap_count - 1 - offset]
    return summed.reshape(num_seqs * length, channels)

def ssd_scan(inputs, input_keys, input_reads, step_sizes, decay_rates, seg_rows, block_size):
    num_seqs, length = seg_rows.shape
    blocks = length // block_size
    head_count = step_sizes.shape[1]
    head_dim = inputs.shape[2]
    state_size = input_keys.shape[1]

    def to_blocks(tensor):
        shaped = tensor.reshape((num_seqs, blocks, block_size) + tensor.shape[1:])
        return jnp.moveaxis(shaped, 1, 0)
    series = (to_blocks(inputs), to_blocks(input_keys), to_blocks(input_reads), to_blocks(step_sizes), to_blocks(seg_rows.reshape(-1)))
    positions = jnp.arange(block_size)
    causal_mask = positions[:, None] >= positions[None, :]

    def advance(carry, piece):
        state_now, before = carry
        value_block, key_block, read_block, step_block, label_block = piece
        cumulative = jnp.cumsum(step_block * decay_rates, axis=1)
        matching = (label_block[:, :, None] == label_block[:, None, :]) & causal_mask
        log_gaps = cumulative[:, :, None, :] - cumulative[:, None, :, :]
        decays = jnp.where(matching[..., None], jnp.exp(jnp.where(matching[..., None], log_gaps, 0.0)), 0.0)
        intersections = jnp.einsum('sin,sjn->sij', read_block, key_block, precision=HIGH)
        mixing = decays * intersections[..., None] * step_block[:, None, :, :]
        result = jnp.einsum('sijh,sjhp->sihp', mixing, value_block, precision=HIGH)
        carried = jnp.einsum('sin,shpn->sihp', read_block, state_now, precision=HIGH)
        continues = (label_block == before[:, None])[:, :, None, None]
        result = result + jnp.where(continues, jnp.exp(cumulative)[..., None] * carried, 0.0)
        last_label = label_block[:, -1]
        trailing = (label_block == last_label[:, None])[:, :, None]
        weights = jnp.where(trailing, jnp.exp(cumulative[:, -1:, :] - cumulative), 0.0) * step_block
        increment = jnp.einsum('sjh,sjhp,sjn->shpn', weights, value_block, key_block, precision=HIGH)
        unbroken = (last_label == before)[:, None, None, None]
        state_now = jnp.where(unbroken, jnp.exp(cumulative[:, -1, :])[:, :, None, None] * state_now, 0.0) + increment
        return ((state_now, last_label), result)
    initial = (jnp.zeros((num_seqs, head_count, head_dim, state_size), jnp.float32), jnp.full((num_seqs,), -1, jnp.int32))
    ignore, outputs = lax.scan(jax.checkpoint(advance), initial, series)
    return jnp.moveaxis(outputs, 0, 1).reshape(num_seqs * length, head_count, head_dim)

def layer(params, rows, seg_rows):
    in_gain, proj_gate, proj_input, proj_state, proj_step, conv_input, bias_input, conv_state, bias_state, step_bias, decay_log, skip_gain, gate_gain, proj_out = params
    scale_one = lax.rsqrt(lax.optimization_barrier(jnp.mean(rows * rows, axis=1, keepdims=True)) + EPS)
    normed = low(rows * scale_one * in_gain)
    gate_pre = low_back(jnp.dot(normed, proj_gate, precision=HIGH))
    input_pre = low_back(jnp.dot(normed, proj_input, precision=HIGH))
    state_pre = low_back(jnp.dot(normed, proj_state, precision=HIGH))
    step_pre = low_back(jnp.dot(normed, proj_step, precision=HIGH))
    mixed_inputs = jax.nn.silu(causal_conv(input_pre, conv_input, bias_input, seg_rows))
    mixed_states = jax.nn.silu(causal_conv(state_pre, conv_state, bias_state, seg_rows))
    step_sizes = jax.nn.softplus(step_pre + step_bias)
    tokens_here = rows.shape[0]
    shaped = mixed_inputs.reshape(tokens_here, H, P_SIZE)
    scanned = ssd_scan(shaped, mixed_states[:, :NS], mixed_states[:, NS:], step_sizes, -jnp.exp(decay_log), seg_rows, SPAN)
    joined = (scanned + skip_gain[None, :, None] * shaped).reshape(tokens_here, H * P_SIZE)
    gated_rows = joined * jax.nn.silu(gate_pre)
    scale_two = lax.rsqrt(lax.optimization_barrier(jnp.mean(gated_rows * gated_rows, axis=1, keepdims=True)) + EPS)
    inner_out = low(gated_rows * scale_two * gate_gain)
    return rows + jnp.dot(inner_out, proj_out, precision=HIGH)

def reference(hidden, in_gain, proj_gate, proj_input, proj_state, proj_step, conv_input, bias_input, conv_state, bias_state, step_bias, decay_log, skip_gain, gate_gain, proj_out, segment_ids, cotangent):
    params = tuple((tensor.astype(jnp.float32) for tensor in (in_gain, proj_gate, proj_input, proj_state, proj_step, conv_input, bias_input, conv_state, bias_state, step_bias, decay_log, skip_gain, gate_gain, proj_out)))
    group_rows = SEQ_DEV * LEN
    group_count = TOKENS // group_rows
    series = (hidden.astype(jnp.float32).reshape(group_count, group_rows, D), segment_ids.reshape(group_count, SEQ_DEV, LEN), cotangent.astype(jnp.float32).reshape(group_count, group_rows, D))

    def visit_group(totals, element):
        rows_in, labels, upstream = element
        result, pullback = jax.vjp(lambda weights, values: layer(weights, values, labels), params, rows_in)
        gradients, row_grad = pullback(upstream)
        totals = jax.tree.map(jnp.add, totals, gradients)
        return (totals, (result.astype(jnp.bfloat16), row_grad))
    initial = jax.tree.map(jnp.zeros_like, params)
    totals, (results, row_grads) = lax.scan(visit_group, initial, series)
    return (results.reshape(TOKENS, D), row_grads.reshape(TOKENS, D), totals[0], totals[1], totals[2], totals[3], totals[4], totals[5], totals[6], totals[7], totals[8], totals[9], totals[10], totals[11], totals[12], totals[13])
```

```python
import functools
import jax
import jax.numpy as jnp
from jax import lax
from jax.sharding import PartitionSpec as P
from jax.experimental import pallas as pl
from jax.experimental.pallas import tpu as pltpu

T = 128
PH = 64
NEG = -1e30
BF = jnp.bfloat16
F32 = jnp.float32


def mm(a, b):
    return jnp.dot(a, b, preferred_element_type=F32)


def mm_nt(a, b):
    return lax.dot_general(a, b, (((1,), (1,)), ((), ())), preferred_element_type=F32)


def sigm(v):
    return 0.5 * jnp.tanh(0.5 * v) + 0.5


def iota(shape, axis):
    return lax.broadcasted_iota(jnp.int32, shape, axis)


def prefix_sum(v):
    rows = iota(v.shape, 0)
    step = 1
    while step < v.shape[0]:
        v = v + jnp.where(rows >= step, pltpu.roll(v, step, 0), 0.0)
        step *= 2
    return v


def suffix_sum(v):
    size = v.shape[0]
    rows = iota(v.shape, 0)
    step = 1
    while step < size:
        v = v + jnp.where(rows < size - step, pltpu.roll(v, size - step, 0), 0.0)
        step *= 2
    return v


def step_values(z):
    dt = jnp.maximum(z, 0.0) + jnp.log1p(jnp.exp(-jnp.abs(z)))
    low = z < -15.0
    logdt = jnp.where(low, z, jnp.log(jnp.where(low, 1.0, dt)))
    return dt, logdt


def tile2(v, reps):
    return v if reps == 1 else jnp.concatenate([v] * reps, axis=1)


def per_pair(cols, width):
    lanes = iota((T, 128), 1)
    out = []
    for p in range(len(cols) // 2):
        out.append(jnp.where(lanes < PH, cols[2 * p], cols[2 * p + 1]))
    return out[0] if len(out) == 1 else jnp.concatenate(out, axis=1)


def block_diag(v):
    lanes = iota(v.shape, 1)
    zero = jnp.zeros_like(v)
    return jnp.concatenate([jnp.where(lanes < PH, v, zero), jnp.where(lanes >= PH, v, zero)], axis=0)


def head_cols(mat, group, hq):
    shift = lax.rem(128 - group * hq, 128)
    rolled = pltpu.roll(mat, shift, 1)
    return [jnp.broadcast_to(rolled[:, i : i + 1], (T, 128)) for i in range(hq)]


MESH = pl.DeviceIdType.MESH
ANY = pl.BlockSpec(memory_space=pl.ANY)
FWD_CHUNKS = 4


class Spot:
    def __init__(self, dp):
        self.dp = dp
        self.z = lax.axis_index("dp")
        self.y = lax.axis_index("head")
        m = lax.axis_index("mp")
        self.x = m // 2
        self.c = m % 2
        self.same = self.x == self.y

    def at(self, z, y, x, c):
        return (z, y, 2 * x + c)

    def core(self):
        return self.at(self.z, self.y, self.x, 1 - self.c)

    def meet(self):
        sem = pltpu.get_barrier_semaphore()
        peers = []
        for dy in range(2):
            for dx in range(2):
                for dc in range(2):
                    if dy + dx + dc:
                        peers.append((self.z, (self.y + dy) % 2, 2 * ((self.x + dx) % 2) + (self.c + dc) % 2))
        for r in range(1, self.dp):
            peers.append(((self.z + r) % self.dp, self.y, 2 * self.x + self.c))
        for p in peers:
            pl.semaphore_signal(sem, inc=1, device_id=p, device_id_type=MESH)
        pl.semaphore_wait(sem, len(peers))


def remote(src, dst, ss, rs, dev):
    return pltpu.make_async_remote_copy(src_ref=src, dst_ref=dst, send_sem=ss, recv_sem=rs, device_id=dev, device_id_type=MESH)


class RowsGather:
    def __init__(self, spot, src, dst, fbuf, bounce, ss, rs, ls):
        self.p, self.src, self.dst, self.fbuf, self.bounce, self.ss, self.rs, self.ls = spot, src, dst, fbuf, bounce, ss, rs, ls
        self.R = dst.shape[0]
        self.w = dst.shape[1] // 4
        self.n = self.R * 7 // 32 // 16 * 16
        self.far = self.n * FWD_CHUNKS

    def rows(self, t):
        return pl.ds(pl.multiple_of(t * self.R, 16), self.R)

    def cols(self, pos):
        return pl.ds(pl.multiple_of(pos * self.w, 128), self.w)

    def local_in(self):
        return pltpu.make_async_copy(self.src.at[self.rows(self.p.c), :], self.bounce, self.ls.at[0])

    def local_out(self):
        return pltpu.make_async_copy(self.bounce, self.dst.at[:, self.cols(0)], self.ls.at[1])

    def to_core(self):
        p = self.p
        return remote(self.src.at[self.rows(1 - p.c), :], self.dst.at[:, self.cols(2)], self.ss.at[0], self.rs.at[2], p.core())

    def to_y(self, t):
        p = self.p
        j = (p.c + t) % 2
        return remote(self.src.at[self.rows(t), :], self.dst.at[:, self.cols(2 * j)], self.ss.at[1 + t], self.rs.at[2 * j],
                      p.at(p.z, 1 - p.y, p.x, t))

    def to_x(self, t):
        p = self.p
        j = (p.c + t) % 2
        return remote(self.src.at[self.rows(t), :], self.dst.at[:, self.cols(2 * j + 1)], self.ss.at[t], self.rs.at[2 * j + 1],
                      p.at(p.z, p.y, 1 - p.x, t))

    def to_diag(self, t):
        p = self.p
        j = (p.c + t) % 2
        n = self.R - self.far
        return remote(self.src.at[pl.ds(pl.multiple_of(t * self.R + self.far, 16), n), :],
                      self.dst.at[pl.ds(self.far, n), self.cols(2 * j + 1)], self.ss.at[2 + t], self.rs.at[2 * j + 1],
                      p.at(p.z, 1 - p.y, 1 - p.x, t))

    def to_relay(self, k, t):
        p = self.p
        return remote(self.src.at[pl.ds(pl.multiple_of(t * self.R + k * self.n, 16), self.n), :],
                      self.fbuf.at[t, pl.ds(k * self.n, self.n), :], self.ss.at[4 + 2 * k + t], self.rs.at[4 + 2 * k + t],
                      p.at(p.z, 1 - p.y, p.x, p.c))

    def relay(self, k, t):
        p = self.p
        j = (p.c + t) % 2
        return remote(self.fbuf.at[t, pl.ds(k * self.n, self.n), :],
                      self.dst.at[pl.ds(k * self.n, self.n), self.cols(2 * j + 1)], self.ss.at[4 + 2 * k + t],
                      self.rs.at[4 + 2 * k + j], p.at(p.z, p.y, 1 - p.x, t))

    def start(self):
        @pl.when(self.p.same)
        def _():
            self.to_y(0).start()
            self.to_y(1).start()
            self.to_core().start()
            self.local_in().start()

        @pl.when(jnp.logical_not(self.p.same))
        def _():
            for k in range(FWD_CHUNKS):
                for t in range(2):
                    self.to_relay(k, t).start()
            for t in range(2):
                self.to_x(t).start()
            for t in range(2):
                self.to_diag(t).start()

    def forward(self, k):
        @pl.when(self.p.same)
        def _():
            if k == 0:
                self.local_in().wait()
                self.local_out().start()
            for t in range(2):
                self.to_relay(k, t).wait_recv()
                self.relay(k, t).start()

    def finish(self):
        @pl.when(self.p.same)
        def _():
            self.to_core().wait()
            for j in range(2):
                self.to_x_wait(j)
            for t in range(2):
                self.to_y(t).wait_send()
                for k in range(FWD_CHUNKS):
                    self.relay(k, t).wait_send()
            self.local_out().wait()

        @pl.when(jnp.logical_not(self.p.same))
        def _():
            for t in range(2):
                self.to_y(t).wait_recv()
                self.to_x(t).wait_send()
                self.to_diag(t).wait()
                for k in range(FWD_CHUNKS):
                    self.relay(k, t).wait_recv()
                    self.to_relay(k, t).wait_send()

    def to_x_wait(self, t):
        self.to_x(t).wait_recv()


class WeightGather:
    def __init__(self, spot, src, dst, axis, bounce, ss, rs, ls):
        self.p, self.src, self.dst, self.axis, self.bounce, self.ss, self.rs, self.ls = spot, src, dst, axis, bounce, ss, rs, ls
        self.n = src.shape[0] // spot.dp

    def chunk(self, k):
        return self.src.at[pl.ds(pl.multiple_of(k * self.n, 16), self.n), :]

    def slot(self, pos, k=None):
        size = self.src.shape[0]
        width = self.src.shape[1]
        if self.axis == 0:
            if k is None:
                return self.dst.at[pl.ds(pos * size, size), :]
            return self.dst.at[pl.ds(pl.multiple_of(pos * size + k * self.n, 16), self.n), :]
        cols = pl.ds(pos * width, width)
        if k is None:
            return self.dst.at[:, cols]
        return self.dst.at[pl.ds(pl.multiple_of(k * self.n, 16), self.n), cols]

    def to_x(self):
        p = self.p
        return remote(self.chunk(p.z), self.slot(1, p.z), self.ss.at[0], self.rs.at[0], p.at(p.z, p.y, 1 - p.x, p.c))

    def to_core(self):
        return remote(self.src, self.slot(2), self.ss.at[1], self.rs.at[1], self.p.core())

    def to_z(self, r):
        p = self.p
        return remote(self.slot(1, p.z), self.slot(1, p.z), self.ss.at[1 + r], self.rs.at[1 + r],
                      p.at((p.z + r) % p.dp, p.y, p.x, p.c))

    def across(self, r):
        p = self.p
        k = (p.z + p.dp - r) % p.dp
        return remote(self.slot(1, k), self.slot(3, k), self.ss.at[1 + p.dp + r], self.rs.at[1 + p.dp + r], p.core())

    def local_in(self):
        return pltpu.make_async_copy(self.src, self.bounce, self.ls.at[0])

    def local_out(self):
        return pltpu.make_async_copy(self.bounce, self.slot(0), self.ls.at[1])

    def start(self):
        self.to_x().start()
        self.to_core().start()
        self.local_in().start()

    def middle(self):
        self.to_x().wait_recv()
        for r in range(1, self.p.dp):
            self.to_z(r).start()
        self.across(0).start()
        self.local_in().wait()
        self.local_out().start()

    def spread(self):
        for r in range(1, self.p.dp):
            self.to_z(r).wait_recv()
            self.across(r).start()

    def finish(self):
        self.to_x().wait_send()
        self.to_core().wait()
        for r in range(1, self.p.dp):
            self.to_z(r).wait_send()
        for r in range(self.p.dp):
            self.across(r).wait()
        self.local_out().wait()


ROW_SEMS = 4 + 2 * FWD_CHUNKS


def rows_scratch(src):
    R, w = src.shape[0] // 2, src.shape[1]
    dma = pltpu.SemaphoreType.DMA
    return [pltpu.VMEM((2, R, w), BF), pltpu.VMEM((R, w), BF), dma((ROW_SEMS,)), dma((ROW_SEMS,)), dma((2,))]


def weight_scratch(src, dp):
    dma = pltpu.SemaphoreType.DMA
    return [pltpu.VMEM(src.shape, BF), dma((1 + 2 * dp,)), dma((1 + 2 * dp,)), dma((2,))]


def front_kernel(dp, h, wa, hid, waf, *scr):
    spot = Spot(dp)
    rg = RowsGather(spot, h, hid, *scr[:5])
    wg = WeightGather(spot, wa, waf, 0, *scr[5:])
    spot.meet()
    wg.start()
    rg.start()
    wg.middle()
    rg.forward(0)
    rg.forward(1)
    rg.forward(2)
    wg.spread()
    rg.forward(3)
    wg.finish()
    rg.finish()


def front_gather(h, wa, dp):
    R, w = h.shape[0] // 2, h.shape[1]
    return pl.pallas_call(
        functools.partial(front_kernel, dp),
        in_specs=[ANY, ANY],
        out_specs=[ANY, ANY],
        out_shape=[jax.ShapeDtypeStruct((R, 4 * w), BF), jax.ShapeDtypeStruct((4 * wa.shape[0], wa.shape[1]), BF)],
        scratch_shapes=rows_scratch(h) + weight_scratch(wa, dp),
        compiler_params=pltpu.CompilerParams(collective_id=1, has_side_effects=True, vmem_limit_bytes=16 << 20),
        name="front_gather",
    )(h, wa)


def fwd_kernel(hq, groups, dp, *refs):
    inp, st, stp, segb, segr, cw, cb, cws, cbs, sbias, arow, skip = refs[:12]
    if dp:
        cot, wg, wo = refs[12:15]
        j_out, s_out, cotf, wgf, wof = refs[15:20]
        S, vbuf, sbuf, gbuf, mbuf, cjt = refs[20:26]
        scr = refs[26:]
    else:
        j_out, s_out = refs[12:14]
        S, vbuf, sbuf, gbuf, mbuf, cjt = refs[14:20]
    c = pl.program_id(0)
    W = hq * PH
    reps = W // 128
    if dp:
        spot = Spot(dp)
        rg = RowsGather(spot, cot, cotf, *scr[:5])
        ga = WeightGather(spot, wg, wgf, 0, *scr[5:9])
        go = WeightGather(spot, wo, wof, 1, *scr[9:13])

        @pl.when(c == 0)
        def _():
            spot.meet()
            ga.start()
            go.start()
            rg.start()

        @pl.when(c == 2)
        def _():
            ga.middle()

        @pl.when(c == 3)
        def _():
            go.middle()
            rg.forward(0)

        @pl.when(c == 5)
        def _():
            rg.forward(1)
            rg.forward(2)

    @pl.when(c == 0)
    def _():
        S[...] = jnp.zeros_like(S)
        vbuf[pl.ds(0, 8), :] = jnp.zeros((8, vbuf.shape[1]), F32)
        sbuf[pl.ds(0, 8), :] = jnp.zeros((8, sbuf.shape[1]), F32)
        gbuf[pl.ds(0, 8), :] = jnp.full((8, 128), -1.0, F32)

    @pl.when(c > 0)
    def _():
        vbuf[pl.ds(0, 8), :] = vbuf[pl.ds(T, 8), :]
        sbuf[pl.ds(0, 8), :] = sbuf[pl.ds(T, 8), :]
        gbuf[pl.ds(0, 8), :] = gbuf[pl.ds(T, 8), :]

    vbuf[pl.ds(8, T), :] = inp[...]
    sbuf[pl.ds(8, T), :] = st[...]
    gbuf[pl.ds(8, T), :] = segb[...]
    seg = segb[...]
    for k in range(1, 4):
        mbuf[k - 1] = jnp.where(gbuf[pl.ds(8 - k, T), :] == seg, 1.0, 0.0)
    before = gbuf[pl.ds(7, 1), :]
    last = gbuf[pl.ds(T + 7, 1), :]
    cs = sbuf[pl.ds(8, T), :] * cws[3:4, :] + cbs[...]
    for k in range(1, 4):
        cs = cs + tile2(mbuf[k - 1], 2) * sbuf[pl.ds(8 - k, T), :] * cws[3 - k : 4 - k, :]
    ms = cs * sigm(cs)
    Bf = ms[:, :128]
    Bb = Bf.astype(BF)
    Cb = ms[:, 128:].astype(BF)
    Bt = Bf.T.astype(BF)
    G = mm_nt(Cb, Bb)
    dt, logdt = step_values(stp[...] + sbias[...])
    cum = prefix_sum(arow[...] * dt)
    cj = cum - logdt
    cjt[...] = cj.T
    rows = iota((T, T), 0)
    cols = iota((T, T), 1)
    segrow = segr[pl.ds(c, 1), :]
    maskb = jnp.where((seg == segrow) & (rows >= cols), 0.0, NEG)
    cont = tile2(jnp.where(seg == before, 1.0, 0.0), reps)
    trail = tile2(jnp.where(seg == last, 1.0, 0.0), reps)
    unbroken = tile2(jnp.where(last == before, 1.0, 0.0), reps)

    def body(q, carry):
        lane = pl.ds(pl.multiple_of(q * W, 128), W)
        cv = vbuf[pl.ds(8, T), lane] * cw[3:4, lane] + cb[:, lane]
        for k in range(1, 4):
            cv = cv + tile2(mbuf[k - 1], reps) * vbuf[pl.ds(8 - k, T), lane] * cw[3 - k : 4 - k, lane]
        x = cv * sigm(cv)
        xb = x.astype(BF)
        tcols = head_cols(cum, q, hq)
        jcols = head_cols(cj, q, hq)
        M = []
        for i in range(hq):
            row = cjt[pl.ds(q * hq + i, 1), :]
            M.append((jnp.exp(tcols[i] - row + maskb) * G).astype(BF))
        yin = []
        for p in range(hq // 2):
            yin.append(mm(jnp.concatenate(M[2 * p : 2 * p + 2], axis=1), block_diag(xb[:, 128 * p : 128 * p + 128])))
        yintra = yin[0] if len(yin) == 1 else jnp.concatenate(yin, axis=1)
        te = per_pair(tcols, W)
        tl = te[T - 1 : T, :]
        Sq = S[:, lane]
        Sb = Sq.astype(BF)
        yinter = mm(Cb, Sb) * (jnp.exp(te) * cont)
        s_out[0, :, lane] = Sb
        j_out[:, lane] = (yintra + yinter) + skip[:, lane] * x
        w = jnp.exp(tl - per_pair(jcols, W)) * trail
        wx = (x * w).astype(BF)
        S[:, lane] = Sq * (jnp.exp(tl) * unbroken) + mm(Bt, wx)
        return carry

    lax.fori_loop(0, groups, body, 0)
    if dp:
        @pl.when(c == pl.num_programs(0) - 1)
        def _():
            ga.spread()
            rg.forward(3)
            go.spread()
            ga.finish()
            go.finish()
            rg.finish()


def full(shape):
    return pl.BlockSpec(shape, lambda i: (0,) * len(shape))


def scan_forward(proj, segb, segr, cw, cb, cws, cbs, sbias, arow, skip, gain, moves=None, dp=0):
    L = proj.shape[0]
    CI = proj.shape[1] - 384
    heads = CI // PH
    hq = 4 if heads % 4 == 0 else 2
    nch = L // T
    blk = lambda w: pl.BlockSpec((T, w), lambda i: (i, 0))
    part = lambda w, at: pl.BlockSpec((T, w), lambda i: (i, at // w))
    outs = [jax.ShapeDtypeStruct((L, CI), F32), jax.ShapeDtypeStruct((nch, 128, CI), BF)]
    out_specs = [blk(CI), pl.BlockSpec((1, 128, CI), lambda i: (i, 0, 0))]
    scratch = [pltpu.VMEM((128, CI), F32), pltpu.VMEM((T + 8, CI), F32), pltpu.VMEM((T + 8, 256), F32),
               pltpu.VMEM((T + 8, 128), F32), pltpu.VMEM((3, T, 128), F32), pltpu.VMEM((128, T), F32)]
    extra = {}
    ins = []
    if dp:
        cot, wg, wo = ins = list(moves)
        outs += [jax.ShapeDtypeStruct((cot.shape[0] // 2, 4 * cot.shape[1]), BF), jax.ShapeDtypeStruct((4 * wg.shape[0], wg.shape[1]), BF),
                 jax.ShapeDtypeStruct((wo.shape[0], 4 * wo.shape[1]), BF)]
        scratch += rows_scratch(cot) + weight_scratch(wg, dp) + weight_scratch(wo, dp)
        extra = dict(collective_id=2, has_side_effects=True)
    return pl.pallas_call(
        functools.partial(fwd_kernel, hq, heads // hq, dp),
        grid=(nch,),
        in_specs=[blk(CI), part(256, CI), part(128, CI + 256), blk(128), full(segr.shape), full(cw.shape), full(cb.shape),
                  full(cws.shape), full(cbs.shape), full(sbias.shape), full(arow.shape), full(skip.shape)] + [ANY] * len(ins),
        out_specs=out_specs + [ANY] * len(ins),
        out_shape=outs,
        scratch_shapes=scratch,
        compiler_params=pltpu.CompilerParams(dimension_semantics=("arbitrary",), vmem_limit_bytes=40 << 20, **extra),
        cost_estimate=pl.CostEstimate(flops=2 * L * CI * (2 * T + 256), bytes_accessed=L * CI * 12, transcendentals=L * CI * 6),
        name="scan_forward",
    )(proj, proj, proj, segb, segr, cw, cb, cws, cbs, sbias, arow, skip, *ins)


NB = 256


def out_kernel(nrm, wg, jn, gain, wo, cot, gate_out, u_out, p_out, ss_out, dots_out, acc):
    CI = jn.shape[1]
    D = cot.shape[1]
    nb = 128 if CI % NB else NB
    acc[...] = jnp.zeros_like(acc)

    def one(n, carry):
        lane = pl.ds(pl.multiple_of(n * nb, nb), nb)
        gt = mm(nrm[...], wg[:, lane])
        gate_out[:, lane] = gt
        gated = jn[:, lane] * (gt * sigm(gt))
        u_out[:, lane] = (gated * gain[:, lane]).astype(BF)
        sq = gated * gated
        for p in range(nb // 128):
            acc[0] += sq[:, 128 * p : 128 * p + 128]
        return carry

    def two(n, carry):
        lane = pl.ds(pl.multiple_of(n * NB, NB), NB)
        pv = mm(u_out[...], wo[:, lane])
        p_out[:, lane] = pv
        d = pv * cot[:, lane].astype(F32)
        for p in range(NB // 128):
            acc[1] += d[:, 128 * p : 128 * p + 128]
        return carry

    lax.fori_loop(0, CI // nb, one, 0)
    lax.fori_loop(0, D // NB, two, 0)
    ss_out[...] = jnp.broadcast_to(jnp.sum(acc[0], axis=1, keepdims=True), ss_out.shape)
    dots_out[...] = jnp.broadcast_to(jnp.sum(acc[1], axis=1, keepdims=True), ss_out.shape)


def gate_and_out(nrm, wg, jn, gain, wo, cot):
    L, D = nrm.shape
    CI = wg.shape[1]
    R = 256
    blk = lambda w: pl.BlockSpec((R, w), lambda i: (i, 0))
    once = lambda shape: pl.BlockSpec(shape, lambda i: (0, 0), pipeline_mode=pl.Buffered(1))
    return pl.pallas_call(
        out_kernel,
        grid=(L // R,),
        in_specs=[blk(D), once(wg.shape), blk(CI), full(gain.shape), once(wo.shape), blk(D)],
        out_specs=[blk(CI), blk(CI), blk(D), blk(128), blk(128)],
        out_shape=[jax.ShapeDtypeStruct((L, CI), F32), jax.ShapeDtypeStruct((L, CI), BF), jax.ShapeDtypeStruct((L, D), F32),
                   jax.ShapeDtypeStruct((L, 128), F32), jax.ShapeDtypeStruct((L, 128), F32)],
        scratch_shapes=[pltpu.VMEM((2, R, 128), F32)],
        compiler_params=pltpu.CompilerParams(dimension_semantics=("arbitrary",), vmem_limit_bytes=40 << 20),
        cost_estimate=pl.CostEstimate(flops=4 * L * CI * D, bytes_accessed=L * D * 22 + CI * D * 4, transcendentals=L * CI),
        name="gate_and_out",
    )(nrm, wg, jn, gain, wo, cot)


def back_kernel(gg, ca, wg, wa, hid, s1, gain, h_out, ig_out, ng):
    D = hid.shape[1]

    @pl.when(pl.program_id(0) == 0)
    def _():
        ig_out[...] = jnp.zeros_like(ig_out)

    def one(n, srow):
        lane = pl.ds(pl.multiple_of(n * NB, NB), NB)
        v = mm_nt(gg[...], wg[lane, :]) + mm_nt(ca[...], wa[lane, :])
        rows = hid[:, lane].astype(F32)
        sv = jnp.concatenate([s1[...]] * (NB // 128), axis=1)
        t = v * rows
        ig_out[0:8, lane] += sum8(t * sv)
        v = v * gain[:, lane]
        ng[:, lane] = v
        t = v * rows
        for p in range(NB // 128):
            srow = srow + t[:, 128 * p : 128 * p + 128]
        return srow

    srow = lax.fori_loop(0, D // NB, one, jnp.zeros((hid.shape[0], 128), F32))
    sc = s1[...]
    coef = sc * sc * sc * (jnp.sum(srow, axis=1, keepdims=True) / D)

    def two(n, carry):
        lane = pl.ds(pl.multiple_of(n * 128, 128), 128)
        h_out[:, lane] = (ng[:, lane] * sc - hid[:, lane].astype(F32) * coef).astype(BF)
        return carry

    lax.fori_loop(0, D // 128, two, 0)


def sum8(v):
    acc = v[0:8]
    for r in range(1, v.shape[0] // 8):
        acc = acc + v[8 * r : 8 * r + 8]
    return acc


def input_backward(gg, ca, wg, wa, hid, s1c, gain):
    L, D = hid.shape
    R = 256
    blk = lambda w: pl.BlockSpec((R, w), lambda i: (i, 0))
    once = lambda shape: pl.BlockSpec(shape, lambda i: (0, 0), pipeline_mode=pl.Buffered(1))
    return pl.pallas_call(
        back_kernel,
        grid=(L // R,),
        in_specs=[blk(gg.shape[1]), blk(ca.shape[1]), once(wg.shape), once(wa.shape), blk(D), blk(128), full(gain.shape)],
        out_specs=[blk(D), full((8, D))],
        out_shape=[jax.ShapeDtypeStruct((L, D), BF), jax.ShapeDtypeStruct((8, D), F32)],
        scratch_shapes=[pltpu.VMEM((R, D), F32)],
        compiler_params=pltpu.CompilerParams(dimension_semantics=("arbitrary",), vmem_limit_bytes=40 << 20),
        cost_estimate=pl.CostEstimate(flops=2 * L * D * (gg.shape[1] + ca.shape[1]), bytes_accessed=L * D * 10 + D * D * 4, transcendentals=0),
        name="input_backward",
    )(gg, ca, wg, wa, hid, s1c, gain)


def bwd_kernel(hq, groups, inp, inp8, gate, st, st8, stp, segb, segb8, segr, ig, y, s_in, s2c, cfc,
               cw, cb, cws, cbs, sbias, arow, skip, gain, eye,
               gg_out, ca_out, wg_out, ws_out, hg_out,
               dS, vbuf, sbuf, gbuf, mbuf, nbuf, pg, ps, cmt, Z, WT, DBC):
    i = pl.program_id(0)
    c = pl.num_programs(0) - 1 - i
    W = hq * PH
    reps = W // 128
    CI = gate.shape[1]

    @pl.when(i == 0)
    def _():
        dS[...] = jnp.zeros_like(dS)
        pg[pl.ds(T, 8), :] = jnp.zeros((8, CI), F32)
        gbuf[pl.ds(T + 8, 8), :] = jnp.full((8, 128), -1.0, F32)
        ps[pl.ds(T, 8), :] = jnp.zeros((8, 256), F32)
        wg_out[...] = jnp.zeros_like(wg_out)
        ws_out[...] = jnp.zeros_like(ws_out)
        hg_out[...] = jnp.zeros_like(hg_out)

    @pl.when(i > 0)
    def _():
        pg[pl.ds(T, 8), :] = pg[pl.ds(0, 8), :]
        ps[pl.ds(T, 8), :] = ps[pl.ds(0, 8), :]
        gbuf[pl.ds(T + 8, 8), :] = gbuf[pl.ds(8, 8), :]

    vbuf[pl.ds(0, 8), :] = inp8[...]
    vbuf[pl.ds(8, T), :] = inp[...]
    sbuf[pl.ds(0, 8), :] = st8[...]
    sbuf[pl.ds(8, T), :] = st[...]
    first = jnp.where(c == 0, 1.0, 0.0)
    gbuf[pl.ds(0, 8), :] = segb8[...] * (1.0 - first) - first
    gbuf[pl.ds(8, T), :] = segb[...]
    seg = segb[...]
    for k in range(1, 4):
        mbuf[k - 1] = jnp.where(gbuf[pl.ds(8 - k, T), :] == seg, 1.0, 0.0)
        nbuf[k - 1] = jnp.where(gbuf[pl.ds(8 + k, T), :] == seg, 1.0, 0.0)
    before = gbuf[pl.ds(7, 1), :]
    last = gbuf[pl.ds(T + 7, 1), :]
    cs = sbuf[pl.ds(8, T), :] * cws[3:4, :] + cbs[...]
    for k in range(1, 4):
        cs = cs + tile2(mbuf[k - 1], 2) * sbuf[pl.ds(8 - k, T), :] * cws[3 - k : 4 - k, :]
    ss = sigm(cs)
    ms = cs * ss
    Cf = ms[:, 128:]
    Bb = ms[:, :128].astype(BF)
    Cb = Cf.astype(BF)
    Ct = Cf.T.astype(BF)
    GT = mm_nt(Bb, Cb)
    z = stp[...] + sbias[...]
    dt, logdt = step_values(z)
    a = arow[...] * dt
    cum = prefix_sum(a)
    cj = cum - logdt
    cmt[...] = cum.T
    rows = iota((T, T), 0)
    cols = iota((T, T), 1)
    segrow = segr[pl.ds(c, 1), :]
    maskb = jnp.where((seg == segrow) & (rows <= cols), 0.0, NEG)
    cont = tile2(jnp.where(seg == before, 1.0, 0.0), reps)
    trail = tile2(jnp.where(seg == last, 1.0, 0.0), reps)
    unbroken = tile2(jnp.where(last == before, 1.0, 0.0), reps)
    s2 = tile2(s2c[...], reps)
    cf = tile2(cfc[...], reps)
    Z[...] = jnp.zeros_like(Z)
    WT[...] = jnp.zeros_like(WT)
    DBC[...] = jnp.zeros_like(DBC)

    def colsum(v):
        acc = v[0:8]
        for r in range(1, T // 8):
            acc = acc + v[8 * r : 8 * r + 8]
        return acc

    def body(q, carry):
        lane = pl.ds(pl.multiple_of(q * W, 128), W)
        v0 = vbuf[pl.ds(8, T), lane]
        cv = v0 * cw[3:4, lane] + cb[:, lane]
        vk = []
        for k in range(1, 4):
            vk.append(tile2(mbuf[k - 1], reps) * vbuf[pl.ds(8 - k, T), lane])
            cv = cv + vk[-1] * cw[3 - k : 4 - k, lane]
        sx = sigm(cv)
        x = cv * sx
        xb = x.astype(BF)
        xr = xb.astype(F32)
        gt = gate[:, lane]
        sg = sigm(gt)
        sl = gt * sg
        joined = y[:, lane]
        yv = joined - skip[:, lane] * x
        gated = joined * sl
        gi = ig[:, lane].astype(F32)
        gis = gi * s2
        gg = gis * gain[:, lane] - gated * cf
        gg_out[:, lane] = (gg * joined * (sg * (1.0 + gt * (1.0 - sg)))).astype(BF)
        g = gg * sl
        gb = g.astype(BF)
        gr = gb.astype(F32)
        tcols = head_cols(cum, q, hq)
        jcols = head_cols(cj, q, hq)
        te = per_pair(tcols, W)
        tl = te[T - 1 : T, :]
        ec = jnp.exp(te) * cont
        w = jnp.exp(tl - per_pair(jcols, W)) * trail
        dxs = []
        wt = jnp.zeros((T, T), F32)
        for p in range(hq // 2):
            gbd = block_diag(gb[:, 128 * p : 128 * p + 128])
            et = mm_nt(xb[:, 128 * p : 128 * p + 128], gbd)
            mts = []
            for h in range(2):
                n = 2 * p + h
                row = cmt[pl.ds(q * hq + n, 1), :]
                kt = jnp.exp(row - jcols[n] + maskb)
                mts.append((kt * GT).astype(BF))
                wt = wt + kt * et[:, T * h : T * h + T]
            dxs.append(mm(jnp.concatenate(mts, axis=1), gbd))
        WT[...] += wt
        dxi = dxs[0] if len(dxs) == 1 else jnp.concatenate(dxs, axis=1)
        Sb = s_in[0, :, lane]
        dSq = dS[:, lane]
        dSb = dSq.astype(BF)
        dxo = mm(Bb, dSb) * w
        wx = (x * w).astype(BF)
        eg = (g * ec).astype(BF)
        DBC[:, :128] += mm_nt(wx, dSb)
        DBC[:, 128:] += mm_nt(eg, Sb)
        el = jnp.exp(tl) * unbroken
        prow = jnp.sum(Sb.astype(F32) * dSq, axis=0, keepdims=True) * el
        dS[:, lane] = dSq * el + mm(Ct, eg)
        ci = xr * dxi
        co = xr * dxo
        stack = jnp.concatenate([gr * yv - ci, co, ci + co, jnp.broadcast_to(prow, (8, W))], axis=0)
        hi = stack.astype(BF)
        lo = (stack - hi.astype(F32)).astype(BF)
        ey = eye[pl.ds(pl.multiple_of(q * W, 128), W), :]
        Z[...] += mm(hi, ey) + mm(lo, ey)
        pre = (dxi + dxo + skip[:, lane] * g) * (sx * (1.0 + cv * (1.0 - sx)))
        pg[pl.ds(0, T), lane] = pre
        dv = pre * cw[3:4, lane]
        for k in range(1, 4):
            dv = dv + tile2(nbuf[k - 1], reps) * pg[pl.ds(k, T), lane] * cw[3 - k : 4 - k, lane]
        ca_out[:, lane] = dv.astype(BF)
        wg_out[0:8, lane] += colsum(pre * vk[2])
        wg_out[8:16, lane] += colsum(pre * vk[1])
        wg_out[16:24, lane] += colsum(pre * vk[0])
        wg_out[24:32, lane] += colsum(pre * v0)
        wg_out[32:40, lane] += colsum(pre)
        wg_out[40:48, lane] += colsum(g * x)
        wg_out[48:56, lane] += colsum(gis * gated)
        return carry

    lax.fori_loop(0, groups, body, 0)
    z2 = Z[T : 2 * T, :]
    D = suffix_sum(Z[0:T, :]) + (prefix_sum(z2) - z2) + Z[3 * T : 3 * T + 1, :]
    sz = sigm(z)
    lowz = z < -15.0
    rho = jnp.where(lowz, 1.0, jax.nn.sigmoid(z) / jnp.where(lowz, 1.0, dt))
    dz = Z[2 * T : 3 * T, :] * rho + D * arow[...] * jnp.where(lowz, dt, sz)
    ca_out[:, CI + 256 : CI + 384] = dz.astype(BF)
    hg_out[0:8, :] += colsum(D * a)
    hg_out[8:16, :] += colsum(dz)
    wtb = WT[...]
    dbs = DBC[:, :128] + mm(wtb.astype(BF), Cb)
    dcs = DBC[:, 128:] + mm(wtb.T.astype(BF), Bb)
    pres = jnp.concatenate([dbs, dcs], axis=1) * (ss * (1.0 + cs * (1.0 - ss)))
    ps[pl.ds(0, T), :] = pres
    dsv = pres * cws[3:4, :]
    ws_out[24:32, :] += colsum(pres * sbuf[pl.ds(8, T), :])
    ws_out[32:40, :] += colsum(pres)
    for k in range(1, 4):
        dsv = dsv + tile2(nbuf[k - 1], 2) * ps[pl.ds(k, T), :] * cws[3 - k : 4 - k, :]
        ws_out[24 - 8 * k : 32 - 8 * k, :] += colsum(pres * (tile2(mbuf[k - 1], 2) * sbuf[pl.ds(8 - k, T), :]))
    ca_out[:, CI : CI + 256] = dsv.astype(BF)


def scan_backward(proj, gate, segb, segr, ig, y, s_in, s2c, cfc, cw, cb, cws, cbs, sbias, arow, skip, gain, eye):
    L, CI = gate.shape
    heads = CI // PH
    hq = 4 if heads % 4 == 0 else 2
    nch = L // T
    blk = lambda w: pl.BlockSpec((T, w), lambda i: (nch - 1 - i, 0))
    part = lambda w, at: pl.BlockSpec((T, w), lambda i: (nch - 1 - i, at // w))
    tail = lambda w, at: pl.BlockSpec((8, w), lambda i: (jnp.maximum((nch - 1 - i) * (T // 8) - 1, 0), at // w))
    return pl.pallas_call(
        functools.partial(bwd_kernel, hq, heads // hq),
        grid=(nch,),
        in_specs=[blk(CI), tail(CI, 0), blk(CI), part(256, CI), tail(256, CI), part(128, CI + 256), blk(128), tail(128, 0),
                  full(segr.shape), blk(CI), blk(CI), pl.BlockSpec((1, 128, CI), lambda i: (nch - 1 - i, 0, 0)), blk(128), blk(128),
                  full(cw.shape), full(cb.shape), full(cws.shape), full(cbs.shape), full(sbias.shape), full(arow.shape),
                  full(skip.shape), full(gain.shape), full(eye.shape)],
        out_specs=[blk(CI), blk(CI + 384), full((56, CI)), full((40, 256)), full((16, 128))],
        out_shape=[jax.ShapeDtypeStruct((L, CI), BF), jax.ShapeDtypeStruct((L, CI + 384), BF),
                   jax.ShapeDtypeStruct((56, CI), F32), jax.ShapeDtypeStruct((40, 256), F32), jax.ShapeDtypeStruct((16, 128), F32)],
        scratch_shapes=[pltpu.VMEM((128, CI), F32), pltpu.VMEM((T + 8, CI), F32), pltpu.VMEM((T + 8, 256), F32),
                        pltpu.VMEM((T + 16, 128), F32), pltpu.VMEM((3, T, 128), F32), pltpu.VMEM((3, T, 128), F32),
                        pltpu.VMEM((T + 8, CI), F32), pltpu.VMEM((T + 8, 256), F32), pltpu.VMEM((128, T), F32),
                        pltpu.VMEM((3 * T + 8, 128), F32), pltpu.VMEM((T, T), F32), pltpu.VMEM((T, 256), F32)],
        compiler_params=pltpu.CompilerParams(dimension_semantics=("arbitrary",), vmem_limit_bytes=48 << 20),
        cost_estimate=pl.CostEstimate(flops=2 * L * CI * (4 * T + 768), bytes_accessed=L * CI * 24, transcendentals=L * CI * 8),
        name="scan_backward",
    )(proj, proj, gate, proj, proj, proj, segb, segb, segr, ig, y, s_in, s2c, cfc, cw, cb, cws, cbs, sbias, arow, skip, gain, eye)


EPS = 1e-05


class Plain:
    def gather_rows(self, h):
        rows = lax.all_gather(h, "head", axis=0, tiled=True)
        return lax.all_to_all(rows, "mp", split_axis=0, concat_axis=1, tiled=True)

    def scatter_rows(self, part):
        rows = lax.all_to_all(part, "mp", split_axis=1, concat_axis=0, tiled=True)
        return lax.psum_scatter(rows.astype(F32), "head", scatter_dimension=0, tiled=True)

    def gather_weight(self, w, axis):
        return lax.all_gather(w, "mp", axis=axis, tiled=True)

    def feature_order(self, v):
        return v

    def feature_place(self, v):
        return v

    def head_sum(self, v):
        return lax.psum(v, "head")

    def weight_sum(self, dw, axis):
        own = lax.psum_scatter(dw, "mp", scatter_dimension=axis, tiled=True)
        return lax.psum(own, "dp")

    def state_sum(self, dw):
        size = dw.shape[1] // lax.axis_size("head")
        return lax.psum_scatter(dw, "head", scatter_dimension=1, tiled=True)

    def total(self, v):
        return lax.psum(v, ("dp", "head", "mp"))


class Square:
    def __init__(self, sizes):
        self.dp, self.head, self.mp = sizes
        self.axes = ("dp", "head", "mp")
        self.x = lax.axis_index("mp") // 2
        self.c = lax.axis_index("mp") % 2
        self.y = lax.axis_index("head")
        self.z = lax.axis_index("dp")

    def perm(self, v, rule):
        pairs = []
        for z in range(self.dp):
            for y in range(2):
                for x in range(2):
                    for c in range(2):
                        to = rule(z, y, x, c)
                        if to is not None:
                            flat = lambda p: (p[0] * 2 + p[1]) * 4 + p[2] * 2 + p[3]
                            pairs.append((flat((z, y, x, c)), flat(to)))
        return lax.ppermute(v, self.axes, pairs)

    def core(self, v):
        return self.perm(v, lambda z, y, x, c: (z, y, x, 1 - c))

    def chip(self, v):
        return self.perm(v, lambda z, y, x, c: (z, y, 1 - x, c))

    def pair(self, v):
        return self.perm(v, lambda z, y, x, c: (z, 1 - y, x, c))

    def gather_rows(self, h):
        half = h.shape[0] // 2
        width = h.shape[1]
        mine = lax.dynamic_slice_in_dim(h, self.c * half, half, 0)
        other = self.core(lax.dynamic_slice_in_dim(h, (1 - self.c) * half, half, 0))
        both = jnp.concatenate([mine, other], axis=1)
        a = self.perm(both, lambda z, y, x, c: (z, y, 1 - x, c) if x != y else None)
        b = self.perm(both, lambda z, y, x, c: (z, 1 - y, x, c) if x == y else None)
        d = self.perm(both, lambda z, y, x, c: (z, 1 - y, x, c) if x != y else None)
        d = self.perm(d, lambda z, y, x, c: (z, y, 1 - x, c) if x == y else None)
        same = self.x == self.y
        near = jnp.where(same, both, b)
        far = jnp.where(same, a, d)
        return jnp.concatenate([near[:, :width], far[:, :width], near[:, width:], far[:, width:]], axis=1)

    def scatter_rows(self, part):
        width = part.shape[1] // 4
        near = jnp.concatenate([part[:, :width], part[:, 2 * width : 3 * width]], axis=1)
        far = jnp.concatenate([part[:, width : 2 * width], part[:, 3 * width :]], axis=1)
        a = self.perm(far, lambda z, y, x, c: (z, y, 1 - x, c) if x == y else None)
        b = self.perm(near, lambda z, y, x, c: (z, 1 - y, x, c) if x != y else None)
        d = self.perm(far, lambda z, y, x, c: (z, 1 - y, 1 - x, c) if x != y else None)
        same = self.x == self.y
        total = jnp.where(same, near, a).astype(F32) + jnp.where(same, b, d).astype(F32)
        own = total[:, :width]
        recv = self.core(total[:, width:])
        return jnp.concatenate([jnp.where(self.c == 0, own, recv), jnp.where(self.c == 0, recv, own)], axis=0)

    def gather_weight(self, w, axis):
        far = self.chip(w)
        other = self.core(w)
        last = self.core(far)
        return jnp.concatenate([w, far, other, last], axis=axis)

    def quarters(self):
        x, c = self.x, self.c
        return [x * 2 + c, (1 - x) * 2 + c, x * 2 + 1 - c, (1 - x) * 2 + 1 - c]

    def feature_order(self, v):
        width = v.shape[0] // 4
        return jnp.concatenate([lax.dynamic_slice_in_dim(v, q * width, width, 0) for q in self.quarters()])

    def feature_place(self, v):
        width = v.shape[0] // 4
        out = jnp.zeros_like(v)
        for i, q in enumerate(self.quarters()):
            out = lax.dynamic_update_slice_in_dim(out, v[i * width : (i + 1) * width], q * width, 0)
        return out

    def head_sum(self, v):
        return v + self.pair(v)

    def weight_sum(self, parts):
        keep0, keep1, send0, send1 = parts
        got1 = self.core(send1.astype(BF))
        got0 = self.core(send0.astype(BF))
        go = (keep1 + got1.astype(F32)).astype(BF)
        near = keep0 + got0.astype(F32)
        near = near + self.chip(go).astype(F32)
        n = self.dp
        rows = near.shape[0] // n
        low = near.astype(BF)
        own = lax.dynamic_slice_in_dim(near, self.z * rows, rows, 0)
        for r in range(1, n):
            piece = lax.dynamic_slice_in_dim(low, ((self.z + r) % n) * rows, rows, 0)
            own = own + self.perm(piece, lambda z, y, x, c: ((z + r) % n, y, x, c)).astype(F32)
        own = own.astype(BF)
        out = jnp.zeros((rows * n,) + near.shape[1:], BF)
        out = lax.dynamic_update_slice_in_dim(out, own, self.z * rows, 0)
        for r in range(1, n):
            piece = self.perm(own, lambda z, y, x, c: ((z + r) % n, y, x, c))
            out = lax.dynamic_update_slice_in_dim(out, piece, ((self.z - r) % n) * rows, 0)
        return out.astype(F32)

    def state_sum(self, dw):
        half = dw.shape[1] // 2
        own = lax.dynamic_slice_in_dim(dw, self.y * half, half, 1)
        return own + self.pair(lax.dynamic_slice_in_dim(dw, (1 - self.y) * half, half, 1))

    def total(self, v):
        v = v + self.core(v)
        v = v + self.chip(v)
        v = v + self.pair(v)
        step = 1
        while step < self.dp:
            v = v + self.perm(v, lambda z, y, x, c: (z ^ step, y, x, c))
            step *= 2
        return v


def shards(hidden, in_gain, proj_gate, proj_input, proj_state, proj_step, conv_input, bias_input, conv_state, bias_state,
           step_bias, decay_log, skip_gain, gate_gain, proj_out, segment_ids, cotangent):
    head_pos = lax.axis_index("head")
    sizes = (lax.axis_size("dp"), lax.axis_size("head"), lax.axis_size("mp"))
    square = sizes[1] == 2 and sizes[2] == 4 and (sizes[0] & (sizes[0] - 1)) == 0
    net = Square(sizes) if square else Plain()
    CI = proj_gate.shape[1]
    heads = proj_step.shape[1]
    head_dim = CI // heads
    D = in_gain.shape[0]
    HP = gate_gain.shape[0]
    L = segment_ids.shape[1]
    NST = proj_state.shape[1]
    wa = jnp.concatenate([proj_input, proj_state, jnp.pad(proj_step, ((0, 0), (0, 128 - heads)))], axis=1)

    if square:
        hid, wa = front_gather(hidden, wa, sizes[0])
    else:
        hid = net.gather_rows(hidden)
        wa = net.gather_weight(wa, 0)

    own_cols = lambda v: lax.dynamic_slice_in_dim(v, head_pos * CI, CI, v.ndim - 1)
    own_heads = lambda v: lax.dynamic_slice_in_dim(v, head_pos * heads, heads, 0)
    lanes = lambda v: jnp.pad(v[None], ((0, 0), (0, 128 - heads)))
    cw, cb = own_cols(conv_input), own_cols(bias_input)[None]
    gain2 = own_cols(gate_gain)[None]
    sbias = lanes(own_heads(step_bias))
    arow = lanes(-jnp.exp(own_heads(decay_log)))
    skip = jnp.repeat(own_heads(skip_gain), head_dim)[None]
    eye = (jnp.arange(CI)[:, None] // head_dim == jnp.arange(128)[None, :]).astype(BF)
    seg = segment_ids.astype(F32).reshape(L)
    segb = jnp.broadcast_to(seg[:, None], (L, 128))
    segr = seg.reshape(L // T, T)
    small = (cw, cb, conv_state, bias_state[None], sbias, arow, skip, gain2)

    gain1 = net.feature_order(in_gain)
    rows = hid.astype(F32)
    s1 = lax.rsqrt(jnp.mean(rows * rows, axis=1, keepdims=True) + EPS)
    normed = (rows * s1 * gain1).astype(BF)
    proj = jnp.dot(normed, wa, preferred_element_type=F32)
    if square:
        jn, s_in, cot, wg, wo = scan_forward(proj, segb, segr, *small, moves=(cotangent, proj_gate, proj_out), dp=sizes[0])
    else:
        jn, s_in = scan_forward(proj, segb, segr, *small)
        cot = net.gather_rows(cotangent)
        wg = net.gather_weight(proj_gate, 0)
        wo = net.gather_weight(proj_out, 1)
    gate, u, part, ss, dots = gate_and_out(normed, wg, jn, gain2, wo, cot)
    both = net.head_sum(jnp.stack([ss[:, 0], dots[:, 0]]))
    s2 = lax.rsqrt(both[0] / HP + EPS)
    coef = s2 * s2 * s2 * both[1] / HP
    ig = lax.dot_general(cot, wo, (((1,), (1,)), ((), ())), preferred_element_type=F32)
    s2c = jnp.broadcast_to(s2[:, None], (L, 128))
    cfc = jnp.broadcast_to(coef[:, None], (L, 128))
    block = net.scatter_rows((part * s2[:, None]).astype(BF))
    block_out = (hidden.astype(F32) + block).astype(BF)

    gg, ca, wgr, wsr, hgr = scan_backward(proj, gate, segb, segr, ig, jn, s_in, s2c, cfc, *small, eye)

    tn = lambda a, b: lax.dot_general(a, b, (((0,), (0,)), ((), ())), preferred_element_type=F32)
    nt = lambda a, b: lax.dot_general(a, b, (((1,), (1,)), ((), ())), preferred_element_type=F32)
    inner_out = (u.astype(F32) * s2[:, None]).astype(BF)
    if square:
        w4 = D // 4
        cut = lambda v: [v[:, i * w4 : (i + 1) * w4] for i in range(4)]
        dwo = net.weight_sum([tn(p, inner_out) for p in cut(cot)]).T
        dwg = net.weight_sum([tn(p, gg) for p in cut(normed)])
        dwa = net.weight_sum([tn(p, ca) for p in cut(normed)])
    else:
        dwo = net.weight_sum(tn(inner_out, cot), 1)
        dwg = net.weight_sum(tn(normed, gg), 0)
        dwa = net.weight_sum(tn(normed, ca), 0)
    dws = net.state_sum(dwa[:, CI : CI + NST])

    hpart, dgain1 = input_backward(gg, ca, wg, wa, hid, jnp.broadcast_to(s1, (L, 128)), gain1[None])
    hidden_grad = cotangent.astype(F32) + net.scatter_rows(hpart)

    wide = lambda v: lax.dynamic_update_slice_in_dim(jnp.zeros(v.shape[:-1] + (HP,), F32), v, head_pos * CI, v.ndim - 1)
    nheads = step_bias.shape[0]
    few = lambda v: lax.dynamic_update_slice_in_dim(jnp.zeros((nheads,), F32), v, head_pos * heads, 0)
    w7 = jnp.sum(wgr.reshape(7, 8, CI), axis=1)
    w5 = jnp.sum(wsr.reshape(5, 8, NST), axis=1)
    h2 = jnp.sum(hgr.reshape(2, 8, 128), axis=1)[:, :heads]
    dskip = jnp.sum(w7[5].reshape(heads, head_dim), axis=1)
    pack = [net.feature_place(jnp.sum(dgain1, axis=0)), wide(w7[0:4]), wide(w7[4]), w5[0:4], w5[4], few(h2[1]), few(h2[0]),
            few(dskip), wide(w7[6])]
    flat = jnp.concatenate([v.reshape(-1) for v in pack])
    fill = -flat.shape[0] % 1024
    flat = net.total(jnp.pad(flat, (0, fill)).reshape(-1, 128)).reshape(-1)
    outs = []
    at = 0
    for v in pack:
        outs.append(flat[at : at + v.size].reshape(v.shape))
        at += v.size
    return (block_out, hidden_grad, outs[0], dwg, dwa[:, :CI], dws, dwa[:, CI + NST : CI + NST + heads], outs[1], outs[2], outs[3],
            outs[4], outs[5], outs[6], outs[7], outs[8], dwo)


def solution(mesh):
    return jax.shard_map(
        shards,
        mesh=mesh,
        in_specs=(
            P(("dp", "head"), "mp"), P(), P("mp", "head"), P("mp", "head"), P("mp", None), P("mp", "head"), P(), P(), P(), P(),
            P(), P(), P(), P(), P("head", "mp"), P(("dp", "mp"), None), P(("dp", "head"), "mp"),
        ),
        out_specs=(
            P(("dp", "head"), "mp"), P(("dp", "head"), "mp"), P(), P("mp", "head"), P("mp", "head"), P("mp", "head"), P("mp", "head"),
            P(), P(), P(), P(), P(), P(), P(), P(), P("head", "mp"),
        ),
        check_vma=False,
    )
```

```python
import functools
import jax
import jax.numpy as jnp
from jax import lax
from jax.sharding import PartitionSpec as P
from jax.experimental import pallas as pl
from jax.experimental.pallas import tpu as pltpu

T = 128
PH = 64
NEG = -1e30
EPS = 1e-05
BF = jnp.bfloat16
F32 = jnp.float32


def mm(a, b):
    return jnp.dot(a, b, preferred_element_type=F32)


def mm_nt(a, b):
    return lax.dot_general(a, b, (((1,), (1,)), ((), ())), preferred_element_type=F32)


def mm_fine(a, b):
    ah, bh = a.astype(BF), b.astype(BF)
    al, bl = (a - ah.astype(F32)).astype(BF), (b - bh.astype(F32)).astype(BF)
    return mm(ah, bh) + mm(ah, bl) + mm(al, bh)


def sigm(v):
    return 0.5 * jnp.tanh(0.5 * v) + 0.5


def iota(shape, axis):
    return lax.broadcasted_iota(jnp.int32, shape, axis)


def prefix_sum(v):
    rows = iota(v.shape, 0)
    step = 1
    while step < v.shape[0]:
        v = v + jnp.where(rows >= step, pltpu.roll(v, step, 0), 0.0)
        step *= 2
    return v


def suffix_sum(v):
    size = v.shape[0]
    rows = iota(v.shape, 0)
    step = 1
    while step < size:
        v = v + jnp.where(rows < size - step, pltpu.roll(v, size - step, 0), 0.0)
        step *= 2
    return v


def step_values(z):
    dt = jnp.maximum(z, 0.0) + jnp.log1p(jnp.exp(-jnp.abs(z)))
    low = z < -15.0
    logdt = jnp.where(low, z, jnp.log(jnp.where(low, 1.0, dt)))
    return dt, logdt


def tile2(v, reps):
    return v if reps == 1 else jnp.concatenate([v] * reps, axis=1)


def per_pair(cols, width):
    lanes = iota((T, 128), 1)
    out = []
    for p in range(len(cols) // 2):
        out.append(jnp.where(lanes < PH, cols[2 * p], cols[2 * p + 1]))
    return out[0] if len(out) == 1 else jnp.concatenate(out, axis=1)


def block_diag(v):
    lanes = iota(v.shape, 1)
    zero = jnp.zeros_like(v)
    return jnp.concatenate([jnp.where(lanes < PH, v, zero), jnp.where(lanes >= PH, v, zero)], axis=0)


def head_cols(mat, group, hq):
    shift = lax.rem(128 - group * hq, 128)
    rolled = pltpu.roll(mat, shift, 1)
    return [jnp.broadcast_to(rolled[:, i : i + 1], (T, 128)) for i in range(hq)]


MESH = pl.DeviceIdType.MESH
ANY = pl.BlockSpec(memory_space=pl.ANY)
FWD_CHUNKS = 4


class Spot:
    def __init__(self, dp):
        self.dp = dp
        self.z = lax.axis_index("dp")
        self.y = lax.axis_index("head")
        m = lax.axis_index("mp")
        self.x = m // 2
        self.c = m % 2
        self.same = self.x == self.y

    def at(self, z, y, x, c):
        return (z, y, 2 * x + c)

    def core(self):
        return self.at(self.z, self.y, self.x, 1 - self.c)

    def meet(self):
        sem = pltpu.get_barrier_semaphore()
        peers = []
        for dy in range(2):
            for dx in range(2):
                for dc in range(2):
                    if dy + dx + dc:
                        peers.append((self.z, (self.y + dy) % 2, 2 * ((self.x + dx) % 2) + (self.c + dc) % 2))
        for r in range(1, self.dp):
            peers.append(((self.z + r) % self.dp, self.y, 2 * self.x + self.c))
        for p in peers:
            pl.semaphore_signal(sem, inc=1, device_id=p, device_id_type=MESH)
        pl.semaphore_wait(sem, len(peers))


def remote(src, dst, ss, rs, dev):
    return pltpu.make_async_remote_copy(src_ref=src, dst_ref=dst, send_sem=ss, recv_sem=rs, device_id=dev, device_id_type=MESH)


class RowsGather:
    def __init__(self, spot, src, dst, fbuf, bounce, ss, rs, ls):
        self.p, self.src, self.dst, self.fbuf, self.bounce, self.ss, self.rs, self.ls = spot, src, dst, fbuf, bounce, ss, rs, ls
        self.R = dst.shape[0]
        self.w = dst.shape[1] // 4
        self.n = self.R * 7 // 32 // 16 * 16
        self.far = self.n * FWD_CHUNKS

    def rows(self, t):
        return pl.ds(pl.multiple_of(t * self.R, 16), self.R)

    def cols(self, pos):
        return pl.ds(pl.multiple_of(pos * self.w, 128), self.w)

    def local_in(self):
        return pltpu.make_async_copy(self.src.at[self.rows(self.p.c), :], self.bounce, self.ls.at[0])

    def local_out(self):
        return pltpu.make_async_copy(self.bounce, self.dst.at[:, self.cols(0)], self.ls.at[1])

    def to_core(self):
        p = self.p
        return remote(self.src.at[self.rows(1 - p.c), :], self.dst.at[:, self.cols(2)], self.ss.at[0], self.rs.at[2], p.core())

    def to_y(self, t):
        p = self.p
        j = (p.c + t) % 2
        return remote(self.src.at[self.rows(t), :], self.dst.at[:, self.cols(2 * j)], self.ss.at[1 + t], self.rs.at[2 * j],
                      p.at(p.z, 1 - p.y, p.x, t))

    def to_x(self, t):
        p = self.p
        j = (p.c + t) % 2
        return remote(self.src.at[self.rows(t), :], self.dst.at[:, self.cols(2 * j + 1)], self.ss.at[t], self.rs.at[2 * j + 1],
                      p.at(p.z, p.y, 1 - p.x, t))

    def to_diag(self, t):
        p = self.p
        j = (p.c + t) % 2
        n = self.R - self.far
        return remote(self.src.at[pl.ds(pl.multiple_of(t * self.R + self.far, 16), n), :],
                      self.dst.at[pl.ds(self.far, n), self.cols(2 * j + 1)], self.ss.at[2 + t], self.rs.at[2 * j + 1],
                      p.at(p.z, 1 - p.y, 1 - p.x, t))

    def to_relay(self, k, t):
        p = self.p
        return remote(self.src.at[pl.ds(pl.multiple_of(t * self.R + k * self.n, 16), self.n), :],
                      self.fbuf.at[t, pl.ds(k * self.n, self.n), :], self.ss.at[4 + 2 * k + t], self.rs.at[4 + 2 * k + t],
                      p.at(p.z, 1 - p.y, p.x, p.c))

    def relay(self, k, t):
        p = self.p
        j = (p.c + t) % 2
        return remote(self.fbuf.at[t, pl.ds(k * self.n, self.n), :],
                      self.dst.at[pl.ds(k * self.n, self.n), self.cols(2 * j + 1)], self.ss.at[4 + 2 * k + t],
                      self.rs.at[4 + 2 * k + j], p.at(p.z, p.y, 1 - p.x, t))

    def start(self):
        @pl.when(self.p.same)
        def _():
            self.to_y(0).start()
            self.to_y(1).start()
            self.to_core().start()
            self.local_in().start()

        @pl.when(jnp.logical_not(self.p.same))
        def _():
            for k in range(FWD_CHUNKS):
                for t in range(2):
                    self.to_relay(k, t).start()
            for t in range(2):
                self.to_x(t).start()
            for t in range(2):
                self.to_diag(t).start()

    def forward(self, k):
        @pl.when(self.p.same)
        def _():
            if k == 0:
                self.local_in().wait()
                self.local_out().start()
            for t in range(2):
                self.to_relay(k, t).wait_recv()
                self.relay(k, t).start()

    def finish(self):
        @pl.when(self.p.same)
        def _():
            self.to_core().wait()
            for j in range(2):
                self.to_x_wait(j)
            for t in range(2):
                self.to_y(t).wait_send()
                for k in range(FWD_CHUNKS):
                    self.relay(k, t).wait_send()
            self.local_out().wait()

        @pl.when(jnp.logical_not(self.p.same))
        def _():
            for t in range(2):
                self.to_y(t).wait_recv()
                self.to_x(t).wait_send()
                self.to_diag(t).wait()
                for k in range(FWD_CHUNKS):
                    self.relay(k, t).wait_recv()
                    self.to_relay(k, t).wait_send()

    def to_x_wait(self, t):
        self.to_x(t).wait_recv()


class WeightGather:
    def __init__(self, spot, src, dst, axis, bounce, ss, rs, ls):
        self.p, self.src, self.dst, self.axis, self.bounce, self.ss, self.rs, self.ls = spot, src, dst, axis, bounce, ss, rs, ls
        self.n = src.shape[0] // spot.dp

    def chunk(self, k):
        return self.src.at[pl.ds(pl.multiple_of(k * self.n, 16), self.n), :]

    def slot(self, pos, k=None):
        size = self.src.shape[0]
        width = self.src.shape[1]
        if self.axis == 0:
            if k is None:
                return self.dst.at[pl.ds(pos * size, size), :]
            return self.dst.at[pl.ds(pl.multiple_of(pos * size + k * self.n, 16), self.n), :]
        cols = pl.ds(pos * width, width)
        if k is None:
            return self.dst.at[:, cols]
        return self.dst.at[pl.ds(pl.multiple_of(k * self.n, 16), self.n), cols]

    def to_x(self):
        p = self.p
        return remote(self.chunk(p.z), self.slot(1, p.z), self.ss.at[0], self.rs.at[0], p.at(p.z, p.y, 1 - p.x, p.c))

    def to_core(self):
        return remote(self.src, self.slot(2), self.ss.at[1], self.rs.at[1], self.p.core())

    def to_z(self, r):
        p = self.p
        return remote(self.slot(1, p.z), self.slot(1, p.z), self.ss.at[1 + r], self.rs.at[1 + r],
                      p.at((p.z + r) % p.dp, p.y, p.x, p.c))

    def across(self, r):
        p = self.p
        k = (p.z + p.dp - r) % p.dp
        return remote(self.slot(1, k), self.slot(3, k), self.ss.at[1 + p.dp + r], self.rs.at[1 + p.dp + r], p.core())

    def local_in(self):
        return pltpu.make_async_copy(self.src, self.bounce, self.ls.at[0])

    def local_out(self):
        return pltpu.make_async_copy(self.bounce, self.slot(0), self.ls.at[1])

    def start(self):
        self.to_x().start()
        self.to_core().start()
        self.local_in().start()

    def middle(self):
        self.to_x().wait_recv()
        for r in range(1, self.p.dp):
            self.to_z(r).start()
        self.across(0).start()
        self.local_in().wait()
        self.local_out().start()

    def spread(self):
        for r in range(1, self.p.dp):
            self.to_z(r).wait_recv()
            self.across(r).start()

    def finish(self):
        self.to_x().wait_send()
        self.to_core().wait()
        for r in range(1, self.p.dp):
            self.to_z(r).wait_send()
        for r in range(self.p.dp):
            self.across(r).wait()
        self.local_out().wait()


ROW_SEMS = 4 + 2 * FWD_CHUNKS


def rows_scratch(src):
    R, w = src.shape[0] // 2, src.shape[1]
    dma = pltpu.SemaphoreType.DMA
    return [pltpu.VMEM((2, R, w), BF), pltpu.VMEM((R, w), BF), dma((ROW_SEMS,)), dma((ROW_SEMS,)), dma((2,))]


def weight_scratch(src, dp):
    dma = pltpu.SemaphoreType.DMA
    return [pltpu.VMEM(src.shape, BF), dma((1 + 2 * dp,)), dma((1 + 2 * dp,)), dma((2,))]


def front_kernel(dp, h, wa, hid, waf, *scr):
    spot = Spot(dp)
    rg = RowsGather(spot, h, hid, *scr[:5])
    wg = WeightGather(spot, wa, waf, 0, *scr[5:])
    spot.meet()
    wg.start()
    rg.start()
    wg.middle()
    rg.forward(0)
    rg.forward(1)
    rg.forward(2)
    wg.spread()
    rg.forward(3)
    wg.finish()
    rg.finish()


def front_gather(h, wa, dp):
    R, w = h.shape[0] // 2, h.shape[1]
    return pl.pallas_call(
        functools.partial(front_kernel, dp),
        in_specs=[ANY, ANY],
        out_specs=[ANY, ANY],
        out_shape=[jax.ShapeDtypeStruct((R, 4 * w), BF), jax.ShapeDtypeStruct((4 * wa.shape[0], wa.shape[1]), BF)],
        scratch_shapes=rows_scratch(h) + weight_scratch(wa, dp),
        compiler_params=pltpu.CompilerParams(collective_id=1, has_side_effects=True, vmem_limit_bytes=16 << 20),
        name="front_gather",
    )(h, wa)


def fwd_kernel(hq, groups, dp, *refs):
    inp, st, stp, segb, segr, cw, cb, cws, cbs, sbias, arow, skip = refs[:12]
    if dp:
        cot, wg, wo = refs[12:15]
        j_out, s_out, cotf, wgf, wof = refs[15:20]
        S, vbuf, sbuf, gbuf, mbuf, cjt = refs[20:26]
        scr = refs[26:]
    else:
        j_out, s_out = refs[12:14]
        S, vbuf, sbuf, gbuf, mbuf, cjt = refs[14:20]
    c = pl.program_id(0)
    W = hq * PH
    reps = W // 128
    if dp:
        spot = Spot(dp)
        rg = RowsGather(spot, cot, cotf, *scr[:5])
        ga = WeightGather(spot, wg, wgf, 0, *scr[5:9])
        go = WeightGather(spot, wo, wof, 1, *scr[9:13])

        @pl.when(c == 0)
        def _():
            spot.meet()
            ga.start()
            go.start()
            rg.start()

        @pl.when(c == 2)
        def _():
            ga.middle()

        @pl.when(c == 3)
        def _():
            go.middle()
            rg.forward(0)

        @pl.when(c == 5)
        def _():
            rg.forward(1)
            rg.forward(2)

    @pl.when(c == 0)
    def _():
        S[...] = jnp.zeros_like(S)
        vbuf[pl.ds(0, 8), :] = jnp.zeros((8, vbuf.shape[1]), F32)
        sbuf[pl.ds(0, 8), :] = jnp.zeros((8, sbuf.shape[1]), F32)
        gbuf[pl.ds(0, 8), :] = jnp.full((8, 128), -1.0, F32)

    @pl.when(c > 0)
    def _():
        vbuf[pl.ds(0, 8), :] = vbuf[pl.ds(T, 8), :]
        sbuf[pl.ds(0, 8), :] = sbuf[pl.ds(T, 8), :]
        gbuf[pl.ds(0, 8), :] = gbuf[pl.ds(T, 8), :]

    vbuf[pl.ds(8, T), :] = inp[...]
    sbuf[pl.ds(8, T), :] = st[...]
    gbuf[pl.ds(8, T), :] = segb[...]
    seg = segb[...]
    for k in range(1, 4):
        mbuf[k - 1] = jnp.where(gbuf[pl.ds(8 - k, T), :] == seg, 1.0, 0.0)
    before = gbuf[pl.ds(7, 1), :]
    last = gbuf[pl.ds(T + 7, 1), :]
    cs = sbuf[pl.ds(8, T), :] * cws[3:4, :] + cbs[...]
    for k in range(1, 4):
        cs = cs + tile2(mbuf[k - 1], 2) * sbuf[pl.ds(8 - k, T), :] * cws[3 - k : 4 - k, :]
    ms = cs * sigm(cs)
    Bf = ms[:, :128]
    Bb = Bf.astype(BF)
    Cb = ms[:, 128:].astype(BF)
    Bt = Bf.T.astype(BF)
    G = mm_nt(Cb, Bb)
    dt, logdt = step_values(stp[...] + sbias[...])
    cum = prefix_sum(arow[...] * dt)
    cj = cum - logdt
    cjt[...] = cj.T
    rows = iota((T, T), 0)
    cols = iota((T, T), 1)
    segrow = segr[pl.ds(c, 1), :]
    maskb = jnp.where((seg == segrow) & (rows >= cols), 0.0, NEG)
    cont = tile2(jnp.where(seg == before, 1.0, 0.0), reps)
    trail = tile2(jnp.where(seg == last, 1.0, 0.0), reps)
    unbroken = tile2(jnp.where(last == before, 1.0, 0.0), reps)

    def body(q, carry):
        lane = pl.ds(pl.multiple_of(q * W, 128), W)
        cv = vbuf[pl.ds(8, T), lane] * cw[3:4, lane] + cb[:, lane]
        for k in range(1, 4):
            cv = cv + tile2(mbuf[k - 1], reps) * vbuf[pl.ds(8 - k, T), lane] * cw[3 - k : 4 - k, lane]
        x = cv * sigm(cv)
        xb = x.astype(BF)
        tcols = head_cols(cum, q, hq)
        jcols = head_cols(cj, q, hq)
        M = []
        for i in range(hq):
            row = cjt[pl.ds(q * hq + i, 1), :]
            M.append((jnp.exp(tcols[i] - row + maskb) * G).astype(BF))
        yin = []
        for p in range(hq // 2):
            yin.append(mm(jnp.concatenate(M[2 * p : 2 * p + 2], axis=1), block_diag(xb[:, 128 * p : 128 * p + 128])))
        yintra = yin[0] if len(yin) == 1 else jnp.concatenate(yin, axis=1)
        te = per_pair(tcols, W)
        tl = te[T - 1 : T, :]
        Sq = S[:, lane]
        Sb = Sq.astype(BF)
        yinter = mm(Cb, Sb) * (jnp.exp(te) * cont)
        s_out[0, :, lane] = Sb
        j_out[:, lane] = (yintra + yinter) + skip[:, lane] * x
        w = jnp.exp(tl - per_pair(jcols, W)) * trail
        wx = (x * w).astype(BF)
        S[:, lane] = Sq * (jnp.exp(tl) * unbroken) + mm(Bt, wx)
        return carry

    lax.fori_loop(0, groups, body, 0)
    if dp:
        @pl.when(c == pl.num_programs(0) - 1)
        def _():
            ga.spread()
            rg.forward(3)
            go.spread()
            ga.finish()
            go.finish()
            rg.finish()


def full(shape):
    return pl.BlockSpec(shape, lambda i: (0,) * len(shape))


def scan_forward(proj, segb, segr, cw, cb, cws, cbs, sbias, arow, skip, moves=None, dp=0):
    L = proj.shape[0]
    CI = proj.shape[1] - 384
    heads = CI // PH
    hq = 4 if heads % 4 == 0 else 2
    nch = L // T
    blk = lambda w: pl.BlockSpec((T, w), lambda i: (i, 0))
    part = lambda w, at: pl.BlockSpec((T, w), lambda i: (i, at // w))
    outs = [jax.ShapeDtypeStruct((L, CI), F32), jax.ShapeDtypeStruct((nch, 128, CI), BF)]
    out_specs = [blk(CI), pl.BlockSpec((1, 128, CI), lambda i: (i, 0, 0))]
    scratch = [pltpu.VMEM((128, CI), F32), pltpu.VMEM((T + 8, CI), F32), pltpu.VMEM((T + 8, 256), F32),
               pltpu.VMEM((T + 8, 128), F32), pltpu.VMEM((3, T, 128), F32), pltpu.VMEM((128, T), F32)]
    extra = {}
    ins = []
    if dp:
        cot, wg, wo = ins = list(moves)
        outs += [jax.ShapeDtypeStruct((cot.shape[0] // 2, 4 * cot.shape[1]), BF), jax.ShapeDtypeStruct((4 * wg.shape[0], wg.shape[1]), BF),
                 jax.ShapeDtypeStruct((wo.shape[0], 4 * wo.shape[1]), BF)]
        scratch += rows_scratch(cot) + weight_scratch(wg, dp) + weight_scratch(wo, dp)
        extra = dict(collective_id=2, has_side_effects=True)
    return pl.pallas_call(
        functools.partial(fwd_kernel, hq, heads // hq, dp),
        grid=(nch,),
        in_specs=[blk(CI), part(256, CI), part(128, CI + 256), blk(128), full(segr.shape), full(cw.shape), full(cb.shape),
                  full(cws.shape), full(cbs.shape), full(sbias.shape), full(arow.shape), full(skip.shape)] + [ANY] * len(ins),
        out_specs=out_specs + [ANY] * len(ins),
        out_shape=outs,
        scratch_shapes=scratch,
        compiler_params=pltpu.CompilerParams(dimension_semantics=("arbitrary",), vmem_limit_bytes=40 << 20, **extra),
        cost_estimate=pl.CostEstimate(flops=2 * L * CI * (2 * T + 256), bytes_accessed=L * CI * 12, transcendentals=L * CI * 6),
        name="scan_forward",
    )(proj, proj, proj, segb, segr, cw, cb, cws, cbs, sbias, arow, skip, *ins)


NB = 256
MB = 512
OR = 256


class RowsScatter:
    def __init__(self, spot, dst, nb, ss, rs, ls):
        self.p, self.dst, self.nb, self.ss, self.rs, self.ls = spot, dst, nb, ss, rs, ls
        self.R = dst.shape[1] // 2
        self.w = dst.shape[2]
        self.n = self.R // nb

    def slot(self, y, seq, k):
        return self.dst.at[y, pl.ds(pl.multiple_of(seq * self.R + k * self.n, 16), self.n), :]

    def send(self, buf, k, i, j):
        p = self.p
        src = buf.at[:, pl.ds((2 * j + i) * self.w, self.w)]
        dev = p.at(p.z, p.x, (p.x + i) % 2, (p.c + j) % 2)
        return remote(src, self.slot(p.y, p.c, k), self.ss.at[2 * j + i, k], self.rs.at[p.y, p.c, k], dev)

    def keep(self, buf, k):
        p = self.p
        return pltpu.make_async_copy(buf.at[:, pl.ds(0, self.w)], self.slot(p.y, p.c, k), self.ls.at[k])

    def start(self, buf, k):
        for i, j in ((1, 0), (1, 1), (0, 1)):
            self.send(buf, k, i, j).start()

        @pl.when(self.p.same)
        def _():
            self.keep(buf, k).start()

        @pl.when(jnp.logical_not(self.p.same))
        def _():
            self.send(buf, k, 0, 0).start()

    def sent(self, buf, k):
        for i, j in ((1, 0), (1, 1), (0, 1)):
            self.send(buf, k, i, j).wait_send()

        @pl.when(self.p.same)
        def _():
            self.keep(buf, k).wait()

        @pl.when(jnp.logical_not(self.p.same))
        def _():
            self.send(buf, k, 0, 0).wait_send()

    def got(self, k):
        p = self.p
        for y in range(2):
            for q in range(2):
                own = p.same & (p.y == y) & (p.c == q)

                @pl.when(jnp.logical_not(own))
                def _():
                    v = self.slot(y, q, k)
                    remote(v, v, self.ss.at[0, k], self.rs.at[y, q, k], p.core()).wait_recv()


def scatter_sems(nb):
    dma = pltpu.SemaphoreType.DMA
    return [dma((4, nb)), dma((2, 2, nb)), dma((nb,))]


def mid_kernel(dp, nb, HP, nrm, jn, jb, wg, wo, cot, gain, gg_out, g_out, io_out, p_out, gn_out,
               gbuf, pbuf, ub, ib, ss, ex, rx, acc, es, er):
    i = pl.program_id(0)
    CI = jn.shape[1]
    D = cot.shape[1]
    spot = Spot(dp)
    par = i % 2
    old = (i + 1) % 2
    acc[...] = jnp.zeros_like(acc)
    lanes = iota((OR, 128), 1)

    def swap(k):
        dev = spot.at(spot.z, 1 - spot.y, spot.x, spot.c)
        return remote(ex.at[k % 2], rx.at[k % 2], es.at[k % 2], er.at[k % 2], dev)

    @pl.when(i == 0)
    def _():
        gn_out[...] = jnp.zeros_like(gn_out)
        spot.meet()

    for q in range(nb):
        @pl.when(i == q + 1)
        def _():
            swap(q).start()

    @pl.when(i < nb)
    def _():
        def one(n, carry):
            lane = pl.ds(pl.multiple_of(n * MB, MB), MB)
            gt = mm(nrm[...], wg[:, lane])
            gbuf[par, :, lane] = gt
            gated = jn[:, lane] * (gt * sigm(gt))
            ub[:, lane] = (gated * gain[:, lane]).astype(BF)
            sq = gated * gated
            for p in range(MB // 128):
                acc[0] += sq[:, 128 * p : 128 * p + 128]
            return carry

        lax.fori_loop(0, CI // MB, one, 0)

        def two(n, carry):
            lane = pl.ds(pl.multiple_of(n * MB, MB), MB)
            pv = mm(ub[...], wo[:, lane])
            pbuf[par, :, lane] = pv
            d = pv * cot[pl.ds(pl.multiple_of(i * OR, OR), OR), lane].astype(F32)
            for p in range(MB // 128):
                acc[1] += d[:, 128 * p : 128 * p + 128]
            return carry

        lax.fori_loop(0, D // MB, two, 0)
        s_sum = jnp.sum(acc[0], axis=1, keepdims=True)
        d_sum = jnp.sum(acc[1], axis=1, keepdims=True)
        both = jnp.where(lanes == 0, s_sum, d_sum)
        ss[par] = both
        ex[par] = both.T[0:8, :]

    @pl.when(i > 0)
    def _():
        k = i - 1

        def three(n, carry):
            lane = pl.ds(pl.multiple_of(n * MB, MB), MB)
            ib[:, lane] = mm_nt(cot[pl.ds(pl.multiple_of(k * OR, OR), OR), :], wo[lane, :])
            return carry

        lax.fori_loop(0, CI // MB, three, 0)
        for q in range(nb):
            @pl.when(k == q)
            def _():
                swap(q).wait()
        theirs = jnp.concatenate([rx[old], jnp.zeros((120, OR), F32)], axis=0).T
        tot = ss[old] + theirs
        s2 = lax.rsqrt(jnp.broadcast_to(tot[:, 0:1], (OR, 128)) / HP + EPS)
        cf = s2 * s2 * s2 * (jnp.broadcast_to(tot[:, 1:2], (OR, 128)) / HP)
        s2w = tile2(s2, MB // 128)
        cfw = tile2(cf, MB // 128)

        def scale(n, carry):
            lane = pl.ds(pl.multiple_of(n * MB, MB), MB)
            p_out[:, lane] = (pbuf[old, :, lane] * s2w).astype(BF)
            return carry

        lax.fori_loop(0, D // MB, scale, 0)

        def four(n, carry):
            lane = pl.ds(pl.multiple_of(n * MB, MB), MB)
            gt = gbuf[old, :, lane]
            joined = jb[:, lane]
            sg = sigm(gt)
            sl = gt * sg
            gated = joined * sl
            gis = ib[:, lane] * s2w
            gv = gis * gain[:, lane] - gated * cfw
            gg_out[:, lane] = (gv * joined * (sg * (1.0 + gt * (1.0 - sg)))).astype(BF)
            g_out[:, lane] = (gv * sl).astype(BF)
            io_out[:, lane] = (gated * s2w * gain[:, lane]).astype(BF)
            gn_out[:, lane] += sum8(gis * gated)
            return carry

        lax.fori_loop(0, CI // MB, four, 0)


def gate_and_out(nrm, jn, wg, wo, cot, gain, HP, dp):
    L, D = nrm.shape
    CI = wg.shape[1]
    nb = L // OR
    now = lambda w: pl.BlockSpec((OR, w), lambda i: (jnp.minimum(i, nb - 1), 0))
    back = lambda w: pl.BlockSpec((OR, w), lambda i: (jnp.maximum(i - 1, 0), 0))
    once = lambda shape: pl.BlockSpec(shape, lambda i: (0, 0), pipeline_mode=pl.Buffered(1))
    dma = pltpu.SemaphoreType.DMA
    return pl.pallas_call(
        functools.partial(mid_kernel, dp, nb, HP),
        grid=(nb + 1,),
        in_specs=[now(D), now(CI), back(CI), once(wg.shape), once(wo.shape), once(cot.shape), full(gain.shape)],
        out_specs=[back(CI), back(CI), back(CI), back(D), full((8, CI))],
        out_shape=[jax.ShapeDtypeStruct((L, CI), BF), jax.ShapeDtypeStruct((L, CI), BF), jax.ShapeDtypeStruct((L, CI), BF),
                   jax.ShapeDtypeStruct((L, D), BF), jax.ShapeDtypeStruct((8, CI), F32)],
        scratch_shapes=[pltpu.VMEM((2, OR, CI), F32), pltpu.VMEM((2, OR, D), F32), pltpu.VMEM((OR, CI), BF), pltpu.VMEM((OR, CI), F32),
                        pltpu.VMEM((2, OR, 128), F32), pltpu.VMEM((2, 8, OR), F32), pltpu.VMEM((2, 8, OR), F32),
                        pltpu.VMEM((2, OR, 128), F32), dma((2,)), dma((2,))],
        compiler_params=pltpu.CompilerParams(dimension_semantics=("arbitrary",), vmem_limit_bytes=48 << 20, collective_id=3,
                                             has_side_effects=True),
        cost_estimate=pl.CostEstimate(flops=6 * L * CI * D, bytes_accessed=L * D * 22 + CI * D * 4, transcendentals=L * CI),
        name="gate_and_out",
    )(nrm, jn, jn, wg, wo, cot, gain)


def mm_tn(a, b):
    return lax.dot_general(a, b, (((0,), (0,)), ((), ())), preferred_element_type=F32)


LINE = 4


class LineSum:
    def __init__(self, spot, own, fin, obuf, ibuf, tbuf, pbuf, ss, rs):
        self.p, self.own, self.fin, self.obuf, self.ibuf, self.tbuf, self.pbuf, self.ss, self.rs = spot, own, fin, obuf, ibuf, tbuf, pbuf, ss, rs
        self.n = own.shape[0] // (2 * LINE)
        self.C = own.shape[1]
        z = spot.z
        self.mid = (z == 1) | (z == 2)
        self.out = jnp.logical_not(self.mid)
        self.inner = jnp.where(z == 0, 1, jnp.where(z == 3, 2, 3 - z))
        self.outer = jnp.where(z == 1, 0, 3)
        self.hm = jnp.where(z == 1, 0, 1)

    def rows(self, ref, h, k):
        return ref.at[pl.ds(pl.multiple_of((h * LINE + k) * self.n, 16), self.n), :]

    def to(self, z):
        return self.p.at(z, self.p.y, self.p.x, self.p.c)

    def up(self, h, k):
        return remote(self.rows(self.own, h, k), self.rows(self.obuf, h, k), self.ss.at[h * LINE + k], self.rs.at[h * LINE + k],
                      self.to(self.inner))

    def across(self, k):
        v = pl.ds(k * self.n, self.n)
        return remote(self.tbuf.at[v, :], self.ibuf.at[v, :], self.ss.at[2 * LINE + k], self.rs.at[2 * LINE + k], self.to(self.inner))

    def down(self, h, k, which):
        v = self.rows(self.fin, h, k)
        dest = self.to(self.outer) if which == 0 else self.to(self.inner)
        return remote(v, v, self.ss.at[(3 + which) * LINE + k], self.rs.at[3 * LINE + h * LINE + k], dest)

    def pass_on(self, k):
        h = 1 - self.hm
        v = self.rows(self.fin, h, k)
        return remote(v, v, self.ss.at[5 * LINE + k], self.rs.at[3 * LINE + h * LINE + k], self.to(self.outer))

    def start(self, k):
        @pl.when(self.out)
        def _():
            self.up(0, k).start()
            self.up(1, k).start()

    def chunked(self, body):
        step = 384 if self.C % 384 == 0 else 128

        def one(n, carry):
            body(pl.ds(pl.multiple_of(n * step, 128), step))
            return carry

        lax.fori_loop(0, self.C // step, one, 0)

    def gather(self, k):
        @pl.when(self.mid)
        def _():
            ho = 1 - self.hm
            self.up(ho, k).wait_recv()
            v = pl.ds(k * self.n, self.n)
            a = pl.ds(pl.multiple_of((ho * LINE + k) * self.n, 16), self.n)
            b = pl.ds(pl.multiple_of((self.hm * LINE + k) * self.n, 16), self.n)

            def theirs(lane):
                self.tbuf[v, lane] = (self.own[a, lane].astype(F32) + self.obuf[a, lane].astype(F32)).astype(BF)

            def mine(lane):
                self.pbuf[v, lane] = self.own[b, lane].astype(F32) + self.obuf[b, lane].astype(F32)

            self.chunked(theirs)
            self.up(self.hm, k).wait_recv()
            self.chunked(mine)
            self.across(k).start()

    def close(self, k):
        @pl.when(self.mid)
        def _():
            self.across(k).wait_recv()
            v = pl.ds(k * self.n, self.n)
            b = pl.ds(pl.multiple_of((self.hm * LINE + k) * self.n, 16), self.n)

            def final(lane):
                self.fin[b, lane] = (self.pbuf[v, lane] + self.ibuf[v, lane].astype(F32)).astype(BF)

            self.chunked(final)

    def back(self, k):
        @pl.when(self.mid)
        def _():
            self.down(self.hm, k, 0).start()
            self.down(self.hm, k, 1).start()

    def relay(self, k):
        @pl.when(self.mid)
        def _():
            self.pass_on(k).wait_recv()
            self.pass_on(k).start()

    def stages(self):
        calls = []
        for k in range(LINE + 2):
            if k < LINE:
                calls.append((k, functools.partial(self.gather, k)))
            if 0 <= k - 1 < LINE:
                calls.append((k, functools.partial(self.close, k - 1)))
            if 0 <= k - 2 < LINE:
                calls.append((k, functools.partial(self.relay, k - 2)))
            if 0 <= k - 1 < LINE:
                calls.append((k, functools.partial(self.back, k - 1)))
        return calls

    def finish(self):
        @pl.when(self.mid)
        def _():
            for k in range(LINE):
                self.across(k).wait_send()
                self.down(self.hm, k, 0).wait_send()
                self.down(self.hm, k, 1).wait_send()
                self.pass_on(k).wait_send()

        @pl.when(self.out)
        def _():
            for k in range(LINE):
                for h in range(2):
                    self.up(h, k).wait_send()
                    self.down(h, k, 0).wait_recv()


def line_scratch(rows, C):
    dma = pltpu.SemaphoreType.DMA
    h = rows // 2
    return [pltpu.VMEM((rows, C), BF), pltpu.VMEM((rows, C), BF), pltpu.VMEM((h, C), BF), pltpu.VMEM((h, C), BF),
            pltpu.VMEM((h, C), F32), dma((6 * LINE,)), dma((5 * LINE,))]


def columns(ref, body, step=128):
    def one(n, carry):
        body(pl.ds(pl.multiple_of(n * step, 128), step))
        return carry

    lax.fori_loop(0, ref.shape[1] // step, one, 0)


def pair_kernel(dp, cot, io, nrm, gg, p_in, f_out, s0g, s1g, rec, give, got, own, s1o, ro, vs, vr, xs, xr, *sems):
    spot = Spot(dp)
    sc = RowsScatter(spot, rec, 1, *sems)
    first = p_in.at[pl.ds(0, rec.shape[1] // 2), :]
    w = cot.shape[1] // 4
    C = io.shape[1]
    spot.meet()
    sc.start(first, 0)
    work = ((cot, io), (nrm, gg))

    def swap(m, b):
        rows = pl.ds(b * w, w)
        return remote(give.at[m, rows, :], got.at[m, rows, :], vs.at[m, b], vr.at[m, b], spot.core())

    def over():
        return remote(s1o, ro, xs, xr, spot.at(spot.z, spot.y, 1 - spot.x, spot.c))

    def theirs(m, b):
        a, r = work[m]

        def tile(lane):
            give[m, b * w : b * w + w, lane] = mm_tn(a[:, (2 + b) * w : (3 + b) * w], r[:, lane]).astype(BF)

        columns(r, tile, MB)

    def mine(m, b):
        a, r = work[m]

        def tile(lane):
            own[b, :, lane] = mm_tn(a[:, b * w : b * w + w], r[:, lane])

        columns(r, tile, MB)

    def joined(m, b, dst):
        swap(m, b).wait()

        def tile(lane):
            dst[:, lane] = (own[b, :, lane] + got[m, b * w : b * w + w, lane].astype(F32)).astype(dst.dtype)

        columns(dst, tile)

    theirs(0, 1)
    theirs(0, 0)
    swap(0, 1).start()
    mine(0, 1)
    swap(0, 0).start()
    joined(0, 1, s1o)
    mine(0, 0)
    over().start()
    theirs(1, 0)
    joined(0, 0, own.at[0])
    theirs(1, 1)
    swap(1, 0).start()
    mine(1, 1)
    swap(1, 1).start()
    joined(1, 1, s1g)
    over().wait()

    def total(lane):
        f_out[:, lane] = (own[0, :, lane] + ro[:, lane].astype(F32)).astype(BF)

    columns(f_out, total)
    mine(1, 0)
    joined(1, 0, s0g)
    sc.sent(first, 0)
    sc.got(0)


def pair_grads(cot, io, nrm, gg, p_in, rows, dp):
    L, D = cot.shape
    C = io.shape[1]
    w = D // 4
    dma = pltpu.SemaphoreType.DMA
    vm = pl.BlockSpec(memory_space=pltpu.VMEM)
    return pl.pallas_call(
        functools.partial(pair_kernel, dp),
        in_specs=[vm, vm, vm, vm, ANY],
        out_specs=[vm, vm, vm, ANY],
        out_shape=[jax.ShapeDtypeStruct((w, C), BF), jax.ShapeDtypeStruct((w, C), F32),
                   jax.ShapeDtypeStruct((w, C), BF), jax.ShapeDtypeStruct((2, 2 * rows, w), BF)],
        scratch_shapes=[pltpu.VMEM((2, 2 * w, C), BF), pltpu.VMEM((2, 2 * w, C), BF), pltpu.VMEM((2, w, C), F32),
                        pltpu.VMEM((w, C), BF), pltpu.VMEM((w, C), BF), dma((2, 2)), dma((2, 2)), dma, dma] + scatter_sems(1),
        compiler_params=pltpu.CompilerParams(vmem_limit_bytes=56 << 20, collective_id=4, has_side_effects=True),
        cost_estimate=pl.CostEstimate(flops=4 * L * C * D, bytes_accessed=L * D * 8 + C * w * 12, transcendentals=0),
        name="pair_grads",
    )(cot, io, nrm, gg, p_in)


def tail_kernel(dp, nb, gg, hid, s1, ca, nrm, fgs, gain, vec, wg_any, wa_any, dwg, dwi, dws, dwt, rec, tot,
                wgv, wav, give, got, own, s1a, ra, fa, ng, hp, igs, vb, vr, sth, ws, vs, vq, xs, xr, bs, br, ys, yr, os, *rest):
    i = pl.program_id(0)
    D = gain.shape[1]
    w = D // 4
    C = ca.shape[1]
    CI = C - 384
    spot = Spot(dp)
    lg = LineSum(spot, fgs, *rest[:7])
    la = LineSum(spot, fa, *rest[7:14])
    sc = RowsScatter(spot, rec, nb, *rest[14:])
    OR = gg.shape[0]
    wide = 640 if C % 640 == 0 else 384
    nv = vec.shape[0]

    def weights():
        return (pltpu.make_async_copy(wg_any, wgv, ws.at[0]), pltpu.make_async_copy(wa_any, wav, ws.at[1]))

    def swap(b):
        rows = pl.ds(b * w, w)
        return remote(give.at[rows, :], got.at[rows, :], vs.at[b], vq.at[b], spot.core())

    def over(h, k):
        rows = pl.ds((h * LINE + k) * la.n, la.n)
        return remote(s1a.at[rows, :], ra.at[rows, :], xs.at[h * LINE + k], xr.at[h * LINE + k],
                      spot.at(spot.z, spot.y, 1 - spot.x, spot.c))

    def theirs(b):
        def tile(lane):
            give[b * w : b * w + w, lane] = mm_tn(nrm[:, (2 + b) * w : (3 + b) * w], ca[:, lane]).astype(BF)

        columns(ca, tile, wide)

    def mine(b):
        def tile(lane):
            own[b, :, lane] = mm_tn(nrm[:, b * w : b * w + w], ca[:, lane])

        columns(ca, tile, wide)

    def joined(b, dst):
        swap(b).wait()

        def tile(lane):
            dst[:, lane] = (own[b, :, lane] + got[b * w : b * w + w, lane].astype(F32)).astype(dst.dtype)

        columns(ca, tile)

    def arrive(k):
        for h in range(2):
            over(h, k).wait_recv()
            rows = pl.ds((h * LINE + k) * la.n, la.n)

            def tile(lane):
                fa[rows, lane] = (own[0, rows, lane] + ra[rows, lane].astype(F32)).astype(BF)

            columns(ca, tile, 384)

    def mix(s):
        z = spot.z
        near = [spot.core(), spot.at(z + 1 - 2 * (z % 2), spot.y, spot.x, spot.c), spot.at((z + 2) % 4, spot.y, spot.x, spot.c),
                spot.at(z, 1 - spot.y, spot.x, spot.c), spot.at(z, spot.y, 1 - spot.x, spot.c)]
        return remote(vb.at[s], vr.at[s], bs.at[s], br.at[s], near[s])

    def mixed(s):
        mix(s).wait()
        v = vb[s] + vr[s]
        if s < 4:
            vb[s + 1] = v
        else:
            tot[...] = v

    def stage(line, k):
        for at, call in line.stages():
            if at == k:
                call()

    @pl.when(i == 0)
    def _():
        for cp in weights():
            cp.start()
        igs[...] = jnp.zeros_like(igs)
        spot.meet()
        for k in range(LINE):
            lg.start(k)
        theirs(1)
        theirs(0)
        swap(1).start()
        mine(1)
        swap(0).start()
        joined(1, s1a)
        mine(0)
        for k in range(LINE):
            for h in range(2):
                over(h, k).start()
        joined(0, own.at[0])
        for cp in weights():
            cp.wait()

    @pl.when(i > 0)
    def _():
        def one(n, srow):
            lane = pl.ds(pl.multiple_of(n * NB, NB), NB)
            v = mm_nt(gg[...], wgv[lane, :]) + mm_nt(ca[pl.ds(pl.multiple_of((i - 1) * OR, OR), OR), :], wav[lane, :])
            rows = hid[:, lane].astype(F32)
            sv = tile2(s1[...], NB // 128)
            t = v * rows
            igs[:, lane] += sum8(t * sv)
            v = v * gain[:, lane]
            ng[:, lane] = v
            t = v * rows
            for p in range(NB // 128):
                srow = srow + t[:, 128 * p : 128 * p + 128]
            return srow

        srow = lax.fori_loop(0, D // NB, one, jnp.zeros((OR, 128), F32))
        scale = s1[...]
        coef = scale * scale * scale * (jnp.sum(srow, axis=1, keepdims=True) / D)
        block = pl.ds(pl.multiple_of((i - 1) * OR, OR), OR)

        def two(lane):
            hp[block, lane] = (ng[:, lane] * scale - hid[:, lane].astype(F32) * coef).astype(BF)

        columns(ng, two)

    def part(k):
        return hp.at[pl.ds(k * OR, OR), :]

    for q in range(1, nb + 1):
        @pl.when(i == q)
        def _():
            if q >= 2:
                sc.start(part(q - 2), q - 2)
            if q <= LINE:
                stage(lg, q - 1)
            if q == nb - 1:
                arrive(0)
            if q == nb:
                la.start(0)

    @pl.when(i == nb)
    def _():
        x, c = spot.x, spot.c
        vb[0] = vec[...]
        ig = jnp.sum(igs[...], axis=0, keepdims=True)
        place = [x * 2 + c, (1 - x) * 2 + c, x * 2 + 1 - c, (1 - x) * 2 + 1 - c]
        for p in range(4):
            for t in range(w // 128):
                at = p * w + t * 128
                vb[0, pl.ds(place[p] * (w // 128) + t, 1), :] = ig[:, at : at + 128]
        stage(lg, LINE)
        mix(0).start()
        sc.start(part(nb - 1), nb - 1)
        arrive(1)
        stage(lg, LINE + 1)
        mixed(0)
        la.start(1)
        stage(la, 0)
        mix(1).start()
        arrive(2)
        mixed(1)
        la.start(2)
        stage(la, 1)
        mix(2).start()
        arrive(3)
        mixed(2)
        la.start(3)
        stage(la, 2)
        mix(3).start()
        stage(la, 3)
        mixed(3)
        stage(la, 4)
        mix(4).start()
        lg.finish()

        def wide_g(lane):
            own[1, :, lane] = lg.fin[:, lane].astype(F32)

        columns(dwg, wide_g)
        stage(la, 5)
        out_g = pltpu.make_async_copy(own.at[1, :, pl.ds(0, CI)], dwg, os.at[0])
        out_g.start()
        la.finish()
        give_half = la.fin.at[:, pl.ds(pl.multiple_of(CI + (1 - spot.y) * 128, 128), 128)]
        state = remote(give_half, sth, ys, yr, spot.at(spot.z, 1 - spot.y, spot.x, spot.c))
        state.start()

        def wide_a(lane):
            own[0, :, lane] = la.fin[:, lane].astype(F32)

        columns(dwi, wide_a)
        out_i = pltpu.make_async_copy(own.at[0, :, pl.ds(0, CI)], dwi, os.at[1])
        out_i.start()
        dwt[...] = la.fin[:, CI + 256 : C].astype(F32)
        mixed(4)
        state.wait()
        dws[...] = la.fin[:, pl.ds(pl.multiple_of(CI + spot.y * 128, 128), 128)].astype(F32) + sth[...].astype(F32)
        out_g.wait()
        out_i.wait()
        for k in range(LINE):
            for h in range(2):
                over(h, k).wait_send()
        for q in range(nb):
            sc.sent(part(q), q)
            sc.got(q)


def tail(gg, ca, wg, wa, nrm, hid, s1c, gain, f_g, vec, dp):
    L, D = hid.shape
    CI = gg.shape[1]
    C = ca.shape[1]
    w = D // 4
    R = 256
    nb = L // R
    back = lambda v: pl.BlockSpec((R, v), lambda i: (jnp.maximum(i - 1, 0), 0))
    once = lambda v: pl.BlockSpec(v.shape, lambda i: (0,) * v.ndim, pipeline_mode=pl.Buffered(1))
    dma = pltpu.SemaphoreType.DMA
    like = lambda shape, t: jax.ShapeDtypeStruct(shape, t)
    shapes = [like((w, CI), F32), like((w, CI), F32), like((w, 128), F32), like((w, 128), F32), like((2, 2 * L, w), BF),
              like(vec.shape, F32)]
    return pl.pallas_call(
        functools.partial(tail_kernel, dp, nb),
        grid=(nb + 1,),
        in_specs=[back(CI), back(D), back(128), once(ca), once(nrm), once(f_g), once(gain), once(vec), ANY, ANY],
        out_specs=[ANY, ANY, full((w, 128)), full((w, 128)), ANY, full(vec.shape)],
        out_shape=shapes,
        scratch_shapes=[pltpu.VMEM(wg.shape, BF), pltpu.VMEM(wa.shape, BF), pltpu.VMEM((2 * w, C), BF), pltpu.VMEM((2 * w, C), BF),
                        pltpu.VMEM((2, w, C), F32), pltpu.VMEM((w, C), BF), pltpu.VMEM((w, C), BF), pltpu.VMEM((w, C), BF),
                        pltpu.VMEM((R, D), F32), pltpu.VMEM((L, D), BF), pltpu.VMEM((8, D), F32),
                        pltpu.VMEM((5,) + vec.shape, F32), pltpu.VMEM((5,) + vec.shape, F32), pltpu.VMEM((w, 128), BF),
                        dma((2,)), dma((2,)), dma((2,)), dma((2 * LINE,)), dma((2 * LINE,)), dma((5,)), dma((5,)), dma, dma, dma((2,))]
        + line_scratch(w, CI) + line_scratch(w, C) + scatter_sems(nb),
        compiler_params=pltpu.CompilerParams(dimension_semantics=("arbitrary",), vmem_limit_bytes=62 << 20, collective_id=6,
                                             has_side_effects=True),
        cost_estimate=pl.CostEstimate(flops=2 * L * D * (CI + 2 * C), bytes_accessed=L * D * 12 + D * D * 4, transcendentals=0),
        name="tail",
    )(gg, hid, s1c, ca, nrm, f_g, gain, vec, wg, wa)


def sum8(v):
    acc = v[0:8]
    for r in range(1, v.shape[0] // 8):
        acc = acc + v[8 * r : 8 * r + 8]
    return acc


def bwd_kernel(hq, groups, dp, *refs):
    inp, inp8, st, st8, stp, segb, segb8, segr, g_in, y, s_in, cw, cb, cws, cbs, sbias, arow, skip, eye = refs[:19]
    refs = refs[19:]
    if dp:
        f_o, s0g, s1g, p_in = refs[:4]
        refs = refs[4:]
    ca_out, wg_out, ws_out, hg_out = refs[:4]
    refs = refs[4:]
    if dp:
        d_out, f_g, rec = refs[:3]
        refs = refs[3:]
    dS, vbuf, sbuf, gbuf, mbuf, nbuf, pg, ps, cmt, Z, WT, DBC = refs[:12]
    i = pl.program_id(0)
    if dp:
        rg, xs, xr, ds = refs[12:16]
        spot = Spot(dp)
        line = LineSum(spot, f_o, *refs[16:23])
        sc = RowsScatter(spot, rec, 1, *refs[23:])
        rest = p_in.at[pl.ds(p_in.shape[0] - rec.shape[1] // 2, rec.shape[1] // 2), :]
        over = remote(s1g, rg, xs, xr, spot.at(spot.z, spot.y, 1 - spot.x, spot.c))

        @pl.when(i == 0)
        def _():
            spot.meet()
            for k in range(LINE):
                line.start(k)
            over.start()
            sc.start(rest, 0)

        for k in range(LINE + 2):
            @pl.when(i == k + 2)
            def _():
                for at, call in line.stages():
                    if at == k:
                        call()
    c = pl.num_programs(0) - 1 - i
    W = hq * PH
    reps = W // 128
    CI = g_in.shape[1]

    @pl.when(i == 0)
    def _():
        dS[...] = jnp.zeros_like(dS)
        pg[pl.ds(T, 8), :] = jnp.zeros((8, CI), F32)
        gbuf[pl.ds(T + 8, 8), :] = jnp.full((8, 128), -1.0, F32)
        ps[pl.ds(T, 8), :] = jnp.zeros((8, 256), F32)
        wg_out[...] = jnp.zeros_like(wg_out)
        ws_out[...] = jnp.zeros_like(ws_out)
        hg_out[...] = jnp.zeros_like(hg_out)

    @pl.when(i > 0)
    def _():
        pg[pl.ds(T, 8), :] = pg[pl.ds(0, 8), :]
        ps[pl.ds(T, 8), :] = ps[pl.ds(0, 8), :]
        gbuf[pl.ds(T + 8, 8), :] = gbuf[pl.ds(8, 8), :]

    vbuf[pl.ds(0, 8), :] = inp8[...]
    vbuf[pl.ds(8, T), :] = inp[...]
    sbuf[pl.ds(0, 8), :] = st8[...]
    sbuf[pl.ds(8, T), :] = st[...]
    first = jnp.where(c == 0, 1.0, 0.0)
    gbuf[pl.ds(0, 8), :] = segb8[...] * (1.0 - first) - first
    gbuf[pl.ds(8, T), :] = segb[...]
    seg = segb[...]
    for k in range(1, 4):
        mbuf[k - 1] = jnp.where(gbuf[pl.ds(8 - k, T), :] == seg, 1.0, 0.0)
        nbuf[k - 1] = jnp.where(gbuf[pl.ds(8 + k, T), :] == seg, 1.0, 0.0)
    before = gbuf[pl.ds(7, 1), :]
    last = gbuf[pl.ds(T + 7, 1), :]
    cs = sbuf[pl.ds(8, T), :] * cws[3:4, :] + cbs[...]
    for k in range(1, 4):
        cs = cs + tile2(mbuf[k - 1], 2) * sbuf[pl.ds(8 - k, T), :] * cws[3 - k : 4 - k, :]
    ss = sigm(cs)
    ms = cs * ss
    Cf = ms[:, 128:]
    Bb = ms[:, :128].astype(BF)
    Cb = Cf.astype(BF)
    Ct = Cf.T.astype(BF)
    GT = mm_nt(Bb, Cb)
    z = stp[...] + sbias[...]
    dt, logdt = step_values(z)
    a = arow[...] * dt
    cum = prefix_sum(a)
    cj = cum - logdt
    cmt[...] = cum.T
    rows = iota((T, T), 0)
    cols = iota((T, T), 1)
    segrow = segr[pl.ds(c, 1), :]
    maskb = jnp.where((seg == segrow) & (rows <= cols), 0.0, NEG)
    cont = tile2(jnp.where(seg == before, 1.0, 0.0), reps)
    trail = tile2(jnp.where(seg == last, 1.0, 0.0), reps)
    unbroken = tile2(jnp.where(last == before, 1.0, 0.0), reps)
    Z[...] = jnp.zeros_like(Z)
    WT[...] = jnp.zeros_like(WT)
    DBC[...] = jnp.zeros_like(DBC)

    def colsum(v):
        acc = v[0:8]
        for r in range(1, T // 8):
            acc = acc + v[8 * r : 8 * r + 8]
        return acc

    def body(q, carry):
        lane = pl.ds(pl.multiple_of(q * W, 128), W)
        v0 = vbuf[pl.ds(8, T), lane]
        cv = v0 * cw[3:4, lane] + cb[:, lane]
        vk = []
        for k in range(1, 4):
            vk.append(tile2(mbuf[k - 1], reps) * vbuf[pl.ds(8 - k, T), lane])
            cv = cv + vk[-1] * cw[3 - k : 4 - k, lane]
        sx = sigm(cv)
        x = cv * sx
        xb = x.astype(BF)
        xr = xb.astype(F32)
        yv = y[:, lane] - skip[:, lane] * x
        gb = g_in[:, lane]
        g = gb.astype(F32)
        tcols = head_cols(cum, q, hq)
        jcols = head_cols(cj, q, hq)
        te = per_pair(tcols, W)
        tl = te[T - 1 : T, :]
        ec = jnp.exp(te) * cont
        w = jnp.exp(tl - per_pair(jcols, W)) * trail
        dxs = []
        wt = jnp.zeros((T, T), F32)
        for p in range(hq // 2):
            gbd = block_diag(gb[:, 128 * p : 128 * p + 128])
            et = mm_nt(xb[:, 128 * p : 128 * p + 128], gbd)
            mts = []
            for h in range(2):
                n = 2 * p + h
                row = cmt[pl.ds(q * hq + n, 1), :]
                kt = jnp.exp(row - jcols[n] + maskb)
                mts.append((kt * GT).astype(BF))
                wt = wt + kt * et[:, T * h : T * h + T]
            dxs.append(mm(jnp.concatenate(mts, axis=1), gbd))
        WT[...] += wt
        dxi = dxs[0] if len(dxs) == 1 else jnp.concatenate(dxs, axis=1)
        Sb = s_in[0, :, lane]
        dSq = dS[:, lane]
        dSb = dSq.astype(BF)
        dxo = mm(Bb, dSb) * w
        wx = (x * w).astype(BF)
        eg = (g * ec).astype(BF)
        DBC[:, :128] += mm_nt(wx, dSb)
        DBC[:, 128:] += mm_nt(eg, Sb)
        el = jnp.exp(tl) * unbroken
        prow = jnp.sum(Sb.astype(F32) * dSq, axis=0, keepdims=True) * el
        dS[:, lane] = dSq * el + mm(Ct, eg)
        ci = xr * dxi
        co = xr * dxo
        stack = jnp.concatenate([g * yv - ci, co, ci + co, jnp.broadcast_to(prow, (8, W))], axis=0)
        hi = stack.astype(BF)
        lo = (stack - hi.astype(F32)).astype(BF)
        ey = eye[pl.ds(pl.multiple_of(q * W, 128), W), :]
        Z[...] += mm(hi, ey) + mm(lo, ey)
        pre = (dxi + dxo + skip[:, lane] * g) * (sx * (1.0 + cv * (1.0 - sx)))
        pg[pl.ds(0, T), lane] = pre
        dv = pre * cw[3:4, lane]
        for k in range(1, 4):
            dv = dv + tile2(nbuf[k - 1], reps) * pg[pl.ds(k, T), lane] * cw[3 - k : 4 - k, lane]
        ca_out[:, lane] = dv.astype(BF)
        wg_out[0:8, lane] += colsum(pre * vk[2])
        wg_out[8:16, lane] += colsum(pre * vk[1])
        wg_out[16:24, lane] += colsum(pre * vk[0])
        wg_out[24:32, lane] += colsum(pre * v0)
        wg_out[32:40, lane] += colsum(pre)
        wg_out[40:48, lane] += colsum(g * x)
        return carry

    lax.fori_loop(0, groups, body, 0)
    z2 = Z[T : 2 * T, :]
    D = suffix_sum(Z[0:T, :]) + (prefix_sum(z2) - z2) + Z[3 * T : 3 * T + 1, :]
    sz = sigm(z)
    lowz = z < -15.0
    rho = jnp.where(lowz, 1.0, jax.nn.sigmoid(z) / jnp.where(lowz, 1.0, dt))
    dz = Z[2 * T : 3 * T, :] * rho + D * arow[...] * jnp.where(lowz, dt, sz)
    ca_out[:, CI + 256 : CI + 384] = dz.astype(BF)
    hg_out[0:8, :] += colsum(D * a)
    hg_out[8:16, :] += colsum(dz)
    wtb = WT[...]
    dbs = DBC[:, :128] + mm_fine(wtb, Cf)
    dcs = DBC[:, 128:] + mm_fine(wtb.T, ms[:, :128])
    pres = jnp.concatenate([dbs, dcs], axis=1) * (ss * (1.0 + cs * (1.0 - ss)))
    ps[pl.ds(0, T), :] = pres
    dsv = pres * cws[3:4, :]
    ws_out[24:32, :] += colsum(pres * sbuf[pl.ds(8, T), :])
    ws_out[32:40, :] += colsum(pres)
    for k in range(1, 4):
        dsv = dsv + tile2(nbuf[k - 1], 2) * ps[pl.ds(k, T), :] * cws[3 - k : 4 - k, :]
        ws_out[24 - 8 * k : 32 - 8 * k, :] += colsum(pres * (tile2(mbuf[k - 1], 2) * sbuf[pl.ds(8 - k, T), :]))
    ca_out[:, CI : CI + 256] = dsv.astype(BF)
    if dp:
        @pl.when(i == pl.num_programs(0) - 1)
        def _():
            over.wait()

            def total(lane):
                f_g[:, lane] = (s0g[:, lane] + rg[:, lane].astype(F32)).astype(BF)

            columns(f_g, total)
            line.finish()
            done = pltpu.make_async_copy(line.fin, d_out, ds)
            done.start()
            done.wait()
            sc.sent(rest, 0)
            sc.got(0)


def scan_backward(proj, segb, segr, g, y, s_in, cw, cb, cws, cbs, sbias, arow, skip, eye, moves=None, rows=0, dp=0):
    L, CI = g.shape
    heads = CI // PH
    hq = 4 if heads % 4 == 0 else 2
    nch = L // T
    blk = lambda w: pl.BlockSpec((T, w), lambda i: (nch - 1 - i, 0))
    part = lambda w, at: pl.BlockSpec((T, w), lambda i: (nch - 1 - i, at // w))
    tail = lambda w, at: pl.BlockSpec((8, w), lambda i: (jnp.maximum((nch - 1 - i) * (T // 8) - 1, 0), at // w))
    ins, in_specs, outs, out_specs, scratch, extra = [], [], [], [], [], {}
    if dp:
        f_o, s0g, s1g, p_in = ins = list(moves)
        once = lambda v: pl.BlockSpec(v.shape, lambda i: (0, 0), pipeline_mode=pl.Buffered(1))
        in_specs = [once(f_o), once(s0g), ANY, ANY]
        like = jax.ShapeDtypeStruct(f_o.shape, BF)
        outs = [like, like, jax.ShapeDtypeStruct((2, 2 * rows, p_in.shape[1] // 4), BF)]
        out_specs = [ANY, full(f_o.shape), ANY]
        dma = pltpu.SemaphoreType.DMA
        scratch = [pltpu.VMEM(s1g.shape, BF), dma, dma, dma] + line_scratch(*f_o.shape) + scatter_sems(1)
        extra = dict(collective_id=5, has_side_effects=True)
    return pl.pallas_call(
        functools.partial(bwd_kernel, hq, heads // hq, dp),
        grid=(nch,),
        in_specs=[blk(CI), tail(CI, 0), part(256, CI), tail(256, CI), part(128, CI + 256), blk(128), tail(128, 0),
                  full(segr.shape), blk(CI), blk(CI), pl.BlockSpec((1, 128, CI), lambda i: (nch - 1 - i, 0, 0)),
                  full(cw.shape), full(cb.shape), full(cws.shape), full(cbs.shape), full(sbias.shape), full(arow.shape),
                  full(skip.shape), full(eye.shape)] + in_specs,
        out_specs=[blk(CI + 384), full((48, CI)), full((40, 256)), full((16, 128))] + out_specs,
        out_shape=[jax.ShapeDtypeStruct((L, CI + 384), BF),
                   jax.ShapeDtypeStruct((48, CI), F32), jax.ShapeDtypeStruct((40, 256), F32), jax.ShapeDtypeStruct((16, 128), F32)] + outs,
        scratch_shapes=[pltpu.VMEM((128, CI), F32), pltpu.VMEM((T + 8, CI), F32), pltpu.VMEM((T + 8, 256), F32),
                        pltpu.VMEM((T + 16, 128), F32), pltpu.VMEM((3, T, 128), F32), pltpu.VMEM((3, T, 128), F32),
                        pltpu.VMEM((T + 8, CI), F32), pltpu.VMEM((T + 8, 256), F32), pltpu.VMEM((128, T), F32),
                        pltpu.VMEM((3 * T + 8, 128), F32), pltpu.VMEM((T, T), F32), pltpu.VMEM((T, 256), F32)] + scratch,
        compiler_params=pltpu.CompilerParams(dimension_semantics=("arbitrary",), vmem_limit_bytes=52 << 20, **extra),
        cost_estimate=pl.CostEstimate(flops=2 * L * CI * (4 * T + 768), bytes_accessed=L * CI * 24, transcendentals=L * CI * 8),
        name="scan_backward",
    )(proj, proj, proj, proj, proj, segb, segb, segr, g, y, s_in, cw, cb, cws, cbs, sbias, arow, skip, eye, *ins)


class Plain:
    def gather_rows(self, h):
        rows = lax.all_gather(h, "head", axis=0, tiled=True)
        return lax.all_to_all(rows, "mp", split_axis=0, concat_axis=1, tiled=True)

    def scatter_rows(self, part):
        rows = lax.all_to_all(part, "mp", split_axis=1, concat_axis=0, tiled=True)
        return lax.psum_scatter(rows.astype(F32), "head", scatter_dimension=0, tiled=True)

    def gather_weight(self, w, axis):
        return lax.all_gather(w, "mp", axis=axis, tiled=True)

    def feature_order(self, v):
        return v

    def head_sum(self, v):
        return lax.psum(v, "head")

    def weight_sum(self, dw, axis):
        own = lax.psum_scatter(dw, "mp", scatter_dimension=axis, tiled=True)
        return lax.psum(own, "dp")

    def state_sum(self, dw):
        size = dw.shape[1] // lax.axis_size("head")
        return lax.psum_scatter(dw, "head", scatter_dimension=1, tiled=True)

    def total(self, v):
        return lax.psum(v, ("dp", "head", "mp"))


class Square:
    def __init__(self):
        self.x = lax.axis_index("mp") // 2
        self.c = lax.axis_index("mp") % 2

    def feature_order(self, v):
        x, c = self.x, self.c
        width = v.shape[0] // 4
        quarters = [x * 2 + c, (1 - x) * 2 + c, x * 2 + 1 - c, (1 - x) * 2 + 1 - c]
        return jnp.concatenate([lax.dynamic_slice_in_dim(v, q * width, width, 0) for q in quarters])


def shards(hidden, in_gain, proj_gate, proj_input, proj_state, proj_step, conv_input, bias_input, conv_state, bias_state,
           step_bias, decay_log, skip_gain, gate_gain, proj_out, segment_ids, cotangent):
    head_pos = lax.axis_index("head")
    sizes = (lax.axis_size("dp"), lax.axis_size("head"), lax.axis_size("mp"))
    square = sizes[1] == 2 and sizes[2] == 4 and sizes[0] == 4
    net = Square() if square else Plain()
    CI = proj_gate.shape[1]
    heads = proj_step.shape[1]
    head_dim = CI // heads
    D = in_gain.shape[0]
    HP = gate_gain.shape[0]
    L = segment_ids.shape[1]
    NST = proj_state.shape[1]
    wa = jnp.concatenate([proj_input, proj_state, jnp.pad(proj_step, ((0, 0), (0, 128 - heads)))], axis=1)

    if square:
        hid, wa = front_gather(hidden, wa, sizes[0])
    else:
        hid = net.gather_rows(hidden)
        wa = net.gather_weight(wa, 0)

    own_cols = lambda v: lax.dynamic_slice_in_dim(v, head_pos * CI, CI, v.ndim - 1)
    own_heads = lambda v: lax.dynamic_slice_in_dim(v, head_pos * heads, heads, 0)
    lanes = lambda v: jnp.pad(v[None], ((0, 0), (0, 128 - heads)))
    cw, cb = own_cols(conv_input), own_cols(bias_input)[None]
    gain2 = own_cols(gate_gain)[None]
    sbias = lanes(own_heads(step_bias))
    arow = lanes(-jnp.exp(own_heads(decay_log)))
    skip = jnp.repeat(own_heads(skip_gain), head_dim)[None]
    eye = (jnp.arange(CI)[:, None] // head_dim == jnp.arange(128)[None, :]).astype(BF)
    seg = segment_ids.astype(F32).reshape(L)
    segb = jnp.broadcast_to(seg[:, None], (L, 128))
    segr = seg.reshape(L // T, T)
    small = (cw, cb, conv_state, bias_state[None], sbias, arow, skip)

    gain1 = net.feature_order(in_gain)
    rows = hid.astype(F32)
    s1 = lax.rsqrt(jnp.mean(rows * rows, axis=1, keepdims=True) + EPS)
    normed = (rows * s1 * gain1).astype(BF)
    proj = jnp.dot(normed, wa, preferred_element_type=F32)
    if square:
        jn, s_in, cot, wg, wo = scan_forward(proj, segb, segr, *small, moves=(cotangent, proj_gate, proj_out), dp=sizes[0])
    else:
        jn, s_in = scan_forward(proj, segb, segr, *small)
        cot = net.gather_rows(cotangent)
        wg = net.gather_weight(proj_gate, 0)
        wo = net.gather_weight(proj_out, 1)
    if square:
        gg, gs, inner_out, pscaled, dgn = gate_and_out(normed, jn, wg, wo, cot, gain2, HP, sizes[0])
        early = L // 4
        f_o, s0g, s1g, rec_a = pair_grads(cot, inner_out, normed, gg, pscaled, early, sizes[0])
    else:
        gate = jnp.dot(normed, wg, preferred_element_type=F32)
        sg = sigm(gate)
        sl = gate * sg
        gated = jn * sl
        part = jnp.dot((gated * gain2).astype(BF), wo, preferred_element_type=F32)
        both = net.head_sum(jnp.stack([jnp.sum(gated * gated, axis=1), jnp.sum(part * cot.astype(F32), axis=1)]))
        s2 = lax.rsqrt(both[0] / HP + EPS)[:, None]
        coef = s2 * s2 * s2 * both[1][:, None] / HP
        block = net.scatter_rows((part * s2).astype(BF))
        gis = lax.dot_general(cot, wo, (((1,), (1,)), ((), ())), preferred_element_type=F32) * s2
        gv = gis * gain2 - gated * coef
        gg = (gv * jn * (sg * (1.0 + gate * (1.0 - sg)))).astype(BF)
        gs = (gv * sl).astype(BF)
        inner_out = (gated * s2 * gain2).astype(BF)
        dgn = jnp.sum(gis * gated, axis=0, keepdims=True)
    if square:
        ca, wgr, wsr, hgr, d_o, f_g, rec_b = scan_backward(proj, segb, segr, gs, jn, s_in, *small, eye, moves=(f_o, s0g, s1g, pscaled),
                                                           rows=L - early, dp=sizes[0])
        split = lambda v: v.reshape(2, 2, -1, D // 4)
        rec = jnp.concatenate([split(rec_a), split(rec_b)], axis=2).reshape(2, 2 * L, D // 4)
        block = rec[0].astype(F32) + rec[1].astype(F32)
    else:
        ca, wgr, wsr, hgr = scan_backward(proj, segb, segr, gs, jn, s_in, *small, eye)
    block_out = (hidden.astype(F32) + block).astype(BF)

    tn = lambda a, b: lax.dot_general(a, b, (((0,), (0,)), ((), ())), preferred_element_type=F32)
    nt = lambda a, b: lax.dot_general(a, b, (((1,), (1,)), ((), ())), preferred_element_type=F32)
    wide = lambda v: lax.dynamic_update_slice_in_dim(jnp.zeros(v.shape[:-1] + (HP,), F32), v, head_pos * CI, v.ndim - 1)
    nheads = step_bias.shape[0]
    few = lambda v: lax.dynamic_update_slice_in_dim(jnp.zeros((nheads,), F32), v, head_pos * heads, 0)
    w7 = jnp.sum(wgr.reshape(6, 8, CI), axis=1)
    w5 = jnp.sum(wsr.reshape(5, 8, NST), axis=1)
    h2 = jnp.sum(hgr.reshape(2, 8, 128), axis=1)[:, :heads]
    dskip = jnp.sum(w7[5].reshape(heads, head_dim), axis=1)
    pack = [jnp.zeros((D,), F32), wide(w7[0:4]), wide(w7[4]), w5[0:4], w5[4], few(h2[1]), few(h2[0]), few(dskip),
            wide(jnp.sum(dgn, axis=0))]
    flat = jnp.concatenate([v.reshape(-1) for v in pack])
    flat = jnp.pad(flat, (0, -flat.shape[0] % 1024))
    if square:
        dwg, dwi, dws, dwt, rec, vec = tail(gg, ca, wg, wa, normed, hid, jnp.broadcast_to(s1, (L, 128)), gain1[None], f_g,
                                            flat.reshape(-1, 128), sizes[0])
        dwo = d_o.astype(F32).T
        dwt = dwt[:, :heads]
        back = rec[0].astype(F32) + rec[1].astype(F32)
        flat = vec.reshape(-1)
    else:
        dwo = net.weight_sum(tn(inner_out, cot), 1)
        dwg = net.weight_sum(tn(normed, gg), 0)
        dwa = net.weight_sum(tn(normed, ca), 0)
        dwi, dwt = dwa[:, :CI], dwa[:, CI + NST : CI + NST + heads]
        dws = net.state_sum(dwa[:, CI : CI + NST])
        ng = nt(gg, wg) + nt(ca, wa)
        grow = ng * gain1
        srow = jnp.sum(grow * rows, axis=1, keepdims=True)
        back = net.scatter_rows((grow * s1 - rows * (s1 * s1 * s1 * srow / D)).astype(BF))
        flat = lax.dynamic_update_slice_in_dim(flat, jnp.sum(ng * rows * s1, axis=0), 0, 0)
        flat = net.total(flat.reshape(-1, 128)).reshape(-1)
    hidden_grad = cotangent.astype(F32) + back

    outs = []
    at = 0
    for v in pack:
        outs.append(flat[at : at + v.size].reshape(v.shape))
        at += v.size
    return (block_out, hidden_grad, outs[0], dwg, dwi, dws, dwt, outs[1], outs[2], outs[3],
            outs[4], outs[5], outs[6], outs[7], outs[8], dwo)


def solution(mesh):
    return jax.shard_map(
        shards,
        mesh=mesh,
        in_specs=(
            P(("dp", "head"), "mp"), P(), P("mp", "head"), P("mp", "head"), P("mp", None), P("mp", "head"), P(), P(), P(), P(),
            P(), P(), P(), P(), P("head", "mp"), P(("dp", "mp"), None), P(("dp", "head"), "mp"),
        ),
        out_specs=(
            P(("dp", "head"), "mp"), P(("dp", "head"), "mp"), P(), P("mp", "head"), P("mp", "head"), P("mp", "head"), P("mp", "head"),
            P(), P(), P(), P(), P(), P(), P(), P(), P("head", "mp"),
        ),
        check_vma=False,
    )
```

```python
import functools
import jax
import jax.numpy as jnp
from jax import lax
from jax.sharding import PartitionSpec as P
from jax.experimental import pallas as pl
from jax.experimental.pallas import tpu as pltpu

T = 128
PH = 64
NEG = -1e30
EPS = 1e-05
LOG2E = 1.4426950408889634
BF = jnp.bfloat16
F32 = jnp.float32


def mm(a, b):
    return jnp.dot(a, b, preferred_element_type=F32)


def mm_nt(a, b):
    return lax.dot_general(a, b, (((1,), (1,)), ((), ())), preferred_element_type=F32)


def mm_fine(a, b):
    ah, bh = a.astype(BF), b.astype(BF)
    al, bl = (a - ah.astype(F32)).astype(BF), (b - bh.astype(F32)).astype(BF)
    return mm(ah, bh) + mm(ah, bl) + mm(al, bh)


def sigm(v):
    return 0.5 * jnp.tanh(0.5 * v) + 0.5


def iota(shape, axis):
    return lax.broadcasted_iota(jnp.int32, shape, axis)


def prefix_sum(v):
    rows = iota(v.shape, 0)
    step = 1
    while step < v.shape[0]:
        v = v + jnp.where(rows >= step, pltpu.roll(v, step, 0), 0.0)
        step *= 2
    return v


def suffix_sum(v):
    size = v.shape[0]
    rows = iota(v.shape, 0)
    step = 1
    while step < size:
        v = v + jnp.where(rows < size - step, pltpu.roll(v, size - step, 0), 0.0)
        step *= 2
    return v


def step_values(z):
    dt = jnp.maximum(z, 0.0) + jnp.log1p(jnp.exp(-jnp.abs(z)))
    low = z < -15.0
    logdt = jnp.where(low, z, jnp.log(jnp.where(low, 1.0, dt)))
    return dt, logdt


def tile2(v, reps):
    return v if reps == 1 else jnp.concatenate([v] * reps, axis=1)


def per_pair(cols, width):
    lanes = iota((T, 128), 1)
    out = []
    for p in range(len(cols) // 2):
        out.append(jnp.where(lanes < PH, cols[2 * p], cols[2 * p + 1]))
    return out[0] if len(out) == 1 else jnp.concatenate(out, axis=1)


def block_diag(v):
    lanes = iota(v.shape, 1)
    zero = jnp.zeros_like(v)
    return jnp.concatenate([jnp.where(lanes < PH, v, zero), jnp.where(lanes >= PH, v, zero)], axis=0)


def head_cols(mat, group, hq):
    shift = lax.rem(128 - group * hq, 128)
    rolled = pltpu.roll(mat, shift, 1)
    return [jnp.broadcast_to(rolled[:, i : i + 1], (T, 128)) for i in range(hq)]


MESH = pl.DeviceIdType.MESH
ANY = pl.BlockSpec(memory_space=pl.ANY)
FWD_CHUNKS = 4


class Spot:
    def __init__(self, dp):
        self.dp = dp
        self.z = lax.axis_index("dp")
        self.y = lax.axis_index("head")
        m = lax.axis_index("mp")
        self.x = m // 2
        self.c = m % 2
        self.same = self.x == self.y

    def at(self, z, y, x, c):
        return (z, y, 2 * x + c)

    def core(self):
        return self.at(self.z, self.y, self.x, 1 - self.c)

    def meet(self):
        sem = pltpu.get_barrier_semaphore()
        peers = []
        for dy in range(2):
            for dx in range(2):
                for dc in range(2):
                    if dy + dx + dc:
                        peers.append((self.z, (self.y + dy) % 2, 2 * ((self.x + dx) % 2) + (self.c + dc) % 2))
        for r in range(1, self.dp):
            peers.append(((self.z + r) % self.dp, self.y, 2 * self.x + self.c))
        for p in peers:
            pl.semaphore_signal(sem, inc=1, device_id=p, device_id_type=MESH)
        pl.semaphore_wait(sem, len(peers))


def remote(src, dst, ss, rs, dev):
    return pltpu.make_async_remote_copy(src_ref=src, dst_ref=dst, send_sem=ss, recv_sem=rs, device_id=dev, device_id_type=MESH)


class RowsGather:
    def __init__(self, spot, src, dst, fbuf, bounce, ss, rs, ls):
        self.p, self.src, self.dst, self.fbuf, self.bounce, self.ss, self.rs, self.ls = spot, src, dst, fbuf, bounce, ss, rs, ls
        self.R = dst.shape[0]
        self.w = dst.shape[1] // 4
        self.n = self.R * 7 // 32 // 16 * 16
        self.far = self.n * FWD_CHUNKS

    def rows(self, t):
        return pl.ds(pl.multiple_of(t * self.R, 16), self.R)

    def cols(self, pos):
        return pl.ds(pl.multiple_of(pos * self.w, 128), self.w)

    def local_in(self):
        to = self.dst.at[:, self.cols(0)] if self.bounce is None else self.bounce
        return pltpu.make_async_copy(self.src.at[self.rows(self.p.c), :], to, self.ls.at[0])

    def local_out(self):
        return pltpu.make_async_copy(self.bounce, self.dst.at[:, self.cols(0)], self.ls.at[1])

    def to_core(self):
        p = self.p
        return remote(self.src.at[self.rows(1 - p.c), :], self.dst.at[:, self.cols(2)], self.ss.at[0], self.rs.at[2], p.core())

    def to_y(self, t):
        p = self.p
        j = (p.c + t) % 2
        return remote(self.src.at[self.rows(t), :], self.dst.at[:, self.cols(2 * j)], self.ss.at[1 + t], self.rs.at[2 * j],
                      p.at(p.z, 1 - p.y, p.x, t))

    def to_x(self, t):
        p = self.p
        j = (p.c + t) % 2
        return remote(self.src.at[self.rows(t), :], self.dst.at[:, self.cols(2 * j + 1)], self.ss.at[t], self.rs.at[2 * j + 1],
                      p.at(p.z, p.y, 1 - p.x, t))

    def to_diag(self, t):
        p = self.p
        j = (p.c + t) % 2
        n = self.R - self.far
        return remote(self.src.at[pl.ds(pl.multiple_of(t * self.R + self.far, 16), n), :],
                      self.dst.at[pl.ds(self.far, n), self.cols(2 * j + 1)], self.ss.at[2 + t], self.rs.at[2 * j + 1],
                      p.at(p.z, 1 - p.y, 1 - p.x, t))

    def to_relay(self, k, t):
        p = self.p
        return remote(self.src.at[pl.ds(pl.multiple_of(t * self.R + k * self.n, 16), self.n), :],
                      self.fbuf.at[t, pl.ds(k * self.n, self.n), :], self.ss.at[4 + 2 * k + t], self.rs.at[4 + 2 * k + t],
                      p.at(p.z, 1 - p.y, p.x, p.c))

    def relay(self, k, t):
        p = self.p
        j = (p.c + t) % 2
        return remote(self.fbuf.at[t, pl.ds(k * self.n, self.n), :],
                      self.dst.at[pl.ds(k * self.n, self.n), self.cols(2 * j + 1)], self.ss.at[4 + 2 * k + t],
                      self.rs.at[4 + 2 * k + j], p.at(p.z, p.y, 1 - p.x, t))

    def start(self):
        @pl.when(self.p.same)
        def _():
            self.to_y(0).start()
            self.to_y(1).start()
            self.to_core().start()
            self.local_in().start()

        @pl.when(jnp.logical_not(self.p.same))
        def _():
            for k in range(FWD_CHUNKS):
                for t in range(2):
                    self.to_relay(k, t).start()
            for t in range(2):
                self.to_x(t).start()
            for t in range(2):
                self.to_diag(t).start()

    def forward(self, k):
        @pl.when(self.p.same)
        def _():
            if k == 0:
                self.local_in().wait()
                if self.bounce is not None:
                    self.local_out().start()
            for t in range(2):
                self.to_relay(k, t).wait_recv()
                self.relay(k, t).start()

    def finish(self):
        @pl.when(self.p.same)
        def _():
            self.to_core().wait()
            for j in range(2):
                self.to_x_wait(j)
            for t in range(2):
                self.to_y(t).wait_send()
                for k in range(FWD_CHUNKS):
                    self.relay(k, t).wait_send()
            if self.bounce is not None:
                self.local_out().wait()

        @pl.when(jnp.logical_not(self.p.same))
        def _():
            for t in range(2):
                self.to_y(t).wait_recv()
                self.to_x(t).wait_send()
                self.to_diag(t).wait()
                for k in range(FWD_CHUNKS):
                    self.relay(k, t).wait_recv()
                    self.to_relay(k, t).wait_send()

    def to_x_wait(self, t):
        self.to_x(t).wait_recv()


class WeightGather:
    def __init__(self, spot, src, dst, axis, bounce, ss, rs, ls):
        self.p, self.src, self.dst, self.axis, self.bounce, self.ss, self.rs, self.ls = spot, src, dst, axis, bounce, ss, rs, ls
        self.n = src.shape[0] // spot.dp

    def chunk(self, k):
        return self.src.at[pl.ds(pl.multiple_of(k * self.n, 16), self.n), :]

    def slot(self, pos, k=None):
        size = self.src.shape[0]
        width = self.src.shape[1]
        if self.axis == 0:
            if k is None:
                return self.dst.at[pl.ds(pos * size, size), :]
            return self.dst.at[pl.ds(pl.multiple_of(pos * size + k * self.n, 16), self.n), :]
        cols = pl.ds(pos * width, width)
        if k is None:
            return self.dst.at[:, cols]
        return self.dst.at[pl.ds(pl.multiple_of(k * self.n, 16), self.n), cols]

    def to_x(self):
        p = self.p
        return remote(self.chunk(p.z), self.slot(1, p.z), self.ss.at[0], self.rs.at[0], p.at(p.z, p.y, 1 - p.x, p.c))

    def to_core(self):
        return remote(self.src, self.slot(2), self.ss.at[1], self.rs.at[1], self.p.core())

    def to_z(self, r):
        p = self.p
        return remote(self.slot(1, p.z), self.slot(1, p.z), self.ss.at[1 + r], self.rs.at[1 + r],
                      p.at((p.z + r) % p.dp, p.y, p.x, p.c))

    def across(self, r):
        p = self.p
        k = (p.z + p.dp - r) % p.dp
        return remote(self.slot(1, k), self.slot(3, k), self.ss.at[1 + p.dp + r], self.rs.at[1 + p.dp + r], p.core())

    def local_in(self):
        to = self.slot(0) if self.bounce is None else self.bounce
        return pltpu.make_async_copy(self.src, to, self.ls.at[0])

    def local_out(self):
        return pltpu.make_async_copy(self.bounce, self.slot(0), self.ls.at[1])

    def start(self):
        self.to_x().start()
        self.to_core().start()
        self.local_in().start()

    def passed(self):
        p = self.p
        k = (p.z + 2) % 4
        low = p.z == 1
        return remote(self.slot(1, k), self.slot(1, k), self.ss.at[1 + 2 * p.dp], self.rs.at[jnp.where(low, 2, 4)],
                      p.at(jnp.where(low, 0, 3), p.y, p.x, p.c))

    def direct(self, r):
        return {1: self.p.z != 3, 2: self.p.z >= 0, 3: self.p.z != 0}[r]

    def middle(self):
        self.to_x().wait_recv()
        for r in (2, 1, 3):
            @pl.when(self.direct(r))
            def _():
                self.to_z(r).start()
        self.across(0).start()
        self.local_in().wait()
        if self.bounce is not None:
            self.local_out().start()

    def hop(self):
        self.to_z(2).wait_recv()
        inner = (self.p.z == 1) | (self.p.z == 2)

        @pl.when(inner)
        def _():
            self.passed().start()

        self.across(2).start()

    def spread(self):
        for r in (1, 3):
            self.to_z(r).wait_recv()
            self.across(r).start()

    def finish(self):
        self.to_x().wait_send()
        self.to_core().wait()
        for r in (1, 2, 3):
            @pl.when(self.direct(r))
            def _():
                self.to_z(r).wait_send()
        inner = (self.p.z == 1) | (self.p.z == 2)

        @pl.when(inner)
        def _():
            self.passed().wait_send()

        for r in range(self.p.dp):
            self.across(r).wait()
        if self.bounce is not None:
            self.local_out().wait()


ROW_SEMS = 4 + 2 * FWD_CHUNKS


def rows_scratch(src):
    R, w = src.shape[0] // 2, src.shape[1]
    dma = pltpu.SemaphoreType.DMA
    return [pltpu.VMEM((2, R, w), BF), pltpu.VMEM((R, w), BF), dma((ROW_SEMS,)), dma((ROW_SEMS,)), dma((2,))]


def weight_scratch(src, dp):
    dma = pltpu.SemaphoreType.DMA
    return [pltpu.VMEM(src.shape, BF), dma((2 + 2 * dp,)), dma((2 + 2 * dp,)), dma((2,))]


def first_scratch(h, C, dp):
    L, w = h.shape[0] // 2, h.shape[1]
    dma = pltpu.SemaphoreType.DMA
    return [pltpu.VMEM((L, 4 * w), BF), pltpu.VMEM((4 * w, C), BF), pltpu.VMEM((L, 4 * w), BF), pltpu.VMEM((L, C), F32),
            pltpu.VMEM((2, L, w), BF), dma((ROW_SEMS,)), dma((ROW_SEMS,)), dma((2,)),
            dma((2 + 2 * dp,)), dma((2 + 2 * dp,)), dma((2,)), dma((2 + 2 * dp,)), dma((2 + 2 * dp,)), dma((2,)), dma((4,))]


def fwd_kernel(hq, groups, dp, *refs):
    c = pl.program_id(0)
    W = hq * PH
    reps = W // 128
    if dp:
        segb, segr, cw, cb, cws, cbs, sbias, arow, skip, gain1, h, wi, wt, cot, wg, wo = refs[:16]
        j_out, s_out, s1_out, hid_out, nrm_out, proj_out, wa_out, cotf, wgf, wof = refs[16:26]
        S, vbuf, sbuf, gbuf, mbuf, cjt = refs[26:32]
        hid, wav, nrm, proj, fb, hs, hr, hl, as_, ar, al, bs_, br, bl, outs = refs[32:47]
        scr = refs[47:]
        CI = j_out.shape[1]
        D = hid.shape[1]
        L = hid.shape[0]
        spot = Spot(dp)
        rh = RowsGather(spot, h, hid, fb, None, hs, hr, hl)
        gw = WeightGather(spot, wi, wav.at[:, pl.ds(0, CI)], 0, None, as_, ar, al)
        gt = WeightGather(spot, wt, wav.at[:, pl.ds(CI, 384)], 0, None, bs_, br, bl)
        rg = RowsGather(spot, cot, cotf, *scr[:5])
        ga = WeightGather(spot, wg, wgf, 0, *scr[5:9])
        go = WeightGather(spot, wo, wof, 1, *scr[9:13])
        keep = [pltpu.make_async_copy(a, b, outs.at[n]) for n, (a, b) in
                enumerate(((hid, hid_out), (nrm, nrm_out), (proj, proj_out), (wav, wa_out)))]

        @pl.when(c == 0)
        def _():
            spot.meet()
            gw.start()
            gt.start()
            rh.start()
            gw.middle()
            gt.middle()
            rh.forward(0)
            rh.forward(1)
            gw.hop()
            gt.hop()
            rh.forward(2)
            gw.spread()
            gt.spread()
            rh.forward(3)
            gw.finish()
            gt.finish()
            rh.finish()
            ga.start()
            go.start()
            rg.start()
            keep[0].start()
            keep[3].start()

            def norm(n, carry):
                rows = pl.ds(pl.multiple_of(n * T, T), T)
                v = hid[rows, :].astype(F32)
                s1 = lax.rsqrt(jnp.sum(v * v, axis=1, keepdims=True) / D + EPS)
                s1_out[rows, :] = jnp.broadcast_to(s1, (T, 128))
                nrm[rows, :] = (v * s1 * gain1[...]).astype(BF)
                return carry

            lax.fori_loop(0, L // T, norm, 0)

            def project(n, carry):
                lane = pl.ds(pl.multiple_of(n * 384, 384), 384)
                for m in range(2):
                    rows = pl.ds(m * (L // 2), L // 2)
                    proj[rows, lane] = mm(nrm[rows, :], wav[:, lane])
                return carry

            tiles = proj.shape[1] // 384
            lax.fori_loop(0, tiles // 2, project, 0)
            ga.middle()
            rg.forward(0)
            lax.fori_loop(tiles // 2, tiles, project, 0)
            keep[1].start()
            keep[2].start()
            go.middle()

        for k in range(2):
            @pl.when(c == 2 * k + 1)
            def _():
                rg.forward(k + 1)

        @pl.when(c == 2)
        def _():
            ga.hop()

        @pl.when(c == 5)
        def _():
            rg.forward(3)
            ga.spread()

        here = pl.ds(pl.multiple_of(c * T, T), T)
        inp = proj.at[here, pl.ds(0, CI)]
        st = proj.at[here, pl.ds(CI, 256)]
        stp = proj.at[here, pl.ds(CI + 256, 128)]
    else:
        inp, st, stp, segb, segr, cw, cb, cws, cbs, sbias, arow, skip = refs[:12]
        j_out, s_out = refs[12:14]
        S, vbuf, sbuf, gbuf, mbuf, cjt = refs[14:20]

    @pl.when(c == 0)
    def _():
        S[...] = jnp.zeros_like(S)
        vbuf[pl.ds(0, 8), :] = jnp.zeros((8, vbuf.shape[1]), F32)
        sbuf[pl.ds(0, 8), :] = jnp.zeros((8, sbuf.shape[1]), F32)
        gbuf[pl.ds(0, 8), :] = jnp.full((8, 128), -1.0, F32)

    @pl.when(c > 0)
    def _():
        vbuf[pl.ds(0, 8), :] = vbuf[pl.ds(T, 8), :]
        sbuf[pl.ds(0, 8), :] = sbuf[pl.ds(T, 8), :]
        gbuf[pl.ds(0, 8), :] = gbuf[pl.ds(T, 8), :]

    vbuf[pl.ds(8, T), :] = inp[...]
    sbuf[pl.ds(8, T), :] = st[...]
    gbuf[pl.ds(8, T), :] = segb[...]
    seg = segb[...]
    for k in range(1, 4):
        mbuf[k - 1] = jnp.where(gbuf[pl.ds(8 - k, T), :] == seg, 1.0, 0.0)
    before = gbuf[pl.ds(7, 1), :]
    last = gbuf[pl.ds(T + 7, 1), :]
    cs = sbuf[pl.ds(8, T), :] * cws[3:4, :] + cbs[...]
    for k in range(1, 4):
        cs = cs + tile2(mbuf[k - 1], 2) * sbuf[pl.ds(8 - k, T), :] * cws[3 - k : 4 - k, :]
    ms = cs * sigm(cs)
    Bf = ms[:, :128]
    Bb = Bf.astype(BF)
    Cb = ms[:, 128:].astype(BF)
    Bt = Bf.T.astype(BF)
    G = mm_nt(Cb, Bb)
    dt, logdt = step_values(stp[...] + sbias[...])
    cum = prefix_sum(arow[...] * dt) * LOG2E
    cj = cum - logdt * LOG2E
    cjt[...] = cj.T
    rows = iota((T, T), 0)
    cols = iota((T, T), 1)
    segrow = segr[pl.ds(c, 1), :]
    maskb = jnp.where((seg == segrow) & (rows >= cols), 0.0, NEG)
    cont = tile2(jnp.where(seg == before, 1.0, 0.0), reps)
    trail = tile2(jnp.where(seg == last, 1.0, 0.0), reps)
    unbroken = tile2(jnp.where(last == before, 1.0, 0.0), reps)

    def body(q, carry):
        lane = pl.ds(pl.multiple_of(q * W, 128), W)
        cv = vbuf[pl.ds(8, T), lane] * cw[3:4, lane] + cb[:, lane]
        for k in range(1, 4):
            cv = cv + tile2(mbuf[k - 1], reps) * vbuf[pl.ds(8 - k, T), lane] * cw[3 - k : 4 - k, lane]
        x = cv * sigm(cv)
        xb = x.astype(BF)
        tcols = head_cols(cum, q, hq)
        jcols = head_cols(cj, q, hq)
        M = []
        for i in range(hq):
            row = cjt[pl.ds(q * hq + i, 1), :]
            M.append((jnp.exp2(tcols[i] - row + maskb) * G).astype(BF))
        yin = []
        for p in range(hq // 2):
            yin.append(mm(jnp.concatenate(M[2 * p : 2 * p + 2], axis=1), block_diag(xb[:, 128 * p : 128 * p + 128])))
        yintra = yin[0] if len(yin) == 1 else jnp.concatenate(yin, axis=1)
        te = per_pair(tcols, W)
        tl = te[T - 1 : T, :]
        Sq = S[:, lane]
        Sb = Sq.astype(BF)
        yinter = mm(Cb, Sb) * (jnp.exp2(te) * cont)
        s_out[0, :, lane] = Sb
        j_out[:, lane] = (yintra + yinter) + skip[:, lane] * x
        w = jnp.exp2(tl - per_pair(jcols, W)) * trail
        wx = (x * w).astype(BF)
        S[:, lane] = Sq * (jnp.exp2(tl) * unbroken) + mm(Bt, wx)
        return carry

    lax.fori_loop(0, groups, body, 0)
    if dp:
        @pl.when(c == pl.num_programs(0) - 1)
        def _():
            go.hop()
            go.spread()
            for cp in keep:
                cp.wait()
            ga.finish()
            go.finish()
            rg.finish()


def full(shape):
    return pl.BlockSpec(shape, lambda i: (0,) * len(shape))


def scan_forward(proj, segb, segr, cw, cb, cws, cbs, sbias, arow, skip, moves=None, dp=0):
    CI = cw.shape[1]
    L = segb.shape[0]
    heads = CI // PH
    hq = 4 if heads % 4 == 0 else 2
    nch = L // T
    blk = lambda w: pl.BlockSpec((T, w), lambda i: (i, 0))
    part = lambda w, at: pl.BlockSpec((T, w), lambda i: (i, at // w))
    outs = [jax.ShapeDtypeStruct((L, CI), F32), jax.ShapeDtypeStruct((nch, 128, CI), BF)]
    out_specs = [blk(CI), pl.BlockSpec((1, 128, CI), lambda i: (i, 0, 0))]
    scratch = [pltpu.VMEM((128, CI), F32), pltpu.VMEM((T + 8, CI), F32), pltpu.VMEM((T + 8, 256), F32),
               pltpu.VMEM((T + 8, 128), F32), pltpu.VMEM((3, T, 128), F32), pltpu.VMEM((128, T), F32)]
    small = [segb, segr, cw, cb, cws, cbs, sbias, arow, skip]
    specs = [blk(128)] + [full(v.shape) for v in small[1:]]
    extra = {}
    if dp:
        gain1, h, wi, wt, cot, wg, wo = moves
        D = gain1.shape[1]
        C = wi.shape[1] + wt.shape[1]
        like = jax.ShapeDtypeStruct
        ins = small + list(moves)
        specs += [full(gain1.shape)] + [ANY] * 6
        outs += [like((L, 128), F32), like((L, D), BF), like((L, D), BF), like((L, C), F32), like((D, C), BF), like((L, D), BF),
                 like((D, wg.shape[1]), BF), like((wo.shape[0], D), BF)]
        out_specs += [full((L, 128))] + [ANY] * 7
        scratch += first_scratch(h, C, dp) + rows_scratch(cot) + weight_scratch(wg, dp) + weight_scratch(wo, dp)
        extra = dict(collective_id=2, has_side_effects=True)
    else:
        ins = [proj, proj, proj] + small
        specs = [blk(CI), part(256, CI), part(128, CI + 256)] + specs
    return pl.pallas_call(
        functools.partial(fwd_kernel, hq, heads // hq, dp),
        grid=(nch,),
        in_specs=specs,
        out_specs=out_specs,
        out_shape=outs,
        scratch_shapes=scratch,
        compiler_params=pltpu.CompilerParams(dimension_semantics=("arbitrary",), vmem_limit_bytes=62 << 20, **extra),
        cost_estimate=pl.CostEstimate(flops=2 * L * CI * (2 * T + 256), bytes_accessed=L * CI * 12, transcendentals=L * CI * 6),
        name="scan_forward",
    )(*ins)


NB = 256
MB = 512
OR = 256


class RowsScatter:
    def __init__(self, spot, dst, nb, ss, rs, ls):
        self.p, self.dst, self.nb, self.ss, self.rs, self.ls = spot, dst, nb, ss, rs, ls
        self.R = dst.shape[1] // 2
        self.w = dst.shape[2]
        self.n = self.R // nb

    def slot(self, y, seq, k):
        return self.dst.at[y, pl.ds(pl.multiple_of(seq * self.R + k * self.n, 16), self.n), :]

    def send(self, buf, k, i, j):
        p = self.p
        src = buf.at[:, pl.ds((2 * j + i) * self.w, self.w)]
        dev = p.at(p.z, p.x, (p.x + i) % 2, (p.c + j) % 2)
        return remote(src, self.slot(p.y, p.c, k), self.ss.at[2 * j + i, k], self.rs.at[p.y, p.c, k], dev)

    def keep(self, buf, k):
        p = self.p
        return pltpu.make_async_copy(buf.at[:, pl.ds(0, self.w)], self.slot(p.y, p.c, k), self.ls.at[k])

    def start(self, buf, k):
        for i, j in ((1, 0), (1, 1), (0, 1)):
            self.send(buf, k, i, j).start()

        @pl.when(self.p.same)
        def _():
            self.keep(buf, k).start()

        @pl.when(jnp.logical_not(self.p.same))
        def _():
            self.send(buf, k, 0, 0).start()

    def sent(self, buf, k):
        for i, j in ((1, 0), (1, 1), (0, 1)):
            self.send(buf, k, i, j).wait_send()

        @pl.when(self.p.same)
        def _():
            self.keep(buf, k).wait()

        @pl.when(jnp.logical_not(self.p.same))
        def _():
            self.send(buf, k, 0, 0).wait_send()

    def got(self, k):
        p = self.p
        for y in range(2):
            for q in range(2):
                own = p.same & (p.y == y) & (p.c == q)

                @pl.when(jnp.logical_not(own))
                def _():
                    v = self.slot(y, q, k)
                    remote(v, v, self.ss.at[0, k], self.rs.at[y, q, k], p.core()).wait_recv()


def scatter_sems(nb):
    dma = pltpu.SemaphoreType.DMA
    return [dma((4, nb)), dma((2, 2, nb)), dma((nb,))]


def mid_kernel(dp, nb, HP, nrm, jn, jb, wg, wo, cot, gain, gg_out, g_out, io_out, p_out, gn_out,
               gbuf, pbuf, ub, ib, ss, ex, rx, acc, es, er):
    i = pl.program_id(0)
    CI = jn.shape[1]
    D = cot.shape[1]
    spot = Spot(dp)
    par = i % 2
    old = (i + 1) % 2
    acc[...] = jnp.zeros_like(acc)
    lanes = iota((OR, 128), 1)

    def swap(k):
        dev = spot.at(spot.z, 1 - spot.y, spot.x, spot.c)
        return remote(ex.at[k % 2], rx.at[k % 2], es.at[k % 2], er.at[k % 2], dev)

    @pl.when(i == 0)
    def _():
        gn_out[...] = jnp.zeros_like(gn_out)
        spot.meet()

    for q in range(nb):
        @pl.when(i == q + 1)
        def _():
            swap(q).start()

    @pl.when(i < nb)
    def _():
        def one(n, carry):
            lane = pl.ds(pl.multiple_of(n * MB, MB), MB)
            gt = mm(nrm[...], wg[:, lane])
            gbuf[par, :, lane] = gt
            gated = jn[:, lane] * (gt * sigm(gt))
            ub[:, lane] = (gated * gain[:, lane]).astype(BF)
            sq = gated * gated
            for p in range(MB // 128):
                acc[0] += sq[:, 128 * p : 128 * p + 128]
            return carry

        lax.fori_loop(0, CI // MB, one, 0)

        def two(n, carry):
            lane = pl.ds(pl.multiple_of(n * MB, MB), MB)
            pv = mm(ub[...], wo[:, lane])
            pbuf[par, :, lane] = pv
            d = pv * cot[pl.ds(pl.multiple_of(i * OR, OR), OR), lane].astype(F32)
            for p in range(MB // 128):
                acc[1] += d[:, 128 * p : 128 * p + 128]
            return carry

        lax.fori_loop(0, D // MB, two, 0)
        s_sum = jnp.sum(acc[0], axis=1, keepdims=True)
        d_sum = jnp.sum(acc[1], axis=1, keepdims=True)
        both = jnp.where(lanes == 0, s_sum, d_sum)
        ss[par] = both
        ex[par] = both.T[0:8, :]

    @pl.when(i > 0)
    def _():
        k = i - 1

        def three(n, carry):
            lane = pl.ds(pl.multiple_of(n * MB, MB), MB)
            ib[:, lane] = mm_nt(cot[pl.ds(pl.multiple_of(k * OR, OR), OR), :], wo[lane, :])
            return carry

        lax.fori_loop(0, CI // MB, three, 0)
        for q in range(nb):
            @pl.when(k == q)
            def _():
                swap(q).wait()
        theirs = jnp.concatenate([rx[old], jnp.zeros((120, OR), F32)], axis=0).T
        tot = ss[old] + theirs
        s2 = lax.rsqrt(jnp.broadcast_to(tot[:, 0:1], (OR, 128)) / HP + EPS)
        cf = s2 * s2 * s2 * (jnp.broadcast_to(tot[:, 1:2], (OR, 128)) / HP)
        s2w = tile2(s2, MB // 128)
        cfw = tile2(cf, MB // 128)

        def scale(n, carry):
            lane = pl.ds(pl.multiple_of(n * MB, MB), MB)
            p_out[:, lane] = (pbuf[old, :, lane] * s2w).astype(BF)
            return carry

        lax.fori_loop(0, D // MB, scale, 0)

        def four(n, carry):
            lane = pl.ds(pl.multiple_of(n * MB, MB), MB)
            gt = gbuf[old, :, lane]
            joined = jb[:, lane]
            sg = sigm(gt)
            sl = gt * sg
            gated = joined * sl
            gis = ib[:, lane] * s2w
            gv = gis * gain[:, lane] - gated * cfw
            gg_out[:, lane] = (gv * joined * (sg * (1.0 + gt * (1.0 - sg)))).astype(BF)
            g_out[:, lane] = (gv * sl).astype(BF)
            io_out[:, lane] = (gated * s2w * gain[:, lane]).astype(BF)
            gn_out[:, lane] += sum8(gis * gated)
            return carry

        lax.fori_loop(0, CI // MB, four, 0)


def gate_and_out(nrm, jn, wg, wo, cot, gain, HP, dp):
    L, D = nrm.shape
    CI = wg.shape[1]
    nb = L // OR
    now = lambda w: pl.BlockSpec((OR, w), lambda i: (jnp.minimum(i, nb - 1), 0))
    back = lambda w: pl.BlockSpec((OR, w), lambda i: (jnp.maximum(i - 1, 0), 0))
    once = lambda shape: pl.BlockSpec(shape, lambda i: (0, 0), pipeline_mode=pl.Buffered(1))
    dma = pltpu.SemaphoreType.DMA
    return pl.pallas_call(
        functools.partial(mid_kernel, dp, nb, HP),
        grid=(nb + 1,),
        in_specs=[now(D), now(CI), back(CI), once(wg.shape), once(wo.shape), once(cot.shape), full(gain.shape)],
        out_specs=[back(CI), back(CI), back(CI), back(D), full((8, CI))],
        out_shape=[jax.ShapeDtypeStruct((L, CI), BF), jax.ShapeDtypeStruct((L, CI), BF), jax.ShapeDtypeStruct((L, CI), BF),
                   jax.ShapeDtypeStruct((L, D), BF), jax.ShapeDtypeStruct((8, CI), F32)],
        scratch_shapes=[pltpu.VMEM((2, OR, CI), F32), pltpu.VMEM((2, OR, D), F32), pltpu.VMEM((OR, CI), BF), pltpu.VMEM((OR, CI), F32),
                        pltpu.VMEM((2, OR, 128), F32), pltpu.VMEM((2, 8, OR), F32), pltpu.VMEM((2, 8, OR), F32),
                        pltpu.VMEM((2, OR, 128), F32), dma((2,)), dma((2,))],
        compiler_params=pltpu.CompilerParams(dimension_semantics=("arbitrary",), vmem_limit_bytes=62 << 20, collective_id=3,
                                             has_side_effects=True),
        cost_estimate=pl.CostEstimate(flops=6 * L * CI * D, bytes_accessed=L * D * 22 + CI * D * 4, transcendentals=L * CI),
        name="gate_and_out",
    )(nrm, jn, jn, wg, wo, cot, gain)


def mm_tn(a, b):
    return lax.dot_general(a, b, (((0,), (0,)), ((), ())), preferred_element_type=F32)


def even(C, width=384):
    return [(at, min(width, C - at)) for at in range(0, C, width)]


class LineSum:
    def __init__(self, spot, pieces, own, fin, obuf, ibuf, tbuf, pbuf, ss, rs):
        self.K = len(pieces)
        self.pieces = pieces
        self.p, self.own, self.fin, self.obuf, self.ibuf, self.tbuf, self.pbuf, self.ss, self.rs = spot, own, fin, obuf, ibuf, tbuf, pbuf, ss, rs
        self.n = own.shape[0] // 2
        z = spot.z
        self.mid = (z == 1) | (z == 2)
        self.out = jnp.logical_not(self.mid)
        self.inner = jnp.where(z == 0, 1, jnp.where(z == 3, 2, 3 - z))
        self.outer = jnp.where(z == 1, 0, 3)
        self.hm = jnp.where(z == 1, 0, 1)

    def cols(self, k):
        return pl.ds(*self.pieces[k])

    def rows(self, ref, h, k):
        return ref.at[pl.ds(pl.multiple_of(h * self.n, 16), self.n), self.cols(k)]

    def to(self, z):
        return self.p.at(z, self.p.y, self.p.x, self.p.c)

    def up(self, h, k):
        return remote(self.rows(self.own, h, k), self.rows(self.obuf, h, k), self.ss.at[h * self.K + k], self.rs.at[h * self.K + k],
                      self.to(self.inner))

    def across(self, k):
        return remote(self.tbuf.at[:, self.cols(k)], self.ibuf.at[:, self.cols(k)], self.ss.at[2 * self.K + k],
                      self.rs.at[2 * self.K + k], self.to(self.inner))

    def down(self, h, k, which):
        v = self.rows(self.fin, h, k)
        dest = self.to(self.outer) if which == 0 else self.to(self.inner)
        return remote(v, v, self.ss.at[(3 + which) * self.K + k], self.rs.at[3 * self.K + h * self.K + k], dest)

    def pass_on(self, k):
        h = 1 - self.hm
        v = self.rows(self.fin, h, k)
        return remote(v, v, self.ss.at[5 * self.K + k], self.rs.at[3 * self.K + h * self.K + k], self.to(self.outer))

    def start(self, k):
        @pl.when(self.out)
        def _():
            self.up(0, k).start()
            self.up(1, k).start()

    def each(self, h, body):
        def one(r, carry):
            body(pl.ds(pl.multiple_of(r * 48, 16), 48), pl.ds(pl.multiple_of(h * self.n + r * 48, 16), 48))
            return carry

        lax.fori_loop(0, self.n // 48, one, 0)

    def gather(self, k):
        @pl.when(self.mid)
        def _():
            ho = 1 - self.hm
            c = self.cols(k)
            self.up(ho, k).wait_recv()

            def theirs(v, a):
                self.tbuf[v, c] = (self.own[a, c].astype(F32) + self.obuf[a, c].astype(F32)).astype(BF)

            def mine(v, a):
                self.pbuf[v, c] = self.own[a, c].astype(F32) + self.obuf[a, c].astype(F32)

            self.each(ho, theirs)
            self.up(self.hm, k).wait_recv()
            self.each(self.hm, mine)
            self.across(k).start()

    def close(self, k):
        @pl.when(self.mid)
        def _():
            c = self.cols(k)
            self.across(k).wait_recv()

            def final(v, a):
                self.fin[a, c] = (self.pbuf[v, c] + self.ibuf[v, c].astype(F32)).astype(BF)

            self.each(self.hm, final)

    def back(self, k):
        @pl.when(self.mid)
        def _():
            self.down(self.hm, k, 0).start()
            self.down(self.hm, k, 1).start()

    def relay(self, k):
        @pl.when(self.mid)
        def _():
            self.pass_on(k).wait_recv()
            self.pass_on(k).start()

    def stages(self):
        calls = []
        for k in range(self.K + 2):
            if k < self.K:
                calls.append((k, functools.partial(self.gather, k)))
            if 0 <= k - 1 < self.K:
                calls.append((k, functools.partial(self.close, k - 1)))
            if 0 <= k - 2 < self.K:
                calls.append((k, functools.partial(self.relay, k - 2)))
            if 0 <= k - 1 < self.K:
                calls.append((k, functools.partial(self.back, k - 1)))
        return calls

    def landed(self, k):
        @pl.when(self.out)
        def _():
            for h in range(2):
                self.down(h, k, 0).wait_recv()

    def finish(self, done=()):
        @pl.when(self.mid)
        def _():
            for k in range(self.K):
                self.across(k).wait_send()
                self.down(self.hm, k, 0).wait_send()
                self.down(self.hm, k, 1).wait_send()
                self.pass_on(k).wait_send()

        @pl.when(self.out)
        def _():
            for k in range(self.K):
                for h in range(2):
                    self.up(h, k).wait_send()

        for k in range(self.K):
            if k not in done:
                self.landed(k)


def line_scratch(rows, C, pieces):
    dma = pltpu.SemaphoreType.DMA
    h = rows // 2
    return [pltpu.VMEM((rows, C), BF), pltpu.VMEM((rows, C), BF), pltpu.VMEM((h, C), BF), pltpu.VMEM((h, C), BF),
            pltpu.VMEM((h, C), F32), dma((6 * len(pieces),)), dma((5 * len(pieces),))]


def columns(ref, body, step=128):
    def one(n, carry):
        body(pl.ds(pl.multiple_of(n * step, 128), step))
        return carry

    lax.fori_loop(0, ref.shape[1] // step, one, 0)


def pair_kernel(dp, cot, io, nrm, gg, p_in, f_out, s0g, s1g, rec, give, got, own, s1o, ro, vs, vr, xs, xr, *sems):
    spot = Spot(dp)
    sc = RowsScatter(spot, rec, 1, *sems)
    first = p_in.at[pl.ds(0, rec.shape[1] // 2), :]
    w = cot.shape[1] // 4
    C = io.shape[1]
    spot.meet()
    sc.start(first, 0)
    work = ((cot, io), (nrm, gg))

    tiles = C // MB
    cut = lambda n: pl.ds(n * MB, MB)

    def over(n):
        return remote(s1o.at[:, cut(n)], ro.at[:, cut(n)], xs.at[n], xr.at[n], spot.at(spot.z, spot.y, 1 - spot.x, spot.c))

    def theirs(m, b, n):
        a, r = work[m]
        give[m, b * w : b * w + w, cut(n)] = mm_tn(a[:, (2 + b) * w : (3 + b) * w], r[:, cut(n)]).astype(BF)

    def mine(m, b, n):
        a, r = work[m]
        own[b + 2 * m * (1 - b), :, cut(n)] = mm_tn(a[:, b * w : b * w + w], r[:, cut(n)])

    def joined(m, b, n, dst):
        swap(m, b, n).wait()

        def part(k, carry):
            rows = pl.ds(pl.multiple_of(k * 48, 48), 48)
            got_rows = pl.ds(pl.multiple_of(b * w + k * 48, 48), 48)
            dst[rows, cut(n)] = (own[b + 2 * m * (1 - b), rows, cut(n)] + got[m, got_rows, cut(n)].astype(F32)).astype(dst.dtype)
            return carry

        lax.fori_loop(0, w // 48, part, 0)

    def swap(m, b, n):
        rows = pl.ds(b * w, w)
        return remote(give.at[m, rows, cut(n)], got.at[m, rows, cut(n)], vs.at[m, b, n], vr.at[m, b, n], spot.core())

    theirs(0, 1, 0)
    for n in range(tiles):
        if n + 1 < tiles:
            theirs(0, 1, n + 1)
        else:
            mine(0, 1, 0)
        swap(0, 1, n).start()
    for n in range(tiles):
        joined(0, 1, n, s1o)
        if n + 1 < tiles:
            mine(0, 1, n + 1)
        else:
            theirs(0, 0, 0)
        over(n).start()
    for n in range(tiles):
        if n + 1 < tiles:
            theirs(0, 0, n + 1)
        else:
            theirs(1, 1, 0)
        swap(0, 0, n).start()
    for n in range(tiles):
        mine(0, 0, n)
        joined(0, 0, n, own.at[0])
    for n in range(tiles):
        if n + 1 < tiles:
            theirs(1, 1, n + 1)
        else:
            theirs(1, 0, 0)
        swap(1, 1, n).start()
    for n in range(tiles):
        mine(1, 1, n)
        joined(1, 1, n, s1g)
        if n + 1 < tiles:
            theirs(1, 0, n + 1)
        swap(1, 0, n).start()
    for n in range(tiles):
        mine(1, 0, n)
        joined(1, 0, n, s0g)
    for n in range(tiles):
        over(n).wait()

        def total(k, carry):
            rows = pl.ds(pl.multiple_of(k * 48, 48), 48)
            f_out[rows, cut(n)] = (own[0, rows, cut(n)] + ro[rows, cut(n)].astype(F32)).astype(BF)
            return carry

        lax.fori_loop(0, w // 48, total, 0)
    sc.sent(first, 0)
    sc.got(0)


def pair_grads(cot, io, nrm, gg, p_in, rows, dp):
    L, D = cot.shape
    C = io.shape[1]
    w = D // 4
    dma = pltpu.SemaphoreType.DMA
    vm = pl.BlockSpec(memory_space=pltpu.VMEM)
    return pl.pallas_call(
        functools.partial(pair_kernel, dp),
        in_specs=[vm, vm, vm, vm, ANY],
        out_specs=[vm, vm, vm, ANY],
        out_shape=[jax.ShapeDtypeStruct((w, C), BF), jax.ShapeDtypeStruct((w, C), F32),
                   jax.ShapeDtypeStruct((w, C), BF), jax.ShapeDtypeStruct((2, 2 * rows, w), BF)],
        scratch_shapes=[pltpu.VMEM((2, 2 * w, C), BF), pltpu.VMEM((2, 2 * w, C), BF), pltpu.VMEM((3, w, C), F32),
                        pltpu.VMEM((w, C), BF), pltpu.VMEM((w, C), BF), dma((2, 2, C // MB)), dma((2, 2, C // MB)), dma((C // MB,)),
                        dma((C // MB,))] + scatter_sems(1),
        compiler_params=pltpu.CompilerParams(vmem_limit_bytes=56 << 20, collective_id=4, has_side_effects=True),
        cost_estimate=pl.CostEstimate(flops=4 * L * C * D, bytes_accessed=L * D * 8 + C * w * 12, transcendentals=0),
        name="pair_grads",
    )(cot, io, nrm, gg, p_in)


def in_pieces(C):
    return [(C - 384, 384)] + even(C - 768) + [(C - 768, 256), (C - 512, 128)]


def tail_kernel(dp, nb, gg, hid, s1, ca, nrm, fgs, gain, vec, wg_any, wa_any, fin_g, fin_a, sth_out, rec, tot,
                wgv, wav, give, got, own, s1a, ra, fa, ng, hp, igs, vb, vr, sth, ws, vs, vq, xs, xr, bs, br, ys, yr, os, *rest):
    i = pl.program_id(0)
    D = gain.shape[1]
    w = D // 4
    C = ca.shape[1]
    CI = C - 384
    spot = Spot(dp)
    lg = LineSum(spot, even(CI), fgs, *rest[:7])
    la = LineSum(spot, in_pieces(C), fa, *rest[7:14])
    sc = RowsScatter(spot, rec, nb, *rest[14:])
    OR = gg.shape[0]
    K = la.K

    def weights():
        return (pltpu.make_async_copy(wg_any, wgv, ws.at[0]), pltpu.make_async_copy(wa_any, wav, ws.at[1]))

    def swap(b, k):
        part = (pl.ds(b * w, w), la.cols(k))
        return remote(give.at[part], got.at[part], vs.at[b, k], vq.at[b, k], spot.core())

    def over(k):
        return remote(s1a.at[:, la.cols(k)], ra.at[:, la.cols(k)], xs.at[k], xr.at[k], spot.at(spot.z, spot.y, 1 - spot.x, spot.c))

    def theirs(b, k):
        give[b * w : b * w + w, la.cols(k)] = mm_tn(nrm[:, (2 + b) * w : (3 + b) * w], ca[:, la.cols(k)]).astype(BF)

    def mine(b, k):
        own[b, :, la.cols(k)] = mm_tn(nrm[:, b * w : b * w + w], ca[:, la.cols(k)])

    def joined(b, k, dst):
        swap(b, k).wait()
        c = la.cols(k)

        def part(r, carry):
            rows = pl.ds(pl.multiple_of(r * 48, 16), 48)
            theirs_at = pl.ds(pl.multiple_of(b * w + r * 48, 16), 48)
            dst[rows, c] = (own[b, rows, c] + got[theirs_at, c].astype(F32)).astype(dst.dtype)
            return carry

        lax.fori_loop(0, w // 48, part, 0)

    def arrive(k):
        over(k).wait_recv()
        c = la.cols(k)

        def part(r, carry):
            rows = pl.ds(pl.multiple_of(r * 48, 16), 48)
            fa[rows, c] = (own[0, rows, c] + ra[rows, c].astype(F32)).astype(BF)
            return carry

        lax.fori_loop(0, w // 48, part, 0)

    def mix(s):
        z = spot.z
        near = [spot.core(), spot.at(z + 1 - 2 * (z % 2), spot.y, spot.x, spot.c), spot.at((z + 2) % 4, spot.y, spot.x, spot.c),
                spot.at(z, 1 - spot.y, spot.x, spot.c), spot.at(z, spot.y, 1 - spot.x, spot.c)]
        return remote(vb.at[s], vr.at[s], bs.at[s], br.at[s], near[s])

    def mixed(s):
        mix(s).wait()
        v = vb[s] + vr[s]
        if s < 4:
            vb[s + 1] = v
        else:
            tot[...] = v

    def stage(line, k):
        for at, call in line.stages():
            if at == k:
                call()

    @pl.when(i == 0)
    def _():
        for cp in weights():
            cp.start()
        igs[...] = jnp.zeros_like(igs)
        spot.meet()
        for k in range(lg.K):
            lg.start(k)
        for k in range(K + 2):
            if k < K:
                theirs(1, k)
                mine(1, k)
                swap(1, k).start()
            if 1 <= k <= K:
                joined(1, k - 1, s1a)
            if k >= 2:
                over(k - 2).start()
        for k in range(K + 1):
            if k < K:
                theirs(0, k)
                mine(0, k)
                swap(0, k).start()
            if k >= 1:
                joined(0, k - 1, own.at[0])
        for cp in weights():
            cp.wait()

    @pl.when(i > 0)
    def _():
        def one(n, srow):
            lane = pl.ds(pl.multiple_of(n * NB, NB), NB)
            v = mm_nt(gg[...], wgv[lane, :]) + mm_nt(ca[pl.ds(pl.multiple_of((i - 1) * OR, OR), OR), :], wav[lane, :])
            rows = hid[:, lane].astype(F32)
            sv = tile2(s1[...], NB // 128)
            t = v * rows
            igs[:, lane] += sum8(t * sv)
            v = v * gain[:, lane]
            ng[:, lane] = v
            t = v * rows
            for p in range(NB // 128):
                srow = srow + t[:, 128 * p : 128 * p + 128]
            return srow

        srow = lax.fori_loop(0, D // NB, one, jnp.zeros((OR, 128), F32))
        scale = s1[...]
        coef = scale * scale * scale * (jnp.sum(srow, axis=1, keepdims=True) / D)
        block = pl.ds(pl.multiple_of((i - 1) * OR, OR), OR)

        def two(lane):
            hp[block, lane] = (ng[:, lane] * scale - hid[:, lane].astype(F32) * coef).astype(BF)

        columns(ng, two)

    def part(k):
        return hp.at[pl.ds(k * OR, OR), :]

    def turn(k, between=None):
        if k < K:
            arrive(k)
        if between is not None:
            between.start()
        if k >= 2:
            stage(la, k - 2)
        if k < K:
            la.start(k)

    early = (0, 1, 2, 3)
    for q in range(1, nb + 1):
        @pl.when(i == q)
        def _():
            if q >= 2:
                sc.start(part(q - 2), q - 2)
            if q <= lg.K:
                stage(lg, q - 1)
            for k in range(early[q - 2] if q >= 2 else 0, early[q - 1]):
                turn(k)

    @pl.when(i == nb)
    def _():
        x, c = spot.x, spot.c
        vb[0] = vec[...]
        ig = jnp.sum(igs[...], axis=0, keepdims=True)
        place = [x * 2 + c, (1 - x) * 2 + c, x * 2 + 1 - c, (1 - x) * 2 + 1 - c]
        for p in range(4):
            for t in range(w // 128):
                at = p * w + t * 128
                vb[0, pl.ds(place[p] * (w // 128) + t, 1), :] = ig[:, at : at + 128]
        stage(lg, lg.K)
        mix(0).start()
        sc.start(part(nb - 1), nb - 1)
        give_half = la.fin.at[:, pl.ds(pl.multiple_of(CI + (1 - spot.y) * 128, 128), 128)]
        state = remote(give_half, sth, ys, yr, spot.at(spot.z, 1 - spot.y, spot.x, spot.c))
        for k in range(early[-1], K + 4):
            s = k - early[-1]
            turn(k, mix(s) if 0 < s < 5 else None)
            if s == 0:
                stage(lg, lg.K + 1)
            if s < 5:
                mixed(s)
            if s == 4:
                la.landed(0)
                state.start()
        out_g = pltpu.make_async_copy(lg.fin, fin_g, os.at[0])
        lg.finish()
        out_g.start()
        la.finish(done=(0,))
        out_a = pltpu.make_async_copy(la.fin, fin_a, os.at[1])
        out_a.start()
        state.wait()
        sth_out[...] = sth[...]
        for k in range(K):
            over(k).wait_send()
        for q in range(nb):
            sc.sent(part(q), q)
            sc.got(q)
        out_g.wait()
        out_a.wait()


def tail(gg, ca, wg, wa, nrm, hid, s1c, gain, f_g, vec, dp):
    L, D = hid.shape
    CI = gg.shape[1]
    C = ca.shape[1]
    w = D // 4
    R = 256
    nb = L // R
    K = len(in_pieces(C))
    back = lambda v: pl.BlockSpec((R, v), lambda i: (jnp.maximum(i - 1, 0), 0))
    once = lambda v: pl.BlockSpec(v.shape, lambda i: (0,) * v.ndim, pipeline_mode=pl.Buffered(1))
    dma = pltpu.SemaphoreType.DMA
    like = lambda shape, t: jax.ShapeDtypeStruct(shape, t)
    shapes = [like((w, CI), BF), like((w, C), BF), like((w, 128), BF), like((2, 2 * L, w), BF), like(vec.shape, F32)]
    return pl.pallas_call(
        functools.partial(tail_kernel, dp, nb),
        grid=(nb + 1,),
        in_specs=[back(CI), back(D), back(128), once(ca), once(nrm), once(f_g), once(gain), once(vec), ANY, ANY],
        out_specs=[ANY, ANY, full((w, 128)), ANY, full(vec.shape)],
        out_shape=shapes,
        scratch_shapes=[pltpu.VMEM(wg.shape, BF), pltpu.VMEM(wa.shape, BF), pltpu.VMEM((2 * w, C), BF), pltpu.VMEM((2 * w, C), BF),
                        pltpu.VMEM((2, w, C), F32), pltpu.VMEM((w, C), BF), pltpu.VMEM((w, C), BF), pltpu.VMEM((w, C), BF),
                        pltpu.VMEM((R, D), F32), pltpu.VMEM((L, D), BF), pltpu.VMEM((8, D), F32),
                        pltpu.VMEM((5,) + vec.shape, F32), pltpu.VMEM((5,) + vec.shape, F32), pltpu.VMEM((w, 128), BF),
                        dma((2,)), dma((2, K)), dma((2, K)), dma((K,)), dma((K,)), dma((5,)), dma((5,)), dma, dma, dma((2,))]
        + line_scratch(w, CI, even(CI)) + line_scratch(w, C, in_pieces(C)) + scatter_sems(nb),
        compiler_params=pltpu.CompilerParams(dimension_semantics=("arbitrary",), vmem_limit_bytes=62 << 20, collective_id=6,
                                             has_side_effects=True),
        cost_estimate=pl.CostEstimate(flops=2 * L * D * (CI + 2 * C), bytes_accessed=L * D * 12 + D * D * 4, transcendentals=0),
        name="tail",
    )(gg, hid, s1c, ca, nrm, f_g, gain, vec, wg, wa)


def finish_kernel(segs, rech, cot, reca, recb, hid, fg, fa, fo, sth, vec, bo_out, hg_out, dwg, dwi, dws, dwt, dwo, *outs):
    i = pl.program_id(0)
    CI = dwi.shape[1]
    hg_out[...] = cot[...].astype(F32) + rech[0].astype(F32) + rech[1].astype(F32)

    @pl.when(i % 4 == 0)
    def _():
        bo_out[...] = (hid[...].astype(F32) + reca[0].astype(F32) + reca[1].astype(F32)).astype(BF)

    @pl.when(i % 4 > 0)
    def _():
        bo_out[...] = (hid[...].astype(F32) + recb[0].astype(F32) + recb[1].astype(F32)).astype(BF)

    dwg[...] = fg[...].astype(F32)
    dwi[...] = fa[:, :CI].astype(F32)
    y = lax.axis_index("head")
    mine = jnp.where(y == 0, fa[:, CI : CI + 128].astype(F32), fa[:, CI + 128 : CI + 256].astype(F32))
    dws[...] = mine + sth[...].astype(F32)
    dwt[...] = fa[:, CI + 256 : CI + 256 + dwt.shape[1]].astype(F32)

    @pl.when(i < 4)
    def _():
        dwo[...] = fo[...].astype(F32).T

    @pl.when(i == 0)
    def _():
        for (at, shape), out in zip(segs, outs):
            width = shape[-1]
            per = -(-width // 128)
            for k in range(shape[0] if len(shape) == 2 else 1):
                for r in range(per):
                    n = min(128, width - 128 * r)
                    row = at + k * per + r
                    if len(shape) == 2:
                        out[k : k + 1, 128 * r : 128 * r + n] = vec[row : row + 1, :n]
                    else:
                        out[pl.ds(128 * r, n)] = vec[row, :n]


def finish(segs, rec_h, cot, rec_a, rec_b, hid, fin_g, fin_a, d_o, sth, vec, heads):
    rows, w = cot.shape
    CI = fin_g.shape[1]
    n = rows // 8
    m = fin_g.shape[0] // 8
    like = jax.ShapeDtypeStruct
    blk = lambda r, c: pl.BlockSpec((r, c), lambda i: (i, 0))
    rec = lambda f: pl.BlockSpec((2, n, w), lambda i: (0, f(i), 0))
    wide = CI // 4
    few = lambda shape: pl.BlockSpec(shape, lambda i: (0,) * len(shape))
    return pl.pallas_call(
        functools.partial(finish_kernel, segs),
        grid=(8,),
        in_specs=[rec(lambda i: i), blk(n, w), rec(lambda i: i // 4), rec(lambda i: (i // 4) * 3 + jnp.maximum(i % 4 - 1, 0)), blk(n, w),
                  blk(m, CI), blk(m, fin_a.shape[1]), pl.BlockSpec((w, wide), lambda i: (0, jnp.minimum(i, 3))), blk(m, 128), few(vec.shape)],
        out_specs=[blk(n, w), blk(n, w), blk(m, CI), blk(m, CI), blk(m, 128), blk(m, heads),
                   pl.BlockSpec((wide, w), lambda i: (jnp.minimum(i, 3), 0))] + [few(shape) for _, shape in segs],
        out_shape=[like((rows, w), BF), like((rows, w), F32), like((8 * m, CI), F32), like((8 * m, CI), F32), like((8 * m, 128), F32),
                   like((8 * m, heads), F32), like((CI, w), F32)] + [like(shape, F32) for _, shape in segs],
        compiler_params=pltpu.CompilerParams(dimension_semantics=("arbitrary",), vmem_limit_bytes=62 << 20),
        cost_estimate=pl.CostEstimate(flops=rows * w * 4, bytes_accessed=rows * w * 20 + CI * w * 18, transcendentals=0),
        name="finish",
    )(rec_h, cot, rec_a, rec_b, hid, fin_g, fin_a, d_o, sth, vec)


def sum8(v):
    acc = v[0:8]
    for r in range(1, v.shape[0] // 8):
        acc = acc + v[8 * r : 8 * r + 8]
    return acc


def bwd_kernel(hq, groups, dp, *refs):
    inp, inp8, st, st8, stp, segb, segb8, segr, g_in, y, s_in, cw, cb, cws, cbs, sbias, arow, skip, eye = refs[:19]
    refs = refs[19:]
    if dp:
        f_o, s0g, s1g, p_in = refs[:4]
        refs = refs[4:]
    ca_out, wg_out, ws_out, hg_out = refs[:4]
    refs = refs[4:]
    if dp:
        d_out, f_g, rec = refs[:3]
        refs = refs[3:]
    dS, vbuf, sbuf, gbuf, mbuf, nbuf, pg, ps, cmt, Z, WT, DBC = refs[:12]
    i = pl.program_id(0)
    if dp:
        rg, xs, xr, ds = refs[12:16]
        spot = Spot(dp)
        line = LineSum(spot, even(f_o.shape[1]), f_o, *refs[16:23])
        sc = RowsScatter(spot, rec, 1, *refs[23:])
        rest = p_in.at[pl.ds(p_in.shape[0] - rec.shape[1] // 2, rec.shape[1] // 2), :]
        over = remote(s1g, rg, xs, xr, spot.at(spot.z, spot.y, 1 - spot.x, spot.c))

        @pl.when(i == 0)
        def _():
            spot.meet()
            for k in range(line.K):
                line.start(k)
            over.start()
            sc.start(rest, 0)

        for k in range(line.K + 2):
            @pl.when(i == k + 2)
            def _():
                for at, call in line.stages():
                    if at == k:
                        call()
    c = pl.num_programs(0) - 1 - i
    W = hq * PH
    reps = W // 128
    CI = g_in.shape[1]

    @pl.when(i == 0)
    def _():
        dS[...] = jnp.zeros_like(dS)
        pg[pl.ds(T, 8), :] = jnp.zeros((8, CI), F32)
        gbuf[pl.ds(T + 8, 8), :] = jnp.full((8, 128), -1.0, F32)
        ps[pl.ds(T, 8), :] = jnp.zeros((8, 256), F32)
        wg_out[...] = jnp.zeros_like(wg_out)
        ws_out[...] = jnp.zeros_like(ws_out)
        hg_out[...] = jnp.zeros_like(hg_out)

    @pl.when(i > 0)
    def _():
        pg[pl.ds(T, 8), :] = pg[pl.ds(0, 8), :]
        ps[pl.ds(T, 8), :] = ps[pl.ds(0, 8), :]
        gbuf[pl.ds(T + 8, 8), :] = gbuf[pl.ds(8, 8), :]

    vbuf[pl.ds(0, 8), :] = inp8[...]
    vbuf[pl.ds(8, T), :] = inp[...]
    sbuf[pl.ds(0, 8), :] = st8[...]
    sbuf[pl.ds(8, T), :] = st[...]
    first = jnp.where(c == 0, 1.0, 0.0)
    gbuf[pl.ds(0, 8), :] = segb8[...] * (1.0 - first) - first
    gbuf[pl.ds(8, T), :] = segb[...]
    seg = segb[...]
    for k in range(1, 4):
        mbuf[k - 1] = jnp.where(gbuf[pl.ds(8 - k, T), :] == seg, 1.0, 0.0)
        nbuf[k - 1] = jnp.where(gbuf[pl.ds(8 + k, T), :] == seg, 1.0, 0.0)
    before = gbuf[pl.ds(7, 1), :]
    last = gbuf[pl.ds(T + 7, 1), :]
    cs = sbuf[pl.ds(8, T), :] * cws[3:4, :] + cbs[...]
    for k in range(1, 4):
        cs = cs + tile2(mbuf[k - 1], 2) * sbuf[pl.ds(8 - k, T), :] * cws[3 - k : 4 - k, :]
    ss = sigm(cs)
    ms = cs * ss
    Cf = ms[:, 128:]
    Bb = ms[:, :128].astype(BF)
    Cb = Cf.astype(BF)
    Ct = Cf.T.astype(BF)
    GT = mm_nt(Bb, Cb)
    z = stp[...] + sbias[...]
    dt, logdt = step_values(z)
    a = arow[...] * dt
    cum = prefix_sum(a) * LOG2E
    cj = cum - logdt * LOG2E
    cmt[...] = cum.T
    rows = iota((T, T), 0)
    cols = iota((T, T), 1)
    segrow = segr[pl.ds(c, 1), :]
    maskb = jnp.where((seg == segrow) & (rows <= cols), 0.0, NEG)
    cont = tile2(jnp.where(seg == before, 1.0, 0.0), reps)
    trail = tile2(jnp.where(seg == last, 1.0, 0.0), reps)
    unbroken = tile2(jnp.where(last == before, 1.0, 0.0), reps)
    Z[...] = jnp.zeros_like(Z)
    WT[...] = jnp.zeros_like(WT)
    DBC[...] = jnp.zeros_like(DBC)

    def colsum(v):
        acc = v[0:8]
        for r in range(1, T // 8):
            acc = acc + v[8 * r : 8 * r + 8]
        return acc

    def body(q, carry):
        lane = pl.ds(pl.multiple_of(q * W, 128), W)
        v0 = vbuf[pl.ds(8, T), lane]
        cv = v0 * cw[3:4, lane] + cb[:, lane]
        vk = []
        for k in range(1, 4):
            vk.append(tile2(mbuf[k - 1], reps) * vbuf[pl.ds(8 - k, T), lane])
            cv = cv + vk[-1] * cw[3 - k : 4 - k, lane]
        sx = sigm(cv)
        x = cv * sx
        xb = x.astype(BF)
        xr = xb.astype(F32)
        yv = y[:, lane] - skip[:, lane] * x
        gb = g_in[:, lane]
        g = gb.astype(F32)
        tcols = head_cols(cum, q, hq)
        jcols = head_cols(cj, q, hq)
        te = per_pair(tcols, W)
        tl = te[T - 1 : T, :]
        ec = jnp.exp2(te) * cont
        w = jnp.exp2(tl - per_pair(jcols, W)) * trail
        dxs = []
        wt = jnp.zeros((T, T), F32)
        for p in range(hq // 2):
            gbd = block_diag(gb[:, 128 * p : 128 * p + 128])
            et = mm_nt(xb[:, 128 * p : 128 * p + 128], gbd)
            mts = []
            for h in range(2):
                n = 2 * p + h
                row = cmt[pl.ds(q * hq + n, 1), :]
                kt = jnp.exp2(row - jcols[n] + maskb)
                mts.append((kt * GT).astype(BF))
                wt = wt + kt * et[:, T * h : T * h + T]
            dxs.append(mm(jnp.concatenate(mts, axis=1), gbd))
        WT[...] += wt
        dxi = dxs[0] if len(dxs) == 1 else jnp.concatenate(dxs, axis=1)
        Sb = s_in[0, :, lane]
        dSq = dS[:, lane]
        dSb = dSq.astype(BF)
        dxo = mm(Bb, dSb) * w
        wx = (x * w).astype(BF)
        eg = (g * ec).astype(BF)
        DBC[:, :128] += mm_nt(wx, dSb)
        DBC[:, 128:] += mm_nt(eg, Sb)
        el = jnp.exp2(tl) * unbroken
        prow = jnp.sum(Sb.astype(F32) * dSq, axis=0, keepdims=True) * el
        dS[:, lane] = dSq * el + mm(Ct, eg)
        ci = xr * dxi
        co = xr * dxo
        diff = g * yv - ci
        hi = diff.astype(BF)
        lo = (diff - hi.astype(F32)).astype(BF)
        stack = jnp.concatenate([hi, co.astype(BF), (ci + co).astype(BF), jnp.broadcast_to(prow, (16, W)).astype(BF)], axis=0)
        ey = eye[pl.ds(pl.multiple_of(q * W, 128), W), :]
        Z[...] += mm(stack, ey)
        Z[0:T, :] += mm(lo, ey)
        pre = (dxi + dxo + skip[:, lane] * g) * (sx + x * (1.0 - sx))
        pg[pl.ds(0, T), lane] = pre
        dv = pre * cw[3:4, lane]
        for k in range(1, 4):
            dv = dv + tile2(nbuf[k - 1], reps) * pg[pl.ds(k, T), lane] * cw[3 - k : 4 - k, lane]
        ca_out[:, lane] = dv.astype(BF)
        wg_out[0:8, lane] += colsum(pre * vk[2])
        wg_out[8:16, lane] += colsum(pre * vk[1])
        wg_out[16:24, lane] += colsum(pre * vk[0])
        wg_out[24:32, lane] += colsum(pre * v0)
        wg_out[32:40, lane] += colsum(pre)
        wg_out[40:48, lane] += colsum(g * x)
        return carry

    lax.fori_loop(0, groups, body, 0)
    z2 = Z[T : 2 * T, :]
    D = suffix_sum(Z[0:T, :]) + (prefix_sum(z2) - z2) + Z[3 * T : 3 * T + 1, :]
    sz = sigm(z)
    lowz = z < -15.0
    rho = jnp.where(lowz, 1.0, jax.nn.sigmoid(z) / jnp.where(lowz, 1.0, dt))
    dz = Z[2 * T : 3 * T, :] * rho + D * arow[...] * jnp.where(lowz, dt, sz)
    ca_out[:, CI + 256 : CI + 384] = dz.astype(BF)
    hg_out[0:8, :] += colsum(D * a)
    hg_out[8:16, :] += colsum(dz)
    wtb = WT[...]
    dbs = DBC[:, :128] + mm_fine(wtb, Cf)
    dcs = DBC[:, 128:] + mm_fine(wtb.T, ms[:, :128])
    pres = jnp.concatenate([dbs, dcs], axis=1) * (ss * (1.0 + cs * (1.0 - ss)))
    ps[pl.ds(0, T), :] = pres
    dsv = pres * cws[3:4, :]
    ws_out[24:32, :] += colsum(pres * sbuf[pl.ds(8, T), :])
    ws_out[32:40, :] += colsum(pres)
    for k in range(1, 4):
        dsv = dsv + tile2(nbuf[k - 1], 2) * ps[pl.ds(k, T), :] * cws[3 - k : 4 - k, :]
        ws_out[24 - 8 * k : 32 - 8 * k, :] += colsum(pres * (tile2(mbuf[k - 1], 2) * sbuf[pl.ds(8 - k, T), :]))
    ca_out[:, CI : CI + 256] = dsv.astype(BF)
    if dp:
        @pl.when(i == pl.num_programs(0) - 1)
        def _():
            over.wait()

            def total(lane):
                f_g[:, lane] = (s0g[:, lane] + rg[:, lane].astype(F32)).astype(BF)

            columns(f_g, total)
            line.finish()
            done = pltpu.make_async_copy(line.fin, d_out, ds)
            done.start()
            done.wait()
            sc.sent(rest, 0)
            sc.got(0)


def scan_backward(proj, segb, segr, g, y, s_in, cw, cb, cws, cbs, sbias, arow, skip, eye, moves=None, rows=0, dp=0):
    L, CI = g.shape
    heads = CI // PH
    hq = 4 if heads % 4 == 0 else 2
    nch = L // T
    blk = lambda w: pl.BlockSpec((T, w), lambda i: (nch - 1 - i, 0))
    part = lambda w, at: pl.BlockSpec((T, w), lambda i: (nch - 1 - i, at // w))
    tail = lambda w, at: pl.BlockSpec((8, w), lambda i: (jnp.maximum((nch - 1 - i) * (T // 8) - 1, 0), at // w))
    ins, in_specs, outs, out_specs, scratch, extra = [], [], [], [], [], {}
    if dp:
        f_o, s0g, s1g, p_in = ins = list(moves)
        once = lambda v: pl.BlockSpec(v.shape, lambda i: (0, 0), pipeline_mode=pl.Buffered(1))
        in_specs = [once(f_o), once(s0g), ANY, ANY]
        like = jax.ShapeDtypeStruct(f_o.shape, BF)
        outs = [like, like, jax.ShapeDtypeStruct((2, 2 * rows, p_in.shape[1] // 4), BF)]
        out_specs = [ANY, full(f_o.shape), ANY]
        dma = pltpu.SemaphoreType.DMA
        scratch = [pltpu.VMEM(s1g.shape, BF), dma, dma, dma] + line_scratch(*f_o.shape, even(f_o.shape[1])) + scatter_sems(1)
        extra = dict(collective_id=5, has_side_effects=True)
    return pl.pallas_call(
        functools.partial(bwd_kernel, hq, heads // hq, dp),
        grid=(nch,),
        in_specs=[blk(CI), tail(CI, 0), part(256, CI), tail(256, CI), part(128, CI + 256), blk(128), tail(128, 0),
                  full(segr.shape), blk(CI), blk(CI), pl.BlockSpec((1, 128, CI), lambda i: (nch - 1 - i, 0, 0)),
                  full(cw.shape), full(cb.shape), full(cws.shape), full(cbs.shape), full(sbias.shape), full(arow.shape),
                  full(skip.shape), full(eye.shape)] + in_specs,
        out_specs=[blk(CI + 384), full((48, CI)), full((40, 256)), full((16, 128))] + out_specs,
        out_shape=[jax.ShapeDtypeStruct((L, CI + 384), BF),
                   jax.ShapeDtypeStruct((48, CI), F32), jax.ShapeDtypeStruct((40, 256), F32), jax.ShapeDtypeStruct((16, 128), F32)] + outs,
        scratch_shapes=[pltpu.VMEM((128, CI), F32), pltpu.VMEM((T + 8, CI), F32), pltpu.VMEM((T + 8, 256), F32),
                        pltpu.VMEM((T + 16, 128), F32), pltpu.VMEM((3, T, 128), F32), pltpu.VMEM((3, T, 128), F32),
                        pltpu.VMEM((T + 8, CI), F32), pltpu.VMEM((T + 8, 256), F32), pltpu.VMEM((128, T), F32),
                        pltpu.VMEM((3 * T + 16, 128), F32), pltpu.VMEM((T, T), F32), pltpu.VMEM((T, 256), F32)] + scratch,
        compiler_params=pltpu.CompilerParams(dimension_semantics=("arbitrary",), vmem_limit_bytes=62 << 20, **extra),
        cost_estimate=pl.CostEstimate(flops=2 * L * CI * (4 * T + 768), bytes_accessed=L * CI * 24, transcendentals=L * CI * 8),
        name="scan_backward",
    )(proj, proj, proj, proj, proj, segb, segb, segr, g, y, s_in, cw, cb, cws, cbs, sbias, arow, skip, eye, *ins)


class Plain:
    def gather_rows(self, h):
        rows = lax.all_gather(h, "head", axis=0, tiled=True)
        return lax.all_to_all(rows, "mp", split_axis=0, concat_axis=1, tiled=True)

    def scatter_rows(self, part):
        rows = lax.all_to_all(part, "mp", split_axis=1, concat_axis=0, tiled=True)
        return lax.psum_scatter(rows.astype(F32), "head", scatter_dimension=0, tiled=True)

    def gather_weight(self, w, axis):
        return lax.all_gather(w, "mp", axis=axis, tiled=True)

    def feature_order(self, v):
        return v

    def head_sum(self, v):
        return lax.psum(v, "head")

    def weight_sum(self, dw, axis):
        own = lax.psum_scatter(dw, "mp", scatter_dimension=axis, tiled=True)
        return lax.psum(own, "dp")

    def state_sum(self, dw):
        size = dw.shape[1] // lax.axis_size("head")
        return lax.psum_scatter(dw, "head", scatter_dimension=1, tiled=True)

    def total(self, v):
        return lax.psum(v, ("dp", "head", "mp"))


class Square:
    def __init__(self):
        self.x = lax.axis_index("mp") // 2
        self.c = lax.axis_index("mp") % 2

    def feature_order(self, v):
        x, c = self.x, self.c
        width = v.shape[0] // 4
        quarters = [x * 2 + c, (1 - x) * 2 + c, x * 2 + 1 - c, (1 - x) * 2 + 1 - c]
        return jnp.concatenate([lax.dynamic_slice_in_dim(v, q * width, width, 0) for q in quarters])


def shards(hidden, in_gain, proj_gate, proj_input, proj_state, proj_step, conv_input, bias_input, conv_state, bias_state,
           step_bias, decay_log, skip_gain, gate_gain, proj_out, segment_ids, cotangent):
    head_pos = lax.axis_index("head")
    sizes = (lax.axis_size("dp"), lax.axis_size("head"), lax.axis_size("mp"))
    square = sizes[1] == 2 and sizes[2] == 4 and sizes[0] == 4
    net = Square() if square else Plain()
    CI = proj_gate.shape[1]
    heads = proj_step.shape[1]
    head_dim = CI // heads
    D = in_gain.shape[0]
    HP = gate_gain.shape[0]
    L = segment_ids.shape[1]
    NST = proj_state.shape[1]
    wt = jnp.concatenate([proj_state, jnp.pad(proj_step, ((0, 0), (0, 128 - heads)))], axis=1)

    own_cols = lambda v: lax.dynamic_slice_in_dim(v, head_pos * CI, CI, v.ndim - 1)
    own_heads = lambda v: lax.dynamic_slice_in_dim(v, head_pos * heads, heads, 0)
    lanes = lambda v: jnp.pad(v[None], ((0, 0), (0, 128 - heads)))
    cw, cb = own_cols(conv_input), own_cols(bias_input)[None]
    gain2 = own_cols(gate_gain)[None]
    sbias = lanes(own_heads(step_bias))
    arow = lanes(-jnp.exp(own_heads(decay_log)))
    skip = jnp.repeat(own_heads(skip_gain), head_dim)[None]
    eye = (jnp.arange(CI)[:, None] // head_dim == jnp.arange(128)[None, :]).astype(BF)
    seg = segment_ids.astype(F32).reshape(L)
    segb = jnp.broadcast_to(seg[:, None], (L, 128))
    segr = seg.reshape(L // T, T)
    small = (cw, cb, conv_state, bias_state[None], sbias, arow, skip)

    gain1 = net.feature_order(in_gain)
    if square:
        jn, s_in, s1c, hid, normed, proj, wa, cot, wg, wo = scan_forward(
            None, segb, segr, *small, moves=(gain1[None], hidden, proj_input, wt, cotangent, proj_gate, proj_out), dp=sizes[0])
    else:
        hid = net.gather_rows(hidden)
        wa = net.gather_weight(jnp.concatenate([proj_input, wt], axis=1), 0)
        rows = hid.astype(F32)
        s1 = lax.rsqrt(jnp.mean(rows * rows, axis=1, keepdims=True) + EPS)
        normed = (rows * s1 * gain1).astype(BF)
        proj = jnp.dot(normed, wa, preferred_element_type=F32)
        jn, s_in = scan_forward(proj, segb, segr, *small)
        cot = net.gather_rows(cotangent)
        wg = net.gather_weight(proj_gate, 0)
        wo = net.gather_weight(proj_out, 1)
    if square:
        gg, gs, inner_out, pscaled, dgn = gate_and_out(normed, jn, wg, wo, cot, gain2, HP, sizes[0])
        early = L // 4
        f_o, s0g, s1g, rec_a = pair_grads(cot, inner_out, normed, gg, pscaled, early, sizes[0])
    else:
        gate = jnp.dot(normed, wg, preferred_element_type=F32)
        sg = sigm(gate)
        sl = gate * sg
        gated = jn * sl
        part = jnp.dot((gated * gain2).astype(BF), wo, preferred_element_type=F32)
        both = net.head_sum(jnp.stack([jnp.sum(gated * gated, axis=1), jnp.sum(part * cot.astype(F32), axis=1)]))
        s2 = lax.rsqrt(both[0] / HP + EPS)[:, None]
        coef = s2 * s2 * s2 * both[1][:, None] / HP
        block = net.scatter_rows((part * s2).astype(BF))
        gis = lax.dot_general(cot, wo, (((1,), (1,)), ((), ())), preferred_element_type=F32) * s2
        gv = gis * gain2 - gated * coef
        gg = (gv * jn * (sg * (1.0 + gate * (1.0 - sg)))).astype(BF)
        gs = (gv * sl).astype(BF)
        inner_out = (gated * s2 * gain2).astype(BF)
        dgn = jnp.sum(gis * gated, axis=0, keepdims=True)
    if square:
        ca, wgr, wsr, hgr, d_o, f_g, rec_b = scan_backward(proj, segb, segr, gs, jn, s_in, *small, eye, moves=(f_o, s0g, s1g, pscaled),
                                                           rows=L - early, dp=sizes[0])
    else:
        ca, wgr, wsr, hgr = scan_backward(proj, segb, segr, gs, jn, s_in, *small, eye)

    tn = lambda a, b: lax.dot_general(a, b, (((0,), (0,)), ((), ())), preferred_element_type=F32)
    nt = lambda a, b: lax.dot_general(a, b, (((1,), (1,)), ((), ())), preferred_element_type=F32)
    wide = lambda v: lax.dynamic_update_slice_in_dim(jnp.zeros(v.shape[:-1] + (HP,), F32), v, head_pos * CI, v.ndim - 1)
    nheads = step_bias.shape[0]
    few = lambda v: lax.dynamic_update_slice_in_dim(jnp.zeros((nheads,), F32), v, head_pos * heads, 0)
    w7 = jnp.sum(wgr.reshape(6, 8, CI), axis=1)
    w5 = jnp.sum(wsr.reshape(5, 8, NST), axis=1)
    h2 = jnp.sum(hgr.reshape(2, 8, 128), axis=1)[:, :heads]
    dskip = jnp.sum(w7[5].reshape(heads, head_dim), axis=1)
    pack = [jnp.zeros((D,), F32), wide(w7[0:4]), wide(w7[4]), w5[0:4], w5[4], few(h2[1]), few(h2[0]), few(dskip),
            wide(jnp.sum(dgn, axis=0))]
    lines = []
    segs = []
    at = 0
    for v in pack:
        width = v.shape[-1]
        r = jnp.pad(v.reshape(-1, width), ((0, 0), (0, -width % 128))).reshape(-1, 128)
        segs.append((at, v.shape))
        lines.append(r)
        at += r.shape[0]
    lines = jnp.pad(jnp.concatenate(lines), ((0, -at % 8), (0, 0)))
    if square:
        fin_g, fin_a, other, rec_h, lines = tail(gg, ca, wg, wa, normed, hid, s1c, gain1[None], f_g, lines, sizes[0])
        block_out, hidden_grad, dwg, dwi, dws, dwt, dwo, *outs = finish(segs, rec_h, cotangent, rec_a, rec_b, hidden, fin_g, fin_a, d_o,
                                                                        other, lines, heads)
    else:
        dwo = net.weight_sum(tn(inner_out, cot), 1)
        dwg = net.weight_sum(tn(normed, gg), 0)
        dwa = net.weight_sum(tn(normed, ca), 0)
        dwi, dwt = dwa[:, :CI], dwa[:, CI + NST : CI + NST + heads]
        dws = net.state_sum(dwa[:, CI : CI + NST])
        ng = nt(gg, wg) + nt(ca, wa)
        grow = ng * gain1
        srow = jnp.sum(grow * rows, axis=1, keepdims=True)
        hidden_grad = cotangent.astype(F32) + net.scatter_rows((grow * s1 - rows * (s1 * s1 * s1 * srow / D)).astype(BF))
        block_out = (hidden.astype(F32) + block).astype(BF)
        lines = lax.dynamic_update_slice_in_dim(lines, jnp.sum(ng * rows * s1, axis=0).reshape(-1, 128), 0, 0)
        lines = net.total(lines)
        outs = []
        for at, shape in segs:
            width = shape[-1]
            per = -(-width // 128)
            count = shape[0] if len(shape) == 2 else 1
            outs.append(lines[at : at + count * per].reshape(count, per * 128)[:, :width].reshape(shape))

    return (block_out, hidden_grad, outs[0], dwg, dwi, dws, dwt, outs[1], outs[2], outs[3],
            outs[4], outs[5], outs[6], outs[7], outs[8], dwo)


def solution(mesh):
    return jax.shard_map(
        shards,
        mesh=mesh,
        in_specs=(
            P(("dp", "head"), "mp"), P(), P("mp", "head"), P("mp", "head"), P("mp", None), P("mp", "head"), P(), P(), P(), P(),
            P(), P(), P(), P(), P("head", "mp"), P(("dp", "mp"), None), P(("dp", "head"), "mp"),
        ),
        out_specs=(
            P(("dp", "head"), "mp"), P(("dp", "head"), "mp"), P(), P("mp", "head"), P("mp", "head"), P("mp", "head"), P("mp", "head"),
            P(), P(), P(), P(), P(), P(), P(), P(), P("head", "mp"),
        ),
        check_vma=False,
    )
```
